16 devices in a mesh: col: 2 (over z), row: 8 (over y, x, core).
Axes of the slice: x: 2, y: 2, z: 2, core: 2. Of those that a mesh axis runs over, the one named last changes fastest.
Arguments:
- vel_x: float32 [16, 2, 1024, 512], P(None, None, 'row', 'col')
- vel_y: float32 [16, 2, 1024, 512], P(None, None, 'row', 'col')
- pot_temp: float32 [16, 2, 1024, 512], P(None, None, 'row', 'col')
- salinity: float32 [16, 2, 1024, 512], P(None, None, 'row', 'col')
- surf_eta: float32 [2, 1024, 512], P(None, 'row', 'col')
- trans_x: float32 [2, 1024, 512], P(None, 'row', 'col')
- trans_y: float32 [2, 1024, 512], P(None, 'row', 'col')
- col_depth: float32 [1024, 512], P('row', 'col')
- wet_levels: int32 [1024, 512], P('row', 'col')
- avg_weights: float32 [30], replicated
Outputs:
- output 1: float32 [2, 1024, 512], P(None, 'row', 'col')
- output 2: float32 [2, 1024, 512], P(None, 'row', 'col')
- output 3: float32 [2, 1024, 512], P(None, 'row', 'col')
- output 4: float32 [16, 2, 1024, 512], P(None, None, 'row', 'col')
- output 5: float32 [16, 2, 1024, 512], P(None, None, 'row', 'col')
- output 6: float32 [16, 2, 1024, 512], P(None, None, 'row', 'col')
- output 7: float32 [16, 2, 1024, 512], P(None, None, 'row', 'col')
All inputs are finite; a program needn't handle non-finite values.
Results may differ from the reference program's by a relative error of at most 0.001.
Values sent between devices are 32-bit elements.
A program may use at most 1 GiB of HBM per device.

```python
import jax
import jax.numpy as jnp
from jax import lax

MEMBERS = 2
LEVELS = 16
SUBCYCLES = 30
GRID_Y = 1024
GRID_X = 512

WAVE_COURANT = 0.4
THERM_EXP = 0.2
HALINE_CON = 0.15
PRESS_SCALE = 0.5
VISC_NUMBER = 1.0
DIFF_NUMBER = 0.5


def east_of(field_in):
    return jnp.roll(field_in, -1, axis=-1)


def west_of(field_in):
    return jnp.roll(field_in, 1, axis=-1)


def north_of(field_in):
    return jnp.concatenate([field_in[..., 1:, :], jnp.zeros_like(field_in[..., :1, :])], axis=-2)


def south_of(field_in):
    return jnp.concatenate([jnp.zeros_like(field_in[..., :1, :]), field_in[..., :-1, :]], axis=-2)


def wet_masks(wet_levels, level_total):
    levels = jnp.arange(level_total).reshape(level_total, 1, 1, 1)
    cell_mask = (levels < wet_levels).astype(jnp.float32)
    xface_mask = cell_mask * (levels < east_of(wet_levels)).astype(jnp.float32)
    yface_mask = cell_mask * (levels < north_of(wet_levels)).astype(jnp.float32)
    return cell_mask, xface_mask, yface_mask


def setup_inputs(seed: int = 0) -> dict:
    key_list = jax.random.split(jax.random.key(seed), 12)
    shape_3d = (LEVELS, MEMBERS, GRID_Y, GRID_X)
    shape_2d = (MEMBERS, GRID_Y, GRID_X)
    land_draw = jax.random.randint(key_list[0], (GRID_Y, GRID_X), 0, 10)
    depth_draw = jax.random.randint(key_list[1], (GRID_Y, GRID_X), 1, LEVELS + 1)
    wet_levels = jnp.where(land_draw == 0, 0, jnp.where(land_draw < 5, LEVELS, depth_draw)).astype(jnp.int32)
    cell_mask, xface_mask, yface_mask = wet_masks(wet_levels, LEVELS)
    profile = jnp.cos(jnp.pi * (jnp.arange(LEVELS) + 0.5) / LEVELS).reshape(LEVELS, 1, 1, 1)

    def tracer_field(key_pair):
        key_a, key_b, key_c = jax.random.split(key_pair, 3)
        base_field = jax.random.normal(key_a, shape_2d, jnp.float32)
        mode_field = jax.random.normal(key_b, shape_2d, jnp.float32)
        noise_3d = jax.random.normal(key_c, shape_3d, jnp.float32)
        return cell_mask * (base_field + mode_field * profile + 0.3 * noise_3d)

    vel_x = xface_mask * 0.3 * jax.random.normal(key_list[2], shape_3d, jnp.float32)
    vel_y = yface_mask * 0.3 * jax.random.normal(key_list[3], shape_3d, jnp.float32)
    pot_temp = tracer_field(key_list[4])
    salinity = tracer_field(key_list[5])
    surf_eta = cell_mask[0] * 0.3 * jax.random.normal(key_list[6], shape_2d, jnp.float32)
    trans_x = xface_mask[0] * 0.3 * jax.random.normal(key_list[7], shape_2d, jnp.float32)
    trans_y = yface_mask[0] * 0.3 * jax.random.normal(key_list[8], shape_2d, jnp.float32)
    col_depth = 0.5 + 1.5 * jax.random.uniform(key_list[9], (GRID_Y, GRID_X), jnp.float32)
    step_frac = (jnp.arange(SUBCYCLES) + 1.0) / SUBCYCLES
    raw_weights = step_frac * step_frac * (2.0 - step_frac * step_frac) * (0.3 + 1.4 * jax.random.uniform(key_list[10], (SUBCYCLES,), jnp.float32))
    avg_weights = raw_weights / jnp.sum(raw_weights)
    return {"vel_x": vel_x, "vel_y": vel_y, "pot_temp": pot_temp, "salinity": salinity, "surf_eta": surf_eta, "trans_x": trans_x, "trans_y": trans_y, "col_depth": col_depth, "wet_levels": wet_levels, "avg_weights": avg_weights}


def vertical_solve(right_side, face_mask, strength):
    mask_below = jnp.concatenate([face_mask[1:], jnp.zeros_like(face_mask[:1])], axis=0)
    face_up = face_mask * mask_below
    face_down = jnp.concatenate([jnp.zeros_like(face_up[:1]), face_up[:-1]], axis=0)
    lower_diag = -strength * face_down
    upper_diag = -strength * face_up
    main_diag = 1.0 + strength * (face_down + face_up)

    def forward(state_prev, level_row):
        upper_prev, side_prev = state_prev
        low_k, diag_k, up_k, side_k = level_row
        divisor = diag_k - low_k * upper_prev
        upper_new = up_k / divisor
        side_new = (side_k - low_k * side_prev) / divisor
        return (upper_new, side_new), (upper_new, side_new)

    zero_level = jnp.zeros_like(right_side[0])
    upper_all, side_all = lax.scan(forward, (zero_level, zero_level), (lower_diag, main_diag, upper_diag, right_side))[1]

    def backward(sol_next, level_row):
        up_k, side_k = level_row
        sol_k = side_k - up_k * sol_next
        return sol_k, sol_k

    return lax.scan(backward, zero_level, (upper_all, side_all), reverse=True)[1]


def tracer_step(tracer, vel_x, vel_y, cell_mask):
    flux_x = vel_x * 0.5 * (tracer + east_of(tracer))
    flux_y = vel_y * 0.5 * (tracer + north_of(tracer))
    advected = cell_mask * (tracer - (flux_x - west_of(flux_x) + flux_y - south_of(flux_y)))
    return vertical_solve(advected, cell_mask, DIFF_NUMBER)


def barotropic(surf_eta, trans_x, trans_y, force_x, force_y, depth_x, depth_y, wet_top, xface_top, yface_top, avg_weights):
    sub_count = avg_weights.shape[0]
    step_x = force_x / sub_count
    step_y = force_y / sub_count

    def subcycle(sub_state, weight):
        eta_now, tx_now, ty_now, eta_avg, tx_avg, ty_avg = sub_state
        eta_now = wet_top * (eta_now - WAVE_COURANT * (tx_now - west_of(tx_now) + ty_now - south_of(ty_now)))
        tx_now = xface_top * (tx_now + step_x - WAVE_COURANT * depth_x * (east_of(eta_now) - eta_now))
        ty_now = yface_top * (ty_now + step_y - WAVE_COURANT * depth_y * (north_of(eta_now) - eta_now))
        return (eta_now, tx_now, ty_now, eta_avg + weight * eta_now, tx_avg + weight * tx_now, ty_avg + weight * ty_now), None

    zero_field = jnp.zeros_like(surf_eta)
    end_state = lax.scan(subcycle, (surf_eta, trans_x, trans_y, zero_field, zero_field, zero_field), avg_weights)[0]
    return end_state[3], end_state[4], end_state[5]


def reference(vel_x, vel_y, pot_temp, salinity, surf_eta, trans_x, trans_y, col_depth, wet_levels, avg_weights):
    level_count = vel_x.shape[0]
    cell_mask, xface_mask, yface_mask = wet_masks(wet_levels, level_count)
    density = HALINE_CON * salinity - THERM_EXP * pot_temp
    pressure = (PRESS_SCALE / level_count) * (jnp.cumsum(density, axis=0) - 0.5 * density)
    vy_south = south_of(vel_y)
    vx_north = north_of(vel_x)
    vy_at_x = 0.25 * (vel_y + vy_south + east_of(vel_y) + east_of(vy_south))
    vx_at_y = 0.25 * (vel_x + west_of(vel_x) + vx_north + west_of(vx_north))
    tend_x = xface_mask * (pressure - east_of(pressure) - 0.5 * vel_x * (east_of(vel_x) - west_of(vel_x)) - 0.5 * vy_at_x * (vx_north - south_of(vel_x)))
    tend_y = yface_mask * (pressure - north_of(pressure) - 0.5 * vx_at_y * (east_of(vel_y) - west_of(vel_y)) - 0.5 * vel_y * (north_of(vel_y) - vy_south))
    count_x = jnp.maximum(jnp.sum(xface_mask, axis=0), 1.0)
    count_y = jnp.maximum(jnp.sum(yface_mask, axis=0), 1.0)
    depth_x = 0.5 * (col_depth + east_of(col_depth)) * xface_mask[0]
    depth_y = 0.5 * (col_depth + north_of(col_depth)) * yface_mask[0]
    force_x = depth_x * jnp.sum(tend_x, axis=0) / count_x
    force_y = depth_y * jnp.sum(tend_y, axis=0) / count_y
    pred_x = vertical_solve(vel_x + tend_x, xface_mask, VISC_NUMBER)
    pred_y = vertical_solve(vel_y + tend_y, yface_mask, VISC_NUMBER)
    temp_new = tracer_step(pot_temp, vel_x, vel_y, cell_mask)
    salt_new = tracer_step(salinity, vel_x, vel_y, cell_mask)
    eta_new, trans_x_new, trans_y_new = barotropic(surf_eta, trans_x, trans_y, force_x, force_y, depth_x, depth_y, cell_mask[0], xface_mask[0], yface_mask[0], avg_weights)
    vel_x_new = xface_mask * (pred_x - jnp.sum(pred_x, axis=0) / count_x + trans_x_new / (depth_x + 1.0 - xface_mask[0]))
    vel_y_new = yface_mask * (pred_y - jnp.sum(pred_y, axis=0) / count_y + trans_y_new / (depth_y + 1.0 - yface_mask[0]))
    return eta_new, trans_x_new, trans_y_new, vel_x_new, vel_y_new, temp_new, salt_new
```

```python
import functools
import jax
import jax.numpy as jnp
from jax import lax
from jax.experimental import pallas as pl
from jax.experimental.pallas import tpu as pltpu
from jax.sharding import PartitionSpec as P

SUB = 8
LANE = 128
LAST = 127
ZERO = 0.0
ONE = 1.0
HALF = 0.5
I0, I1, I2, I3 = range(4)
WAVE = 0.4
THERM = 0.2
HALINE = 0.15
PRESS = HALF
VISC = ONE
DIFF = HALF
LEV = 16
MEM = I2
NSUB = 30
ROWS = LANE
COLS = 256
NR = SUB
NC = I2
HALO = 32
NEXT = 144
EXT = 152
BEXT = 208
NEAR = 192
F32 = jnp.float32
CHUNK = 16
NCH = ROWS // CHUNK
SLOTS = I3
BPC = CHUNK // SUB
MESH = pl.DeviceIdType.MESH
LIMIT = 67043328
TILES = (slice(I0, LANE), slice(LANE, 256))
ANY = pl.BlockSpec(memory_space=pl.ANY)
VM = pl.BlockSpec(memory_space=pltpu.VMEM)
SM = pl.BlockSpec(memory_space=pltpu.SMEM)


def solve_factors(strength):
    gain, inner, last = [], [], []
    prev = None
    for k in range(LEV):
        if k == I0:
            diag, edge = ONE + strength, ONE
        else:
            diag, edge = ONE + 2.0 * strength - strength * prev, ONE + strength - strength * prev
        inner.append(ONE / diag)
        last.append(ONE / edge)
        prev = strength / diag
        gain.append(prev)
    return gain, inner, last


def lane_ids():
    return lax.broadcasted_iota(jnp.int32, (SUB, LANE), I1)


def rot(x, shift):
    shift %= LANE
    return x if shift == I0 else pltpu.roll(x, shift, I1)


def neighbours():
    col = lax.axis_index("col")
    row = lax.axis_index("row")
    other = I1 - col
    north = lax.rem(row + I1, NR)
    south = lax.rem(row + NR - I1, NR)
    return {"x": (other, row), "n": (col, north), "s": (col, south), "nx": (other, north), "sx": (other, south)}


def enter(ids):
    barrier = pltpu.get_barrier_semaphore()
    for target in ids.values():
        pl.semaphore_signal(barrier, inc=I1, device_id=target, device_id_type=MESH)
    pl.semaphore_wait(barrier, len(ids))


def wide_pack(lane, m0t0, m0t1, m1t0, m1t1):
    first = jnp.where(lane < 64, m0t0, m0t1)
    second = jnp.where(lane < 64, m1t0, m1t1)
    return jnp.where((lane < 32) | (lane >= 96), first, rot(second, 64))


def edges_kernel(u, v, te, sa, eta, tx, ty, dep, kmt, px, pd, hr, hx2, hd2, hre, hrx, hry, hrh, hrk, big, s2, sh, sk, pk, rowb, pk2, load_sem, load2_sem, send_sem, recv_sem):
    ids = neighbours()
    fields = (u, v, te, sa)
    loads = []
    for m in range(MEM):
        loads.append([pltpu.make_async_copy(fields[f].at[:, m], big.at[m, f], load_sem.at[m, f]) for f in range(4)])
    loads2 = [pltpu.make_async_copy(a, s2.at[i], load2_sem.at[i]) for i, a in enumerate((eta, tx, ty))]
    loads2.append(pltpu.make_async_copy(dep, sh, load2_sem.at[I3]))
    loads2.append(pltpu.make_async_copy(kmt, sk, load2_sem.at[4]))
    for cp in loads2:
        cp.start()
    for cp in loads[I0] + loads[I1]:
        cp.start()
    enter(ids)
    sent = []

    def send(src, dst, who):
        i = len(sent)
        cp = pltpu.make_async_remote_copy(src_ref=src, dst_ref=dst, send_sem=send_sem.at[i], recv_sem=recv_sem.at[i], device_id=ids[who], device_id_type=MESH)
        cp.start()
        sent.append(cp)

    for src, dst in ((eta, hre), (tx, hrx), (ty, hry)):
        send(src.at[:, pl.ds(ROWS - HALO, HALO), :], dst.at[I0], "n")
        send(src.at[:, pl.ds(I0, HALO), :], dst.at[I1], "s")
    for src, dst in ((dep, hrh), (kmt, hrk)):
        send(src.at[pl.ds(ROWS - HALO, HALO), :], dst.at[I0], "n")
        send(src.at[pl.ds(I0, HALO), :], dst.at[I1], "s")
    lane = lane_ids()
    for cp in loads2:
        cp.wait()

    for r in range(ROWS // SUB):
        rows = pl.ds(SUB * r, SUB)
        for i in range(I3):
            pk2[i, rows, :] = wide_pack(lane, *[s2[i, m, rows, t] for m in range(MEM) for t in TILES])
        pk2[I3, rows, :] = wide_pack(lane, *[sh[rows, t] for t in TILES], *[sk[rows, t].astype(F32) for t in TILES])
    pair = lax.rem(lane + I1, LANE) // I2

    def pack3(m):
        for cp in loads[m]:
            cp.wait()

        def body(g, carry):
            for j in range(4):
                rows = pl.ds(pl.multiple_of(g * 32 + SUB * j, SUB), SUB)
                acc = jnp.zeros((SUB, LANE), F32)
                for f in range(4):
                    for k in range(LEV):
                        q = f * LEV + k
                        both = jnp.where(lane < 64, big[m, f, k, rows, TILES[I0]], big[m, f, k, rows, TILES[I1]])
                        acc = jnp.where(pair == q, rot(both, I2 * q), acc)
                pk[m, rows, :] = acc
            return carry

        lax.fori_loop(I0, 4, body, I0)
        for f in range(4):
            for t in range(I2):
                for g in range(I2):
                    ks = pl.ds(SUB * g, SUB)
                    rowb[I0, m, f, t, ks, :] = big[m, f, ks, ROWS - I1, TILES[t]]
                    rowb[I1, m, f, t, ks, :] = big[m, f, ks, I0, TILES[t]]

    def send3(m):
        send(pk.at[m], px.at[m], "x")
        send(pk.at[m, pl.ds(ROWS - SUB, SUB), :], pd.at[I0, m], "nx")
        send(pk.at[m, pl.ds(I0, SUB), :], pd.at[I1, m], "sx")
        send(rowb.at[I0, m], hr.at[I0, m], "n")
        send(rowb.at[I1, m], hr.at[I1, m], "s")

    send(pk2, hx2, "x")
    send(pk2.at[:, pl.ds(ROWS - HALO, HALO), :], hd2.at[I0], "nx")
    send(pk2.at[:, pl.ds(I0, HALO), :], hd2.at[I1], "sx")
    pack3(I0)
    send3(I0)
    pack3(I1)
    send3(I1)
    for cp in sent:
        cp.wait()


def sds(*shape, dtype=F32):
    return jax.ShapeDtypeStruct(shape, dtype)


NSEND_A = 23


def edges_call(u, v, te, sa, eta, tx, ty, dep, kmt):
    return pl.pallas_call(
        edges_kernel,
        name="edges",
        out_shape=(
            sds(MEM, ROWS, LANE), sds(I2, MEM, SUB, LANE), sds(I2, MEM, 4, I2, LEV, LANE),
            sds(4, ROWS, LANE), sds(I2, 4, HALO, LANE),
            sds(I2, MEM, HALO, COLS), sds(I2, MEM, HALO, COLS), sds(I2, MEM, HALO, COLS),
            sds(I2, HALO, COLS), sds(I2, HALO, COLS, dtype=jnp.int32),
        ),
        in_specs=[ANY] * 9,
        out_specs=(ANY,) * 10,
        scratch_shapes=[
            pltpu.VMEM((MEM, 4, LEV, ROWS, COLS), F32),
            pltpu.VMEM((I3, MEM, ROWS, COLS), F32),
            pltpu.VMEM((ROWS, COLS), F32),
            pltpu.VMEM((ROWS, COLS), jnp.int32),
            pltpu.VMEM((MEM, ROWS, LANE), F32),
            pltpu.VMEM((I2, MEM, 4, I2, LEV, LANE), F32),
            pltpu.VMEM((4, ROWS, LANE), F32),
            pltpu.SemaphoreType.DMA((MEM, 4)),
            pltpu.SemaphoreType.DMA((5,)),
            pltpu.SemaphoreType.DMA((NSEND_A,)),
            pltpu.SemaphoreType.DMA((NSEND_A,)),
        ],
        compiler_params=pltpu.CompilerParams(collective_id=I0, has_side_effects=True, vmem_limit_bytes=LIMIT),
    )(u, v, te, sa, eta, tx, ty, dep, kmt)


def columns_kernel(u, v, te, sa, px, pd, hr, dep, kmt, hx2, hrh, hrk, bu, bv, ot, os, sx, sy, nx, ny, us, vs, ts, ss, ps, vel, uwl, stage, pxs, hrs, hs, ki, kf, hks, obu, obv, ost, oss, load_sem, misc_sem, out_sem):
    row = lax.axis_index("row")
    not_south = jnp.where(row == I0, ZERO, ONE).astype(F32)
    not_north = jnp.where(row == NR - I1, ZERO, ONE).astype(F32)
    fields = ((u, us), (v, vs), (te, ts), (sa, ss))

    def load_copies(c):
        rows = pl.ds(pl.multiple_of(CHUNK * c, CHUNK), CHUNK)
        slot = lax.rem(c, SLOTS)
        return [pltpu.make_async_copy(src.at[:, :, rows, :], stage.at[slot, f], load_sem.at[slot, f]) for f, (src, _) in enumerate(fields)]

    def out_copies(c):
        rows = pl.ds(pl.multiple_of(CHUNK * c, CHUNK), CHUNK)
        return [pltpu.make_async_copy(a.at[:, :, rows, :], b.at[:, :, rows, :], out_sem.at[i]) for i, (a, b) in enumerate(((obu, bu), (obv, bv), (ost, ot), (oss, os)))]

    for c in range(NCH - I1, NCH - I1 - SLOTS, -I1):
        for cp in load_copies(jnp.int32(c)):
            cp.start()
    misc = [
        pltpu.make_async_copy(px, pxs.at[:, pl.ds(SUB, ROWS), :], misc_sem.at[I0]),
        pltpu.make_async_copy(pd.at[I0], pxs.at[:, pl.ds(I0, SUB), :], misc_sem.at[I1]),
        pltpu.make_async_copy(pd.at[I1], pxs.at[:, pl.ds(SUB + ROWS, SUB), :], misc_sem.at[I2]),
        pltpu.make_async_copy(hr, hrs, misc_sem.at[I3]),
        pltpu.make_async_copy(hx2.at[I3], hks, misc_sem.at[4]),
    ]
    for t in range(I2):
        cols = pl.ds(LANE * t, LANE)
        misc.append(pltpu.make_async_copy(dep.at[:, cols], hs.at[t, pl.ds(SUB, ROWS), :], misc_sem.at[5 + 4 * t]))
        misc.append(pltpu.make_async_copy(kmt.at[:, cols], ki.at[t, pl.ds(SUB, ROWS), :], misc_sem.at[6 + 4 * t]))
        misc.append(pltpu.make_async_copy(hrh.at[I1, pl.ds(I0, SUB), cols], hs.at[t, pl.ds(SUB + ROWS, SUB), :], misc_sem.at[7 + 4 * t]))
        misc.append(pltpu.make_async_copy(hrk.at[I1, pl.ds(I0, SUB), cols], ki.at[t, pl.ds(SUB + ROWS, SUB), :], misc_sem.at[SUB + 4 * t]))
    for cp in misc:
        cp.start()
    for cp in misc:
        cp.wait()
    lane = lane_ids()
    is_last = lane == LAST
    is_first = lane == I0
    two = range(I2)
    for m in range(MEM):
        pxs[m, I0:SUB, :] = pxs[m, I0:SUB, :] * not_south
        pxs[m, SUB + ROWS:NEXT, :] = pxs[m, SUB + ROWS:NEXT, :] * not_north
        for f, (_, dst) in enumerate(fields):
            for t in two:
                for g in two:
                    ks = pl.ds(SUB * g, SUB)
                    dst[t, ks, m, 7:SUB, :] = (hrs[I0, m, f, t, ks, :] * not_south)[:, None, :]
                    dst[t, ks, m, SUB + ROWS:9 + ROWS, :] = (hrs[I1, m, f, t, ks, :] * not_north)[:, None, :]
    for t in two:
        kf[t, SUB:SUB + ROWS, :] = ki[t, SUB:SUB + ROWS, :].astype(F32)
        kf[t, SUB + ROWS:NEXT, :] = ki[t, SUB + ROWS:NEXT, :].astype(F32) * not_north
    rho_s = PRESS / LEV * HALINE
    rho_t = PRESS / LEV * THERM
    gain, inner, last = solve_factors(DIFF)
    zero = jnp.zeros((SUB, LANE), F32)

    def east(a, b, halo):
        ra, rb = rot(a, LAST), rot(b, LAST)
        return jnp.where(is_last, rb, ra), jnp.where(is_last, halo, rb)

    def west(a, b, halo):
        ra, rb = rot(a, I1), rot(b, I1)
        return jnp.where(is_first, halo, ra), jnp.where(is_first, ra, rb)

    def keep_east(m, k, rows, a, b, edge):
        for t, x in enumerate(east(a, b, rot(edge, LAST - I2 * (LEV + k)))):
            vel[t, k, m, rows, :] = x

    def unpack(r, m, k, edge):
        slot = lax.rem(jnp.maximum(r, I0) // BPC, SLOTS)
        src_rows = pl.ds(pl.multiple_of(SUB * lax.rem(jnp.maximum(r, I0), BPC), SUB), SUB)
        dst_rows = pl.ds(pl.multiple_of(jnp.where(r < I0, NEXT, SUB * r + SUB), SUB), SUB)
        for f, (_, dst) in enumerate(fields):
            x = [stage[slot, f, k, m, src_rows, TILES[t]] for t in two]
            for t in two:
                dst[t, k, m, dst_rows, :] = x[t]
            if f == I1:
                keep_east(m, k, dst_rows, x[I0], x[I1], edge)

    def prime(m, carry):
        south, north, first = pl.ds(I0, SUB), pl.ds(SUB + ROWS, SUB), pl.ds(ROWS, SUB)
        below = [zero, zero]
        for k in range(LEV):
            unpack(jnp.int32(ROWS // SUB - I1), m, k, pxs[m, first, :])
            keep_east(m, k, south, vs[I0, k, m, south, :], vs[I1, k, m, south, :], pxs[m, south, :])
            for t, x in enumerate(west(us[I0, k, m, north, :], us[I1, k, m, north, :], rot(pxs[m, north, :], 129 - I2 * k))):
                uwl[t, k, m, north, :] = x
            for t in two:
                half = (HALF * rho_s) * ss[t, k, m, north, :] - (HALF * rho_t) * ts[t, k, m, north, :]
                ps[t, k, m, north, :] = below[t] + half
                below[t] = (below[t] + half) + half
        return carry

    def block(r):
        y = pl.multiple_of(r * SUB + SUB, SUB)
        rows = pl.ds(y, SUB)
        up = pl.ds(y + I1, SUB)
        down = pl.ds(y - I1, SUB)
        south = pl.ds(y - SUB, SUB)
        out_rows = pl.ds(pl.multiple_of(r * SUB, SUB), SUB)
        kc = [kf[t, rows, :] for t in two]
        hk = hks[out_rows, :]
        ke = east(kc[I0], kc[I1], rot(hk, 63))
        hc = [hs[t, rows, :] for t in two]
        he = east(hc[I0], hc[I1], rot(hk, LAST))
        kx = [jnp.minimum(kc[t], ke[t]) for t in two]
        ky = [jnp.minimum(kc[t], kf[t, up, :]) for t in two]
        scale_x, scale_y = [], []
        for t in two:
            nx[out_rows, TILES[t]] = kx[t]
            ny[out_rows, TILES[t]] = ky[t]
            scale_x.append(jnp.where(kx[t] > ZERO, HALF * (hc[t] + he[t]), ZERO) / (jnp.maximum(kx[t], ONE) * NSUB))
            scale_y.append(jnp.where(ky[t] > ZERO, HALF * (hc[t] + hs[t, up, :]), ZERO) / (jnp.maximum(ky[t], ONE) * NSUB))

        def member(m, carry):
            pc = pxs[m, rows, :]
            edge = pxs[m, south, :]
            below = [zero, zero, zero]
            sum_x = [zero, zero]
            sum_y = [zero, zero]
            run_t = [None, None]
            run_s = [None, None]
            for k in range(LEV):
                unpack(r - I1, m, k, edge)
                q_u, q_v, q_t, q_s = k, LEV + k, I2 * LEV + k, I3 * LEV + k
                uc = [us[t, k, m, rows, :] for t in two]
                vc = [vs[t, k, m, rows, :] for t in two]
                vd = [vs[t, k, m, down, :] for t in two]
                tc = [ts[t, k, m, rows, :] for t in two]
                sc = [ss[t, k, m, rows, :] for t in two]
                t_east = rot(pc, LAST - I2 * q_t)
                s_east = rot(pc, LAST - I2 * q_s)
                press = []
                for i, (a, b) in enumerate(((tc[I0], sc[I0]), (tc[I1], sc[I1]), (t_east, s_east))):
                    half = (HALF * rho_s) * b - (HALF * rho_t) * a
                    now = below[i] + half
                    below[i] = now + half
                    press.append(now)
                pe = east(press[I0], press[I1], press[I2])
                ue = east(uc[I0], uc[I1], rot(pc, LAST - I2 * q_u))
                uw = west(uc[I0], uc[I1], rot(pc, 129 - I2 * q_u))
                vw = west(vc[I0], vc[I1], rot(pc, 129 - I2 * q_v))
                ve = [vel[t, k, m, rows, :] for t in two]
                for t in two:
                    ps[t, k, m, rows, :] = press[t]
                    uwl[t, k, m, rows, :] = uw[t]
                for t in two:
                    un, ud = us[t, k, m, up, :], us[t, k, m, down, :]
                    vq = (vc[t] + vd[t]) + (ve[t] + vel[t, k, m, down, :])
                    uq = (uc[t] + un) + (uw[t] + uwl[t, k, m, up, :])
                    gu = (press[t] - pe[t]) - HALF * (uc[t] * (ue[t] - uw[t])) - 0.125 * (vq * (un - ud))
                    gu = jnp.where(kx[t] > float(k), gu, ZERO)
                    sum_x[t] = sum_x[t] + gu
                    obu[k, m, out_rows, TILES[t]] = uc[t] + gu
                    gv = (press[t] - ps[t, k, m, up, :]) - 0.125 * (uq * (ve[t] - vw[t])) - HALF * (vc[t] * (vs[t, k, m, up, :] - vd[t]))
                    gv = jnp.where(ky[t] > float(k), gv, ZERO)
                    sum_y[t] = sum_y[t] + gv
                    obv[k, m, out_rows, TILES[t]] = vc[t] + gv
                uh = [HALF * uc[t] for t in two]
                vh = [HALF * vc[t] for t in two]
                vdh = [HALF * vd[t] for t in two]
                uwh = HALF * uw[I0]
                for scr, cen, east_col, q, run, dst in ((ts, tc, t_east, q_t, run_t, ost), (ss, sc, s_east, q_s, run_s, oss)):
                    ce = east(cen[I0], cen[I1], east_col)
                    fx = [uh[t] * (cen[t] + ce[t]) for t in two]
                    fw = west(fx[I0], fx[I1], uwh * (rot(pc, 129 - I2 * q) + cen[I0]))
                    for t in two:
                        fy = vh[t] * (cen[t] + scr[t, k, m, up, :])
                        fs = vdh[t] * (scr[t, k, m, down, :] + cen[t])
                        new = cen[t] - ((fx[t] - fw[t]) + (fy - fs))
                        new = jnp.where(kc[t] > float(k), new, ZERO)
                        run[t] = new if k == I0 else new + gain[k - I1] * run[t]
                        dst[k, m, out_rows, TILES[t]] = run[t]
            for t in two:
                sx[m, out_rows, TILES[t]] = scale_x[t] * sum_x[t]
                sy[m, out_rows, TILES[t]] = scale_y[t] * sum_y[t]
                nt = ns = zero
                for k in range(LEV - I1, -I1, -I1):
                    if k == LEV - I1:
                        coef = last[k]
                    else:
                        coef = jnp.where(kc[t] > float(k + I1), inner[k], last[k])
                    wet = kc[t] > float(k)
                    nt = jnp.where(wet, coef * ost[k, m, out_rows, TILES[t]] + gain[k] * nt, ZERO)
                    ns = jnp.where(wet, coef * oss[k, m, out_rows, TILES[t]] + gain[k] * ns, ZERO)
                    ost[k, m, out_rows, TILES[t]] = nt
                    oss[k, m, out_rows, TILES[t]] = ns
            return carry

        lax.fori_loop(I0, MEM, member, I0)

    for cp in load_copies(jnp.int32(NCH - I1)):
        cp.wait()
    lax.fori_loop(I0, MEM, prime, I0)

    def step(i, carry):
        r = ROWS // SUB - I1 - i
        c = r // BPC
        edge = lax.rem(r, BPC) == I0

        @pl.when(edge & (c >= I1))
        def _():
            for cp in load_copies(c - I1):
                cp.wait()

        @pl.when(edge & (c >= SLOTS))
        def _():
            for cp in load_copies(c - SLOTS):
                cp.start()

        @pl.when(edge & (c + I1 < NCH))
        def _():
            for cp in out_copies(c + I1):
                cp.start()

        block(r)
        return carry

    lax.fori_loop(I0, ROWS // SUB, step, I0)
    for cp in out_copies(jnp.int32(I0)):
        cp.start()
    for c in range(NCH):
        for cp in out_copies(jnp.int32(c)):
            cp.wait()


def columns_call(u, v, te, sa, px, pd, hr, dep, kmt, hx2, hrh, hrk):
    big = pltpu.VMEM((I2, LEV, MEM, EXT, LANE), F32)
    full = pltpu.VMEM((LEV, MEM, ROWS, COLS), F32)
    o3 = sds(LEV, MEM, ROWS, COLS)
    o2 = sds(MEM, ROWS, COLS)
    o1 = sds(ROWS, COLS)
    return pl.pallas_call(
        columns_kernel,
        name="columns",
        out_shape=(o3, o3, o3, o3, o2, o2, o1, o1),
        in_specs=[ANY] * 12,
        out_specs=(ANY,) * 4 + (VM,) * 4,
        scratch_shapes=[big] * 7
        + [
            pltpu.VMEM((SLOTS, 4, LEV, MEM, CHUNK, COLS), F32),
            pltpu.VMEM((MEM, NEXT, LANE), F32),
            pltpu.VMEM((I2, MEM, 4, I2, LEV, LANE), F32),
            pltpu.VMEM((I2, NEXT, LANE), F32),
            pltpu.VMEM((I2, NEXT, LANE), jnp.int32),
            pltpu.VMEM((I2, NEXT, LANE), F32),
            pltpu.VMEM((ROWS, LANE), F32),
            full, full, full, full,
            pltpu.SemaphoreType.DMA((SLOTS, 4)),
            pltpu.SemaphoreType.DMA((13,)),
            pltpu.SemaphoreType.DMA((4,)),
        ],
        compiler_params=pltpu.CompilerParams(vmem_limit_bytes=LIMIT),
    )(u, v, te, sa, px, pd, hr, dep, kmt, hx2, hrh, hrk)


def forcing_kernel(sx, sy, hxs, hds, hrx, hry, pk, send_sem, recv_sem):
    ids = neighbours()
    enter(ids)
    lane = lane_ids()
    sent = []

    def send(src, dst, who):
        i = len(sent)
        cp = pltpu.make_async_remote_copy(src_ref=src, dst_ref=dst, send_sem=send_sem.at[i], recv_sem=recv_sem.at[i], device_id=ids[who], device_id_type=MESH)
        cp.start()
        sent.append(cp)

    for r in range(ROWS // SUB):
        rows = pl.ds(SUB * r, SUB)
        for i, a in enumerate((sx, sy)):
            pk[i, rows, :] = wide_pack(lane, *[a[m, rows, t] for m in range(MEM) for t in TILES])
    for src, dst in ((sx, hrx), (sy, hry)):
        send(src.at[:, pl.ds(ROWS - HALO, HALO), :], dst.at[I0], "n")
        send(src.at[:, pl.ds(I0, HALO), :], dst.at[I1], "s")
    send(pk, hxs, "x")
    send(pk.at[:, pl.ds(ROWS - HALO, HALO), :], hds.at[I0], "nx")
    send(pk.at[:, pl.ds(I0, HALO), :], hds.at[I1], "sx")
    for cp in sent:
        cp.wait()


def forcing_call(sx, sy):
    return pl.pallas_call(
        forcing_kernel,
        name="forcing",
        out_shape=(sds(I2, ROWS, LANE), sds(I2, I2, HALO, LANE), sds(I2, MEM, HALO, COLS), sds(I2, MEM, HALO, COLS)),
        in_specs=[VM, VM],
        out_specs=(ANY,) * 4,
        scratch_shapes=[pltpu.VMEM((I2, ROWS, LANE), F32), pltpu.SemaphoreType.DMA((7,)), pltpu.SemaphoreType.DMA((7,))],
        compiler_params=pltpu.CompilerParams(collective_id=I1, has_side_effects=True, vmem_limit_bytes=LIMIT),
    )(sx, sy)


def east5(x, lane):
    last = lane == LAST
    r = [rot(a, LAST) for a in x]
    far = jnp.where(lane == 63, rot(x[I2], 63), r[4])
    return [jnp.where(last, r[I1], r[I0]), jnp.where(last, r[4], r[I1]), jnp.where(last, r[I3], r[I2]), jnp.where(last, rot(x[4], 63), r[I3]), jnp.where(last, r[I0], far)]


def west5(x, lane):
    first = lane == I0
    r = [rot(a, I1) for a in x]
    far = jnp.where(lane == 64, rot(x[I3], 65), r[4])
    return [jnp.where(first, r[4], r[I0]), jnp.where(first, r[I0], r[I1]), jnp.where(first, rot(x[4], 65), r[I2]), jnp.where(first, r[I2], r[I3]), jnp.where(first, r[I1], far)]


def east3(x, lane):
    last = lane == LAST
    r = [rot(a, LAST) for a in x]
    far = jnp.where(lane == 63, rot(x[I0], 63), r[I2])
    return [jnp.where(last, r[I1], r[I0]), jnp.where(last, r[I2], r[I1]), jnp.where(last, r[I0], far)]


SHARED = (I0, I1, I0, I1, I2)


def subcycle_kernel(weights, eta, tx, ty, sx, sy, dep, kmt, hx2, hd2, hre, hrx, hry, hrh, hrk, hxs, hds, hrsx, hrsy, eta_out, tx_out, ty_out, cx_out, cy_out, nat, side, hn, kn, e0, e1, t1, t2, f1, f2, hh, kf, gx, gy, wv, fo, acc1, acc2, tails, sem):
    row = lax.axis_index("row")
    not_south = jnp.where(row == I0, ZERO, ONE).astype(F32)
    not_north = jnp.where(row == NR - I1, ZERO, ONE).astype(F32)
    lane = lane_ids()
    base = SUB + HALO
    top = base + ROWS
    low, mid, high = pl.ds(I0, HALO), pl.ds(HALO, ROWS), pl.ds(HALO + ROWS, HALO)
    copies = []

    def fetch(src, dst):
        copies.append(pltpu.make_async_copy(src, dst, sem))

    for i, (own_, rows_) in enumerate(((eta, hre), (tx, hrx), (ty, hry), (sx, hrsx), (sy, hrsy))):
        fetch(own_, nat.at[i, :, mid, :])
        fetch(rows_.at[I0], nat.at[i, :, low, :])
        fetch(rows_.at[I1], nat.at[i, :, high, :])
    for first, count, main, corner in ((I0, 4, hx2, hd2), (4, I2, hxs, hds)):
        part = pl.ds(first, count)
        fetch(main, side.at[part, mid, :])
        fetch(corner.at[I0], side.at[part, low, :])
        fetch(corner.at[I1], side.at[part, high, :])
    for own_, rows_, dst in ((dep, hrh, hn), (kmt, hrk, kn)):
        fetch(own_, dst.at[mid, :])
        fetch(rows_.at[I0], dst.at[low, :])
        fetch(rows_.at[I1], dst.at[high, :])
    for cp in copies:
        cp.start()
    total = jnp.float32(ZERO)
    moment = jnp.float32(ZERO)
    for n in range(NSUB - I1, -I1, -I1):
        total = total + weights[n]
        moment = moment + total
        tails[n] = total
    for cp in copies:
        cp.wait()
    own = (lane < 32) | (lane >= 96)
    zero = jnp.zeros((SUB, LANE), F32)
    three, five = range(I3), range(5)
    for i in three:
        kf[i, I0:SUB, :] = zero
        kf[i, SUB + NEAR:BEXT, :] = zero
    for r in range(I1, I1 + NEAR // SUB):
        rows, here = pl.ds(SUB * r, SUB), pl.ds(SUB * r - SUB, SUB)
        packed = side[I3, here, :]
        turned = rot(packed, 64)
        levels = [kn[here, t].astype(F32) for t in TILES] + [jnp.where(own, turned, packed)]
        depths = [hn[here, t] for t in TILES] + [jnp.where(own, packed, turned)]
        keep = not_south if r < base // SUB else not_north
        inside = base // SUB <= r < top // SUB
        for i in three:
            kf[i, rows, :] = levels[i] if inside else levels[i] * keep
            hh[i, rows, :] = depths[i]

    for r in range(I1, I1 + NEAR // SUB):
        y = SUB * r
        rows, up, down, here = pl.ds(y, SUB), pl.ds(y + I1, SUB), pl.ds(y - I1, SUB), pl.ds(y - SUB, SUB)
        kc = [kf[i, rows, :] for i in three]
        ke = east3(kc, lane)
        hc = [hh[i, rows, :] for i in three]
        he = east3(hc, lane)
        wet = [kc[i] > ZERO for i in three]
        wet_x = [jnp.minimum(kc[i], ke[i]) > ZERO for i in three]
        wet_y = [jnp.minimum(kc[i], kf[i, up, :]) > ZERO for i in three]
        for i in three:
            gx[i, rows, :] = jnp.where(wet_x[i], (HALF * WAVE * WAVE) * (hc[i] + he[i]), ZERO)
            gy[i, rows, :] = jnp.where(wet_y[i], (HALF * WAVE * WAVE) * (hc[i] + hh[i, up, :]), ZERO)

        def tiles(f, mask):
            slot = f if f < I3 else f + I1
            raw = [nat[f, m, here, t] for m in range(MEM) for t in TILES] + [side[slot, here, :]]
            return [jnp.where(mask[SHARED[i]], raw[i], ZERO) for i in five]

        e = tiles(I0, wet)
        a, b = tiles(I1, wet_x), tiles(I2, wet_y)
        c, d = tiles(I3, wet_x), tiles(4, wet_y)
        aw = west5(a, lane)
        cw = west5(c, lane)
        for i in five:
            t1[i, rows, :] = a[i]
            t2[i, rows, :] = b[i]
            f1[i, rows, :] = c[i]
            f2[i, rows, :] = d[i]
            w = -WAVE * ((a[i] - aw[i]) + (b[i] - t2[i, down, :]))
            fo[i, rows, :] = -WAVE * ((c[i] - cw[i]) + (d[i] - f2[i, down, :]))
            now = e[i] + w
            wv[i, rows, :] = w
            e0[i, rows, :] = now
            acc1[i, rows, :] = weights[I0] * now
            acc2[i, rows, :] = tails[I0] * now

    def advance(src, dst, r, plan):
        y = SUB * r
        rows, up, down = pl.ds(y, SUB), pl.ds(y + I1, SUB), pl.ds(y - I1, SUB)
        now = [src[i, rows, :] for i in five]
        ne = east5(now, lane)
        gxs = [gx[i, rows, :] for i in three]
        gys = [gy[i, rows, :] for i in three]
        gyd = [gy[i, down, :] for i in three]
        fx = [gxs[SHARED[i]] * (ne[i] - now[i]) for i in five]
        fw = west5(fx, lane)
        for i in five:
            j = SHARED[i]
            w = (wv[i, rows, :] + fo[i, rows, :]) + (fx[i] - fw[i]) + (gys[j] * (src[i, up, :] - now[i]) - gyd[j] * (now[i] - src[i, down, :]))
            new = now[i] + w
            wv[i, rows, :] = w
            dst[i, rows, :] = new
            if plan is not None:
                prev, a0, b0, a1, b1 = plan
                s1, s2 = acc1[i, rows, :], acc2[i, rows, :]
                if prev:
                    s1 = s1 + a0 * now[i]
                    s2 = s2 + b0 * now[i]
                acc1[i, rows, :] = s1 + a1 * new
                acc2[i, rows, :] = s2 + b1 * new

    def sweep(src, dst, lo, hi, plan):
        for r in range(lo, hi):
            advance(src, dst, r, plan if base // SUB <= r <= top // SUB else None)

    for begin, end in ((I0, I2), (I2, 6), (6, 10), (10, 14)):
        lo = (I2 * begin + 12) // SUB
        hi = (196 - I2 * begin) // SUB + I1

        def pair(i, carry):
            m = I2 * i + I2
            sweep(e0, e1, lo, hi, None)
            sweep(e1, e0, lo, hi, (True, weights[m - I1], tails[m - I1], weights[m], tails[m]))
            return carry

        lax.fori_loop(begin, end, pair, I0)
    sweep(e0, e1, base // SUB, top // SUB + I1, (False, None, None, weights[NSUB - I1], tails[NSUB - I1]))

    for r in range(ROWS // SUB):
        y = SUB * r + base
        rows, up, out_rows = pl.ds(y, SUB), pl.ds(y + I1, SUB), pl.ds(SUB * r, SUB)
        s = [acc2[i, rows, :] for i in five]
        se = east5(s, lane)
        for m in range(MEM):
            for t in range(I2):
                i = I2 * m + t
                cols = TILES[t]
                eta_out[m, out_rows, cols] = acc1[i, rows, :]
                gxc, gyc = gx[t, rows, :], gy[t, rows, :]
                ux = total * t1[i, rows, :] + moment * f1[i, rows, :] - (ONE / WAVE) * (gxc * (se[i] - s[i]))
                uy = total * t2[i, rows, :] + moment * f2[i, rows, :] - (ONE / WAVE) * (gyc * (acc2[i, up, :] - s[i]))
                tx_out[m, out_rows, cols] = ux
                ty_out[m, out_rows, cols] = uy
                cx_out[m, out_rows, cols] = ux / jnp.where(gxc > ZERO, gxc * (ONE / (WAVE * WAVE)), ONE)
                cy_out[m, out_rows, cols] = uy / jnp.where(gyc > ZERO, gyc * (ONE / (WAVE * WAVE)), ONE)


def subcycle_call(weights, *arrays):
    o2 = sds(MEM, ROWS, COLS)
    five = pltpu.VMEM((5, BEXT, LANE), F32)
    three = pltpu.VMEM((I3, BEXT, LANE), F32)
    return pl.pallas_call(
        subcycle_kernel,
        name="subcycle",
        out_shape=(o2,) * 5,
        in_specs=[SM] + [ANY] * len(arrays),
        out_specs=(VM,) * 5,
        scratch_shapes=[
            pltpu.VMEM((5, MEM, NEAR, COLS), F32),
            pltpu.VMEM((6, NEAR, LANE), F32),
            pltpu.VMEM((NEAR, COLS), F32),
            pltpu.VMEM((NEAR, COLS), jnp.int32),
            five, five, five, five, five, five, three, three, three, three, five, five, five, five,
            pltpu.SMEM((NSUB,), F32),
            pltpu.SemaphoreType.DMA,
        ],
        compiler_params=pltpu.CompilerParams(vmem_limit_bytes=LIMIT),
    )(weights, *arrays)


DROWS = 16


def correct_kernel(bu, bv, nx, ny, cx, cy, ou, ov):
    gain, inner, last = solve_factors(VISC)

    def body(j, carry):
        m = j // (DROWS // SUB)
        rows = pl.ds(pl.multiple_of((j % (DROWS // SUB)) * SUB, SUB), SUB)
        for src, cnt, shift, dst in ((bu, nx, cx, ou), (bv, ny, cy, ov)):
            for t in range(I2):
                cols = slice(LANE * t, LANE * t + LANE)
                n = cnt[rows, cols]
                run = []
                for k in range(LEV):
                    b = src[k, m, rows, cols]
                    run.append(b if k == I0 else b + gain[k - I1] * run[-I1])
                nxt = jnp.zeros((SUB, LANE), F32)
                tot = jnp.zeros((SUB, LANE), F32)
                sol = [None] * LEV
                for k in range(LEV - I1, -I1, -I1):
                    coef = last[k] if k == LEV - I1 else jnp.where(n > float(k + I1), inner[k], last[k])
                    nxt = jnp.where(n > float(k), coef * run[k] + gain[k] * nxt, ZERO)
                    sol[k] = nxt
                    tot = tot + nxt
                add = shift[m, rows, cols] - tot / jnp.maximum(n, ONE)
                for k in range(LEV):
                    dst[k, m, rows, cols] = jnp.where(n > float(k), sol[k] + add, ZERO)
        return carry

    lax.fori_loop(I0, MEM * (DROWS // SUB), body, I0)


def correct_call(bu, bv, nx, ny, cx, cy):
    s3 = pl.BlockSpec((LEV, MEM, DROWS, COLS), lambda r: (I0, I0, r, I0))
    s2 = pl.BlockSpec((MEM, DROWS, COLS), lambda r: (I0, r, I0))
    s1 = pl.BlockSpec((DROWS, COLS), lambda r: (r, I0))
    o3 = sds(LEV, MEM, ROWS, COLS)
    return pl.pallas_call(
        correct_kernel,
        name="correct",
        grid=(ROWS // DROWS,),
        out_shape=(o3, o3),
        in_specs=[s3, s3, s1, s1, s2, s2],
        out_specs=(s3, s3),
        compiler_params=pltpu.CompilerParams(vmem_limit_bytes=LIMIT),
    )(bu, bv, nx, ny, cx, cy)


def local_step(u, v, te, sa, eta, tx, ty, dep, kmt, weights):
    px, pd, hr, hx2, hd2, hre, hrx, hry, hrh, hrk = edges_call(u, v, te, sa, eta, tx, ty, dep, kmt)
    bu, bv, ot, os, sx, sy, nx, ny = columns_call(u, v, te, sa, px, pd, hr, dep, kmt, hx2, hrh, hrk)
    hxs, hds, hrsx, hrsy = forcing_call(sx, sy)
    eta_new, tx_new, ty_new, cx, cy = subcycle_call(weights, eta, tx, ty, sx, sy, dep, kmt, hx2, hd2, hre, hrx, hry, hrh, hrk, hxs, hds, hrsx, hrsy)
    ou, ov = correct_call(bu, bv, nx, ny, cx, cy)
    return eta_new, tx_new, ty_new, ou, ov, ot, os


def solution(mesh):
    s3 = P(None, None, "row", "col")
    s2 = P(None, "row", "col")
    s1 = P("row", "col")
    return jax.shard_map(local_step, mesh=mesh, in_specs=(s3, s3, s3, s3, s2, s2, s2, s1, s1, P()), out_specs=(s2, s2, s2, s3, s3, s3, s3), check_vma=False)
```

```python
import functools
import jax
import jax.numpy as jnp
from jax import lax
from jax.experimental import pallas as pl
from jax.experimental.pallas import tpu as pltpu
from jax.sharding import PartitionSpec as P

SUB = 8
LANE = 128
LAST = 127
ZERO = 0.0
ONE = 1.0
HALF = 0.5
I0, I1, I2, I3 = range(4)
WAVE = 0.4
THERM = 0.2
HALINE = 0.15
PRESS = HALF
VISC = ONE
DIFF = HALF
LEV = 16
MEM = I2
NSUB = 30
ROWS = LANE
COLS = 256
NR = SUB
NC = I2
HALO = 32
NEXT = 144
EXT = 152
BEXT = 208
NEAR = 192
F32 = jnp.float32
CHUNK = 16
NCH = ROWS // CHUNK
SLOTS = I3
BPC = CHUNK // SUB
DEPTH = I3
MESH = pl.DeviceIdType.MESH
LIMIT = 67043328
TILES = (slice(I0, LANE), slice(LANE, 256))
ANY = pl.BlockSpec(memory_space=pl.ANY)
VM = pl.BlockSpec(memory_space=pltpu.VMEM)
SM = pl.BlockSpec(memory_space=pltpu.SMEM)


def solve_factors(strength):
    gain, inner, last = [], [], []
    prev = None
    for k in range(LEV):
        if k == I0:
            diag, edge = ONE + strength, ONE
        else:
            diag, edge = ONE + 2.0 * strength - strength * prev, ONE + strength - strength * prev
        inner.append(ONE / diag)
        last.append(ONE / edge)
        prev = strength / diag
        gain.append(prev)
    return gain, inner, last


def lane_ids():
    return lax.broadcasted_iota(jnp.int32, (SUB, LANE), I1)


def rot(x, shift):
    shift %= LANE
    return x if shift == I0 else pltpu.roll(x, shift, I1)


def neighbours():
    col = lax.axis_index("col")
    row = lax.axis_index("row")
    other = I1 - col
    north = lax.rem(row + I1, NR)
    south = lax.rem(row + NR - I1, NR)
    return {"x": (other, row), "n": (col, north), "s": (col, south), "nx": (other, north), "sx": (other, south)}


def enter(ids):
    barrier = pltpu.get_barrier_semaphore()
    for target in ids.values():
        pl.semaphore_signal(barrier, inc=I1, device_id=target, device_id_type=MESH)
    pl.semaphore_wait(barrier, len(ids))


def wide_pack(lane, m0t0, m0t1, m1t0, m1t1):
    first = jnp.where(lane < 64, m0t0, m0t1)
    second = jnp.where(lane < 64, m1t0, m1t1)
    return jnp.where((lane < 32) | (lane >= 96), first, rot(second, 64))


def edges_kernel(u, v, te, sa, eta, tx, ty, dep, kmt, px, pd, hr, hx2, hd2, hre, hrx, hry, hrh, hrk, big, s2, sh, sk, pk, rowb, pk2, load_sem, load2_sem, send_sem, recv_sem):
    ids = neighbours()
    fields = (u, v, te, sa)
    loads = []
    for m in range(MEM):
        loads.append([pltpu.make_async_copy(fields[f].at[:, m], big.at[m, f], load_sem.at[m, f]) for f in range(4)])
    loads2 = [pltpu.make_async_copy(a, s2.at[i], load2_sem.at[i]) for i, a in enumerate((eta, tx, ty))]
    loads2.append(pltpu.make_async_copy(dep, sh, load2_sem.at[I3]))
    loads2.append(pltpu.make_async_copy(kmt, sk, load2_sem.at[4]))
    for cp in loads2:
        cp.start()
    for cp in loads[I0] + loads[I1]:
        cp.start()
    enter(ids)
    sent = []

    def send(src, dst, who):
        i = len(sent)
        cp = pltpu.make_async_remote_copy(src_ref=src, dst_ref=dst, send_sem=send_sem.at[i], recv_sem=recv_sem.at[i], device_id=ids[who], device_id_type=MESH)
        cp.start()
        sent.append(cp)

    for src, dst in ((eta, hre), (tx, hrx), (ty, hry)):
        send(src.at[:, pl.ds(ROWS - HALO, HALO), :], dst.at[I0], "n")
        send(src.at[:, pl.ds(I0, HALO), :], dst.at[I1], "s")
    for src, dst in ((dep, hrh), (kmt, hrk)):
        send(src.at[pl.ds(ROWS - HALO, HALO), :], dst.at[I0], "n")
        send(src.at[pl.ds(I0, HALO), :], dst.at[I1], "s")
    lane = lane_ids()
    for cp in loads2:
        cp.wait()

    for r in range(ROWS // SUB):
        rows = pl.ds(SUB * r, SUB)
        for i in range(I3):
            pk2[i, rows, :] = wide_pack(lane, *[s2[i, m, rows, t] for m in range(MEM) for t in TILES])
        pk2[I3, rows, :] = wide_pack(lane, *[sh[rows, t] for t in TILES], *[sk[rows, t].astype(F32) for t in TILES])
    pair = lax.rem(lane + I1, LANE) // I2

    def pack3(m):
        for cp in loads[m]:
            cp.wait()

        def body(g, carry):
            for j in range(4):
                rows = pl.ds(pl.multiple_of(g * 32 + SUB * j, SUB), SUB)
                acc = jnp.zeros((SUB, LANE), F32)
                for f in range(4):
                    for k in range(LEV):
                        q = f * LEV + k
                        both = jnp.where(lane < 64, big[m, f, k, rows, TILES[I0]], big[m, f, k, rows, TILES[I1]])
                        acc = jnp.where(pair == q, rot(both, I2 * q), acc)
                pk[m, rows, :] = acc
            return carry

        lax.fori_loop(I0, 4, body, I0)
        for f in range(4):
            for t in range(I2):
                for g in range(I2):
                    ks = pl.ds(SUB * g, SUB)
                    rowb[I0, m, f, t, ks, :] = big[m, f, ks, ROWS - I1, TILES[t]]
                    rowb[I1, m, f, t, ks, :] = big[m, f, ks, I0, TILES[t]]

    def send3(m):
        send(pk.at[m], px.at[m], "x")
        send(pk.at[m, pl.ds(ROWS - SUB, SUB), :], pd.at[I0, m], "nx")
        send(pk.at[m, pl.ds(I0, SUB), :], pd.at[I1, m], "sx")
        send(rowb.at[I0, m], hr.at[I0, m], "n")
        send(rowb.at[I1, m], hr.at[I1, m], "s")

    send(pk2, hx2, "x")
    send(pk2.at[:, pl.ds(ROWS - HALO, HALO), :], hd2.at[I0], "nx")
    send(pk2.at[:, pl.ds(I0, HALO), :], hd2.at[I1], "sx")
    pack3(I0)
    send3(I0)
    pack3(I1)
    send3(I1)
    for cp in sent:
        cp.wait()


def sds(*shape, dtype=F32):
    return jax.ShapeDtypeStruct(shape, dtype)


NSEND_A = 23


def edges_call(u, v, te, sa, eta, tx, ty, dep, kmt):
    return pl.pallas_call(
        edges_kernel,
        name="edges",
        out_shape=(
            sds(MEM, ROWS, LANE), sds(I2, MEM, SUB, LANE), sds(I2, MEM, 4, I2, LEV, LANE),
            sds(4, ROWS, LANE), sds(I2, 4, HALO, LANE),
            sds(I2, MEM, HALO, COLS), sds(I2, MEM, HALO, COLS), sds(I2, MEM, HALO, COLS),
            sds(I2, HALO, COLS), sds(I2, HALO, COLS, dtype=jnp.int32),
        ),
        in_specs=[ANY] * 9,
        out_specs=(ANY,) * 10,
        scratch_shapes=[
            pltpu.VMEM((MEM, 4, LEV, ROWS, COLS), F32),
            pltpu.VMEM((I3, MEM, ROWS, COLS), F32),
            pltpu.VMEM((ROWS, COLS), F32),
            pltpu.VMEM((ROWS, COLS), jnp.int32),
            pltpu.VMEM((MEM, ROWS, LANE), F32),
            pltpu.VMEM((I2, MEM, 4, I2, LEV, LANE), F32),
            pltpu.VMEM((4, ROWS, LANE), F32),
            pltpu.SemaphoreType.DMA((MEM, 4)),
            pltpu.SemaphoreType.DMA((5,)),
            pltpu.SemaphoreType.DMA((NSEND_A,)),
            pltpu.SemaphoreType.DMA((NSEND_A,)),
        ],
        compiler_params=pltpu.CompilerParams(collective_id=I0, has_side_effects=True, vmem_limit_bytes=LIMIT),
    )(u, v, te, sa, eta, tx, ty, dep, kmt)


def columns_kernel(u, v, te, sa, px, pd, hr, dep, kmt, hx2, hrh, hrk, bu, bv, ot, os, sx, sy, nx, ny, us, vs, ts, ss, ps, vel, uwl, sides, stage, pxs, hrs, hs, ki, kf, hks, obu, obv, ost, oss, load_sem, misc_sem, out_sem):
    row = lax.axis_index("row")
    not_south = jnp.where(row == I0, ZERO, ONE).astype(F32)
    not_north = jnp.where(row == NR - I1, ZERO, ONE).astype(F32)
    fields = ((u, us), (v, vs), (te, ts), (sa, ss))

    def load_copies(c):
        rows = pl.ds(pl.multiple_of(CHUNK * c, CHUNK), CHUNK)
        slot = lax.rem(c, SLOTS)
        return [pltpu.make_async_copy(src.at[:, :, rows, :], stage.at[slot, f], load_sem.at[slot, f]) for f, (src, _) in enumerate(fields)]

    def out_copies(c):
        rows = pl.ds(pl.multiple_of(CHUNK * c, CHUNK), CHUNK)
        return [pltpu.make_async_copy(a.at[:, :, rows, :], b.at[:, :, rows, :], out_sem.at[i]) for i, (a, b) in enumerate(((obu, bu), (obv, bv), (ost, ot), (oss, os)))]

    for c in range(NCH - I1, NCH - I1 - SLOTS, -I1):
        for cp in load_copies(jnp.int32(c)):
            cp.start()
    misc = [
        pltpu.make_async_copy(px, pxs.at[:, pl.ds(SUB, ROWS), :], misc_sem.at[I0]),
        pltpu.make_async_copy(pd.at[I0], pxs.at[:, pl.ds(I0, SUB), :], misc_sem.at[I1]),
        pltpu.make_async_copy(pd.at[I1], pxs.at[:, pl.ds(SUB + ROWS, SUB), :], misc_sem.at[I2]),
        pltpu.make_async_copy(hr, hrs, misc_sem.at[I3]),
        pltpu.make_async_copy(hx2.at[I3], hks, misc_sem.at[4]),
    ]
    for t in range(I2):
        cols = pl.ds(LANE * t, LANE)
        misc.append(pltpu.make_async_copy(dep.at[:, cols], hs.at[t, pl.ds(SUB, ROWS), :], misc_sem.at[5 + 4 * t]))
        misc.append(pltpu.make_async_copy(kmt.at[:, cols], ki.at[t, pl.ds(SUB, ROWS), :], misc_sem.at[6 + 4 * t]))
        misc.append(pltpu.make_async_copy(hrh.at[I1, pl.ds(I0, SUB), cols], hs.at[t, pl.ds(SUB + ROWS, SUB), :], misc_sem.at[7 + 4 * t]))
        misc.append(pltpu.make_async_copy(hrk.at[I1, pl.ds(I0, SUB), cols], ki.at[t, pl.ds(SUB + ROWS, SUB), :], misc_sem.at[SUB + 4 * t]))
    for cp in misc:
        cp.start()
    for cp in misc:
        cp.wait()
    lane = lane_ids()
    is_last = lane == LAST
    is_first = lane == I0
    two = range(I2)
    for m in range(MEM):
        pxs[m, I0:SUB, :] = pxs[m, I0:SUB, :] * not_south
        pxs[m, SUB + ROWS:NEXT, :] = pxs[m, SUB + ROWS:NEXT, :] * not_north
        for f, (_, dst) in enumerate(fields):
            for t in two:
                for g in two:
                    ks = pl.ds(SUB * g, SUB)
                    dst[t, ks, m, 7:SUB, :] = (hrs[I0, m, f, t, ks, :] * not_south)[:, None, :]
                    dst[t, ks, m, SUB + ROWS:9 + ROWS, :] = (hrs[I1, m, f, t, ks, :] * not_north)[:, None, :]
    for t in two:
        kf[t, SUB:SUB + ROWS, :] = ki[t, SUB:SUB + ROWS, :].astype(F32)
        kf[t, SUB + ROWS:NEXT, :] = ki[t, SUB + ROWS:NEXT, :].astype(F32) * not_north
    rho_s = PRESS / LEV * HALINE
    rho_t = PRESS / LEV * THERM
    gain, inner, last = solve_factors(DIFF)
    zero = jnp.zeros((SUB, LANE), F32)

    def east(a, b, halo):
        ra, rb = rot(a, LAST), rot(b, LAST)
        return jnp.where(is_last, rb, ra), jnp.where(is_last, halo, rb)

    def push(x, edge, q):
        return [rot(a, LAST) for a in x] + [rot(edge, LAST - I2 * q)], [rot(a, I1) for a in x] + [rot(edge, 129 - I2 * q)]

    def pop_east(east_):
        return jnp.where(is_last, east_[I1], east_[I0]), jnp.where(is_last, east_[I2], east_[I1])

    def pop_west(west_):
        return jnp.where(is_first, west_[I2], west_[I0]), jnp.where(is_first, west_[I0], west_[I1])

    def unpack(r, m, k, edge):
        slot = lax.rem(jnp.maximum(r, I0) // BPC, SLOTS)
        src_rows = pl.ds(pl.multiple_of(SUB * lax.rem(jnp.maximum(r, I0), BPC), SUB), SUB)
        dst_rows = pl.ds(pl.multiple_of(jnp.where(r < I0, NEXT, SUB * r + SUB), SUB), SUB)
        rolled = []
        for f, (_, dst) in enumerate(fields):
            x = [stage[slot, f, k, m, src_rows, TILES[t]] for t in two]
            for t in two:
                dst[t, k, m, dst_rows, :] = x[t]
            rolled.append(push(x, edge, f * LEV + k))
        return rolled

    def settle(r, m, k, rolled):
        dst_rows = pl.ds(pl.multiple_of(jnp.where(r < I0, NEXT, SUB * r + SUB), SUB), SUB)
        ring = lax.rem(r + I2, I2)
        for f in range(4):
            east_, west_ = pop_east(rolled[f][I0]), pop_west(rolled[f][I1])
            for t in two:
                if f == I0:
                    sides[I0, ring, t, k, m, :, :] = east_[t]
                    uwl[t, k, m, dst_rows, :] = west_[t]
                elif f == I1:
                    vel[t, k, m, dst_rows, :] = east_[t]
                    sides[I1, ring, t, k, m, :, :] = west_[t]
                else:
                    sides[I2 * f - I2, ring, t, k, m, :, :] = east_[t]
                    sides[I2 * f - I1, ring, t, k, m, :, :] = west_[t]

    def prime(m, carry):
        south, north, first = pl.ds(I0, SUB), pl.ds(SUB + ROWS, SUB), pl.ds(ROWS, SUB)
        below = [zero, zero]
        for k in range(LEV):
            settle(jnp.int32(ROWS // SUB - I1), m, k, unpack(jnp.int32(ROWS // SUB - I1), m, k, pxs[m, first, :]))
            v_side = push([vs[t, k, m, south, :] for t in two], pxs[m, south, :], LEV + k)[I0]
            u_side = push([us[t, k, m, north, :] for t in two], pxs[m, north, :], k)[I1]
            for t, x in enumerate(pop_east(v_side)):
                vel[t, k, m, south, :] = x
            for t, x in enumerate(pop_west(u_side)):
                uwl[t, k, m, north, :] = x
            for t in two:
                half = (HALF * rho_s) * ss[t, k, m, north, :] - (HALF * rho_t) * ts[t, k, m, north, :]
                ps[t, k, m, north, :] = below[t] + half
                below[t] = (below[t] + half) + half
        return carry

    def block(r):
        y = pl.multiple_of(r * SUB + SUB, SUB)
        rows = pl.ds(y, SUB)
        up = pl.ds(y + I1, SUB)
        down = pl.ds(y - I1, SUB)
        south = pl.ds(y - SUB, SUB)
        out_rows = pl.ds(pl.multiple_of(r * SUB, SUB), SUB)
        kc = [kf[t, rows, :] for t in two]
        hk = hks[out_rows, :]
        ke = east(kc[I0], kc[I1], rot(hk, 63))
        hc = [hs[t, rows, :] for t in two]
        he = east(hc[I0], hc[I1], rot(hk, LAST))
        kx = [jnp.minimum(kc[t], ke[t]) for t in two]
        ky = [jnp.minimum(kc[t], kf[t, up, :]) for t in two]
        scale_x, scale_y = [], []
        for t in two:
            nx[out_rows, TILES[t]] = kx[t]
            ny[out_rows, TILES[t]] = ky[t]
            scale_x.append(jnp.where(kx[t] > ZERO, HALF * (hc[t] + he[t]), ZERO) / (jnp.maximum(kx[t], ONE) * NSUB))
            scale_y.append(jnp.where(ky[t] > ZERO, HALF * (hc[t] + hs[t, up, :]), ZERO) / (jnp.maximum(ky[t], ONE) * NSUB))

        ring = lax.rem(r, I2)

        def member(m, carry):
            edge = pxs[m, south, :]
            below = [zero] * 4
            sum_x = [zero, zero]
            sum_y = [zero, zero]
            run_t = [None, None]
            run_s = [None, None]
            waiting = []
            for ahead in range(LEV + DEPTH):
                if ahead < LEV:
                    waiting.append(unpack(r - I1, m, ahead, edge))
                k = ahead - DEPTH
                if k < I0:
                    continue
                settle(r - I1, m, k, waiting.pop(I0))
                for t in two:
                    uc, un, ud = us[t, k, m, rows, :], us[t, k, m, up, :], us[t, k, m, down, :]
                    vc, vn, vd = vs[t, k, m, rows, :], vs[t, k, m, up, :], vs[t, k, m, down, :]
                    tc, sc = ts[t, k, m, rows, :], ss[t, k, m, rows, :]
                    ue, vw, t_e, t_w, s_e, s_w = [sides[i, ring, t, k, m, :, :] for i in range(6)]
                    uw, ve = uwl[t, k, m, rows, :], vel[t, k, m, rows, :]
                    half = (HALF * rho_s) * sc - (HALF * rho_t) * tc
                    press = below[t] + half
                    below[t] = press + half
                    half = (HALF * rho_s) * s_e - (HALF * rho_t) * t_e
                    press_e = below[I2 + t] + half
                    below[I2 + t] = press_e + half
                    ps[t, k, m, rows, :] = press
                    uh, vh, vdh, uwh = HALF * uc, HALF * vc, HALF * vd, HALF * uw
                    vq = (vc + vd) + (ve + vel[t, k, m, down, :])
                    uq = (uc + un) + (uw + uwl[t, k, m, up, :])
                    gu = (press - press_e) - uh * (ue - uw) - 0.125 * (vq * (un - ud))
                    gu = jnp.where(kx[t] > float(k), gu, ZERO)
                    sum_x[t] = sum_x[t] + gu
                    obu[k, m, out_rows, TILES[t]] = uc + gu
                    gv = (press - ps[t, k, m, up, :]) - 0.125 * (uq * (ve - vw)) - vh * (vn - vd)
                    gv = jnp.where(ky[t] > float(k), gv, ZERO)
                    sum_y[t] = sum_y[t] + gv
                    obv[k, m, out_rows, TILES[t]] = vc + gv
                    wet = kc[t] > float(k)
                    for scr, cen, e, w, run, dst in ((ts, tc, t_e, t_w, run_t, ost), (ss, sc, s_e, s_w, run_s, oss)):
                        fx = uh * (cen + e) - uwh * (w + cen)
                        fy = vh * (cen + scr[t, k, m, up, :]) - vdh * (scr[t, k, m, down, :] + cen)
                        new = jnp.where(wet, cen - (fx + fy), ZERO)
                        run[t] = new if k == I0 else new + gain[k - I1] * run[t]
                        dst[k, m, out_rows, TILES[t]] = run[t]
            for t in two:
                sx[m, out_rows, TILES[t]] = scale_x[t] * sum_x[t]
                sy[m, out_rows, TILES[t]] = scale_y[t] * sum_y[t]
                nt = ns = zero
                for k in range(LEV - I1, -I1, -I1):
                    if k == LEV - I1:
                        coef = last[k]
                    else:
                        coef = jnp.where(kc[t] > float(k + I1), inner[k], last[k])
                    wet = kc[t] > float(k)
                    nt = jnp.where(wet, coef * ost[k, m, out_rows, TILES[t]] + gain[k] * nt, ZERO)
                    ns = jnp.where(wet, coef * oss[k, m, out_rows, TILES[t]] + gain[k] * ns, ZERO)
                    ost[k, m, out_rows, TILES[t]] = nt
                    oss[k, m, out_rows, TILES[t]] = ns
            return carry

        lax.fori_loop(I0, MEM, member, I0)

    for cp in load_copies(jnp.int32(NCH - I1)):
        cp.wait()
    lax.fori_loop(I0, MEM, prime, I0)

    def step(i, carry):
        r = ROWS // SUB - I1 - i
        c = r // BPC
        edge = lax.rem(r, BPC) == I0

        @pl.when(edge & (c >= I1))
        def _():
            for cp in load_copies(c - I1):
                cp.wait()

        @pl.when(edge & (c >= SLOTS))
        def _():
            for cp in load_copies(c - SLOTS):
                cp.start()

        @pl.when(edge & (c + I1 < NCH))
        def _():
            for cp in out_copies(c + I1):
                cp.start()

        block(r)
        return carry

    lax.fori_loop(I0, ROWS // SUB, step, I0)
    for cp in out_copies(jnp.int32(I0)):
        cp.start()
    for c in range(NCH):
        for cp in out_copies(jnp.int32(c)):
            cp.wait()


def columns_call(u, v, te, sa, px, pd, hr, dep, kmt, hx2, hrh, hrk):
    big = pltpu.VMEM((I2, LEV, MEM, EXT, LANE), F32)
    full = pltpu.VMEM((LEV, MEM, ROWS, COLS), F32)
    o3 = sds(LEV, MEM, ROWS, COLS)
    o2 = sds(MEM, ROWS, COLS)
    o1 = sds(ROWS, COLS)
    return pl.pallas_call(
        columns_kernel,
        name="columns",
        out_shape=(o3, o3, o3, o3, o2, o2, o1, o1),
        in_specs=[ANY] * 12,
        out_specs=(ANY,) * 4 + (VM,) * 4,
        scratch_shapes=[big] * 7
        + [
            pltpu.VMEM((6, I2, I2, LEV, MEM, SUB, LANE), F32),
            pltpu.VMEM((SLOTS, 4, LEV, MEM, CHUNK, COLS), F32),
            pltpu.VMEM((MEM, NEXT, LANE), F32),
            pltpu.VMEM((I2, MEM, 4, I2, LEV, LANE), F32),
            pltpu.VMEM((I2, NEXT, LANE), F32),
            pltpu.VMEM((I2, NEXT, LANE), jnp.int32),
            pltpu.VMEM((I2, NEXT, LANE), F32),
            pltpu.VMEM((ROWS, LANE), F32),
            full, full, full, full,
            pltpu.SemaphoreType.DMA((SLOTS, 4)),
            pltpu.SemaphoreType.DMA((13,)),
            pltpu.SemaphoreType.DMA((4,)),
        ],
        compiler_params=pltpu.CompilerParams(vmem_limit_bytes=LIMIT),
    )(u, v, te, sa, px, pd, hr, dep, kmt, hx2, hrh, hrk)


def forcing_kernel(sx, sy, hxs, hds, hrx, hry, pk, send_sem, recv_sem):
    ids = neighbours()
    enter(ids)
    lane = lane_ids()
    sent = []

    def send(src, dst, who):
        i = len(sent)
        cp = pltpu.make_async_remote_copy(src_ref=src, dst_ref=dst, send_sem=send_sem.at[i], recv_sem=recv_sem.at[i], device_id=ids[who], device_id_type=MESH)
        cp.start()
        sent.append(cp)

    for r in range(ROWS // SUB):
        rows = pl.ds(SUB * r, SUB)
        for i, a in enumerate((sx, sy)):
            pk[i, rows, :] = wide_pack(lane, *[a[m, rows, t] for m in range(MEM) for t in TILES])
    for src, dst in ((sx, hrx), (sy, hry)):
        send(src.at[:, pl.ds(ROWS - HALO, HALO), :], dst.at[I0], "n")
        send(src.at[:, pl.ds(I0, HALO), :], dst.at[I1], "s")
    send(pk, hxs, "x")
    send(pk.at[:, pl.ds(ROWS - HALO, HALO), :], hds.at[I0], "nx")
    send(pk.at[:, pl.ds(I0, HALO), :], hds.at[I1], "sx")
    for cp in sent:
        cp.wait()


def forcing_call(sx, sy):
    return pl.pallas_call(
        forcing_kernel,
        name="forcing",
        out_shape=(sds(I2, ROWS, LANE), sds(I2, I2, HALO, LANE), sds(I2, MEM, HALO, COLS), sds(I2, MEM, HALO, COLS)),
        in_specs=[VM, VM],
        out_specs=(ANY,) * 4,
        scratch_shapes=[pltpu.VMEM((I2, ROWS, LANE), F32), pltpu.SemaphoreType.DMA((7,)), pltpu.SemaphoreType.DMA((7,))],
        compiler_params=pltpu.CompilerParams(collective_id=I1, has_side_effects=True, vmem_limit_bytes=LIMIT),
    )(sx, sy)


def turn_east(x):
    return [rot(a, LAST) for a in x] + [rot(x[I2], 63), rot(x[4], 63)]


def pick_east(r, lane):
    last = lane == LAST
    far = jnp.where(lane == 63, r[5], r[4])
    return [jnp.where(last, r[I1], r[I0]), jnp.where(last, r[4], r[I1]), jnp.where(last, r[I3], r[I2]), jnp.where(last, r[6], r[I3]), jnp.where(last, r[I0], far)]


def turn_west(x):
    return [rot(a, I1) for a in x] + [rot(x[I3], 65), rot(x[4], 65)]


def pick_west(r, lane):
    first = lane == I0
    far = jnp.where(lane == 64, r[5], r[4])
    return [jnp.where(first, r[4], r[I0]), jnp.where(first, r[I0], r[I1]), jnp.where(first, r[6], r[I2]), jnp.where(first, r[I2], r[I3]), jnp.where(first, r[I1], far)]


def turn_east3(x):
    return [rot(a, LAST) for a in x] + [rot(x[I0], 63)]


def pick_east3(r, lane):
    last = lane == LAST
    far = jnp.where(lane == 63, r[I3], r[I2])
    return [jnp.where(last, r[I1], r[I0]), jnp.where(last, r[I2], r[I1]), jnp.where(last, r[I0], far)]


def turn_west3(x):
    return [rot(a, I1) for a in x] + [rot(x[I1], 65)]


def pick_west3(r, lane):
    first = lane == I0
    far = jnp.where(lane == 64, r[I3], r[I2])
    return [jnp.where(first, r[I2], r[I0]), jnp.where(first, r[I0], r[I1]), jnp.where(first, r[I1], far)]


def staged(items, issue, finish, depth):
    queue = []
    for item in items:
        queue.append((item, issue(item)))
        if len(queue) > depth:
            finish(*queue.pop(I0))
    for item, value in queue:
        finish(item, value)


SHARED = (I0, I1, I0, I1, I2)


def subcycle_kernel(weights, eta, tx, ty, sx, sy, dep, kmt, hx2, hd2, hre, hrx, hry, hrh, hrk, hxs, hds, hrsx, hrsy, eta_out, tx_out, ty_out, cx_out, cy_out, nat, side, hn, kn, e0, e1, t1, t2, f1, f2, hh, kf, gx, gy, gxw, gc, wv, fo, acc1, acc2, ee, ew, tails, sem):
    row = lax.axis_index("row")
    not_south = jnp.where(row == I0, ZERO, ONE).astype(F32)
    not_north = jnp.where(row == NR - I1, ZERO, ONE).astype(F32)
    lane = lane_ids()
    base = SUB + HALO
    top = base + ROWS
    low, mid, high = pl.ds(I0, HALO), pl.ds(HALO, ROWS), pl.ds(HALO + ROWS, HALO)
    copies = []

    def fetch(src, dst):
        copies.append(pltpu.make_async_copy(src, dst, sem))

    for i, (own_, rows_) in enumerate(((eta, hre), (tx, hrx), (ty, hry), (sx, hrsx), (sy, hrsy))):
        fetch(own_, nat.at[i, :, mid, :])
        fetch(rows_.at[I0], nat.at[i, :, low, :])
        fetch(rows_.at[I1], nat.at[i, :, high, :])
    for first, count, main, corner in ((I0, 4, hx2, hd2), (4, I2, hxs, hds)):
        part = pl.ds(first, count)
        fetch(main, side.at[part, mid, :])
        fetch(corner.at[I0], side.at[part, low, :])
        fetch(corner.at[I1], side.at[part, high, :])
    for own_, rows_, dst in ((dep, hrh, hn), (kmt, hrk, kn)):
        fetch(own_, dst.at[mid, :])
        fetch(rows_.at[I0], dst.at[low, :])
        fetch(rows_.at[I1], dst.at[high, :])
    for cp in copies:
        cp.start()
    total = jnp.float32(ZERO)
    moment = jnp.float32(ZERO)
    for n in range(NSUB - I1, -I1, -I1):
        total = total + weights[n]
        moment = moment + total
        tails[n] = total
    for cp in copies:
        cp.wait()
    own = (lane < 32) | (lane >= 96)
    zero = jnp.zeros((SUB, LANE), F32)
    three, five = range(I3), range(5)
    for i in three:
        kf[i, I0:SUB, :] = zero
        kf[i, SUB + NEAR:BEXT, :] = zero
    everything = range(I1, I1 + NEAR // SUB)

    def rows_of(r):
        return pl.ds(SUB * r, SUB), pl.ds(SUB * r + I1, SUB), pl.ds(SUB * r - I1, SUB), pl.ds(SUB * r - SUB, SUB)

    def level_issue(r):
        here = rows_of(r)[I3]
        packed = side[I3, here, :]
        return packed, rot(packed, 64)

    def level_finish(r, value):
        packed, turned = value
        rows, _, _, here = rows_of(r)
        levels = [kn[here, t].astype(F32) for t in TILES] + [jnp.where(own, turned, packed)]
        depths = [hn[here, t] for t in TILES] + [jnp.where(own, packed, turned)]
        keep = not_south if r < base // SUB else not_north
        inside = base // SUB <= r < top // SUB
        for i in three:
            kf[i, rows, :] = levels[i] if inside else levels[i] * keep
            hh[i, rows, :] = depths[i]

    staged(everything, level_issue, level_finish, SUB)

    def mask_issue(r):
        rows = rows_of(r)[I0]
        kc = [kf[i, rows, :] for i in three]
        hc = [hh[i, rows, :] for i in three]
        return kc, hc, turn_east3(kc), turn_east3(hc)

    def mask_finish(r, value):
        kc, hc, kt, ht = value
        rows, up, down, here = rows_of(r)
        ke, he = pick_east3(kt, lane), pick_east3(ht, lane)
        wet = [kc[i] > ZERO for i in three]
        wet_x = [jnp.minimum(kc[i], ke[i]) > ZERO for i in three]
        wet_y = [jnp.minimum(kc[i], kf[i, up, :]) > ZERO for i in three]
        for i in three:
            gx[i, rows, :] = jnp.where(wet_x[i], (HALF * WAVE * WAVE) * (hc[i] + he[i]), ZERO)
            gy[i, rows, :] = jnp.where(wet_y[i], (HALF * WAVE * WAVE) * (hc[i] + hh[i, up, :]), ZERO)
        for f, mask, dst in ((I0, wet, e0), (I1, wet_x, t1), (I2, wet_y, t2), (I3, wet_x, f1), (4, wet_y, f2)):
            slot = f if f < I3 else f + I1
            raw = [nat[f, m, here, t] for m in range(MEM) for t in TILES] + [side[slot, here, :]]
            for i in five:
                dst[i, rows, :] = jnp.where(mask[SHARED[i]], raw[i], ZERO)

    staged(everything, mask_issue, mask_finish, I3)

    def start_issue(r):
        rows = rows_of(r)[I0]
        a = [t1[i, rows, :] for i in five]
        c = [f1[i, rows, :] for i in five]
        return a, c, turn_west(a), turn_west(c), turn_west3([gx[i, rows, :] for i in three])

    late = []

    def start_finish(r, value):
        a, c, at, ct, gt = value
        rows, up, down, here = rows_of(r)
        aw, cw, gw = pick_west(at, lane), pick_west(ct, lane), pick_west3(gt, lane)
        for i in three:
            gxw[i, rows, :] = gw[i]
            gc[i, rows, :] = (gx[i, rows, :] + gw[i]) + (gy[i, rows, :] + gy[i, down, :])
        fresh = []
        for i in five:
            w = -WAVE * ((a[i] - aw[i]) + (t2[i, rows, :] - t2[i, down, :]))
            fo[i, rows, :] = -WAVE * ((c[i] - cw[i]) + (f2[i, rows, :] - f2[i, down, :]))
            now = e0[i, rows, :] + w
            wv[i, rows, :] = w
            e0[i, rows, :] = now
            acc1[i, rows, :] = weights[I0] * now
            acc2[i, rows, :] = tails[I0] * now
            fresh.append(now)
        late.append((r, turn_east(fresh), turn_west(fresh)))
        if len(late) > I3:
            store_sides(*late.pop(I0), I0)

    def store_sides(r, et, wt, buf):
        rows = rows_of(r)[I0]
        ne, nw = pick_east(et, lane), pick_west(wt, lane)
        for i in five:
            ee[buf, i, rows, :] = ne[i]
            ew[buf, i, rows, :] = nw[i]

    staged(everything, start_issue, start_finish, I3)
    for item in late:
        store_sides(*item, I0)

    def advance(src, buf, dst, r, plan):
        rows, up, down, _ = rows_of(r)
        gxc, gxm, gyc, gyd, gcc = [[g[i, rows_, :] for i in three] for g, rows_ in ((gx, rows), (gxw, rows), (gy, rows), (gy, down), (gc, rows))]
        fresh = []
        for i in five:
            j = SHARED[i]
            now = src[i, rows, :]
            w = (wv[i, rows, :] + fo[i, rows, :]) - gcc[j] * now
            w = w + ((gxc[j] * ee[buf, i, rows, :] + gxm[j] * ew[buf, i, rows, :]) + (gyc[j] * src[i, up, :] + gyd[j] * src[i, down, :]))
            new = now + w
            wv[i, rows, :] = w
            dst[i, rows, :] = new
            fresh.append(new)
            if plan is not None:
                prev, a0, b0, a1, b1 = plan
                s1, s2 = acc1[i, rows, :], acc2[i, rows, :]
                if prev:
                    s1 = s1 + a0 * now
                    s2 = s2 + b0 * now
                acc1[i, rows, :] = s1 + a1 * new
                acc2[i, rows, :] = s2 + b1 * new
        return turn_east(fresh), turn_west(fresh)

    def sweep(src, buf, dst, lo, hi, plan, depth=I3):
        def issue(r):
            return advance(src, buf, dst, r, plan if base // SUB <= r <= top // SUB else None)

        def finish(r, value):
            store_sides(r, *value, I1 - buf)

        staged(range(lo, hi), issue, finish, depth)

    for begin, end in ((I0, I2), (I2, 6), (6, 10), (10, 14)):
        lo = (I2 * begin + 12) // SUB
        hi = (196 - I2 * begin) // SUB + I1

        def pair(i, carry):
            m = I2 * i + I2
            sweep(e0, I0, e1, lo, hi, None)
            sweep(e1, I1, e0, lo, hi, (True, weights[m - I1], tails[m - I1], weights[m], tails[m]))
            return carry

        lax.fori_loop(begin, end, pair, I0)
    sweep(e0, I0, e1, base // SUB, top // SUB + I1, (False, None, None, weights[NSUB - I1], tails[NSUB - I1]))

    def end_issue(r):
        rows = rows_of(r)[I0]
        s = [acc2[i, rows, :] for i in five]
        return s, turn_east(s)

    def end_finish(r, value):
        s, st = value
        rows, up, _, _ = rows_of(r)
        out_rows = pl.ds(SUB * r - base, SUB)
        se = pick_east(st, lane)
        for m in range(MEM):
            for t in range(I2):
                i = I2 * m + t
                cols = TILES[t]
                eta_out[m, out_rows, cols] = acc1[i, rows, :]
                gxc, gyc = gx[t, rows, :], gy[t, rows, :]
                ux = total * t1[i, rows, :] + moment * f1[i, rows, :] - (ONE / WAVE) * (gxc * (se[i] - s[i]))
                uy = total * t2[i, rows, :] + moment * f2[i, rows, :] - (ONE / WAVE) * (gyc * (acc2[i, up, :] - s[i]))
                tx_out[m, out_rows, cols] = ux
                ty_out[m, out_rows, cols] = uy
                cx_out[m, out_rows, cols] = ux / jnp.where(gxc > ZERO, gxc * (ONE / (WAVE * WAVE)), ONE)
                cy_out[m, out_rows, cols] = uy / jnp.where(gyc > ZERO, gyc * (ONE / (WAVE * WAVE)), ONE)

    staged(range(base // SUB, top // SUB), end_issue, end_finish, I3)


def subcycle_call(weights, *arrays):
    o2 = sds(MEM, ROWS, COLS)
    five = pltpu.VMEM((5, BEXT, LANE), F32)
    three = pltpu.VMEM((I3, BEXT, LANE), F32)
    return pl.pallas_call(
        subcycle_kernel,
        name="subcycle",
        out_shape=(o2,) * 5,
        in_specs=[SM] + [ANY] * len(arrays),
        out_specs=(VM,) * 5,
        scratch_shapes=[
            pltpu.VMEM((5, MEM, NEAR, COLS), F32),
            pltpu.VMEM((6, NEAR, LANE), F32),
            pltpu.VMEM((NEAR, COLS), F32),
            pltpu.VMEM((NEAR, COLS), jnp.int32),
            *[five] * 6, *[three] * 6, *[five] * 4, pltpu.VMEM((I2, 5, BEXT, LANE), F32), pltpu.VMEM((I2, 5, BEXT, LANE), F32),
            pltpu.SMEM((NSUB,), F32),
            pltpu.SemaphoreType.DMA,
        ],
        compiler_params=pltpu.CompilerParams(vmem_limit_bytes=LIMIT),
    )(weights, *arrays)


DROWS = 16


def correct_kernel(bu, bv, nx, ny, cx, cy, ou, ov):
    gain, inner, last = solve_factors(VISC)

    def body(j, carry):
        m = j // (DROWS // SUB)
        rows = pl.ds(pl.multiple_of((j % (DROWS // SUB)) * SUB, SUB), SUB)
        for src, cnt, shift, dst in ((bu, nx, cx, ou), (bv, ny, cy, ov)):
            for t in range(I2):
                cols = slice(LANE * t, LANE * t + LANE)
                n = cnt[rows, cols]
                run = []
                for k in range(LEV):
                    b = src[k, m, rows, cols]
                    run.append(b if k == I0 else b + gain[k - I1] * run[-I1])
                nxt = jnp.zeros((SUB, LANE), F32)
                tot = jnp.zeros((SUB, LANE), F32)
                sol = [None] * LEV
                for k in range(LEV - I1, -I1, -I1):
                    coef = last[k] if k == LEV - I1 else jnp.where(n > float(k + I1), inner[k], last[k])
                    nxt = jnp.where(n > float(k), coef * run[k] + gain[k] * nxt, ZERO)
                    sol[k] = nxt
                    tot = tot + nxt
                add = shift[m, rows, cols] - tot / jnp.maximum(n, ONE)
                for k in range(LEV):
                    dst[k, m, rows, cols] = jnp.where(n > float(k), sol[k] + add, ZERO)
        return carry

    lax.fori_loop(I0, MEM * (DROWS // SUB), body, I0)


def correct_call(bu, bv, nx, ny, cx, cy):
    s3 = pl.BlockSpec((LEV, MEM, DROWS, COLS), lambda r: (I0, I0, r, I0))
    s2 = pl.BlockSpec((MEM, DROWS, COLS), lambda r: (I0, r, I0))
    s1 = pl.BlockSpec((DROWS, COLS), lambda r: (r, I0))
    o3 = sds(LEV, MEM, ROWS, COLS)
    return pl.pallas_call(
        correct_kernel,
        name="correct",
        grid=(ROWS // DROWS,),
        out_shape=(o3, o3),
        in_specs=[s3, s3, s1, s1, s2, s2],
        out_specs=(s3, s3),
        compiler_params=pltpu.CompilerParams(vmem_limit_bytes=LIMIT),
    )(bu, bv, nx, ny, cx, cy)


def local_step(u, v, te, sa, eta, tx, ty, dep, kmt, weights):
    px, pd, hr, hx2, hd2, hre, hrx, hry, hrh, hrk = edges_call(u, v, te, sa, eta, tx, ty, dep, kmt)
    bu, bv, ot, os, sx, sy, nx, ny = columns_call(u, v, te, sa, px, pd, hr, dep, kmt, hx2, hrh, hrk)
    hxs, hds, hrsx, hrsy = forcing_call(sx, sy)
    eta_new, tx_new, ty_new, cx, cy = subcycle_call(weights, eta, tx, ty, sx, sy, dep, kmt, hx2, hd2, hre, hrx, hry, hrh, hrk, hxs, hds, hrsx, hrsy)
    ou, ov = correct_call(bu, bv, nx, ny, cx, cy)
    return eta_new, tx_new, ty_new, ou, ov, ot, os


def solution(mesh):
    s3 = P(None, None, "row", "col")
    s2 = P(None, "row", "col")
    s1 = P("row", "col")
    return jax.shard_map(local_step, mesh=mesh, in_specs=(s3, s3, s3, s3, s2, s2, s2, s1, s1, P()), out_specs=(s2, s2, s2, s3, s3, s3, s3), check_vma=False)
```

```python
import functools
import jax
import jax.numpy as jnp
from jax import lax
from jax.experimental import pallas as pl
from jax.experimental.pallas import tpu as pltpu
from jax.sharding import PartitionSpec as P

SUB = 8
LANE = 128
LAST = 127
ZERO = 0.0
ONE = 1.0
HALF = 0.5
I0, I1, I2, I3 = range(4)
WAVE = 0.4
THERM = 0.2
HALINE = 0.15
PRESS = HALF
VISC = ONE
DIFF = HALF
LEV = 16
MEM = I2
NSUB = 30
ROWS = LANE
COLS = 256
NR = SUB
NC = I2
HALO = 32
NEXT = 144
EXT = 152
BEXT = 208
NEAR = 192
F32 = jnp.float32
CHUNK = 16
NCH = ROWS // CHUNK
SLOTS = I3
BPC = CHUNK // SUB
DEPTH = I2
MESH = pl.DeviceIdType.MESH
LIMIT = 67043328
TILES = (slice(I0, LANE), slice(LANE, 256))
ANY = pl.BlockSpec(memory_space=pl.ANY)
VM = pl.BlockSpec(memory_space=pltpu.VMEM)
SM = pl.BlockSpec(memory_space=pltpu.SMEM)


def solve_factors(strength):
    gain, inner, last = [], [], []
    prev = None
    for k in range(LEV):
        if k == I0:
            diag, edge = ONE + strength, ONE
        else:
            diag, edge = ONE + 2.0 * strength - strength * prev, ONE + strength - strength * prev
        inner.append(ONE / diag)
        last.append(ONE / edge)
        prev = strength / diag
        gain.append(prev)
    return gain, inner, last


def level_factor(count, k, inner, last):
    edge = jnp.where(count > float(k), last[k], ZERO)
    return edge if k == LEV - I1 else jnp.where(count > float(k + I1), inner[k], edge)


def lane_ids():
    return lax.broadcasted_iota(jnp.int32, (SUB, LANE), I1)


def rot(x, shift):
    shift %= LANE
    return x if shift == I0 else pltpu.roll(x, shift, I1)


def neighbours():
    col = lax.axis_index("col")
    row = lax.axis_index("row")
    other = I1 - col
    north = lax.rem(row + I1, NR)
    south = lax.rem(row + NR - I1, NR)
    return {"x": (other, row), "n": (col, north), "s": (col, south), "nx": (other, north), "sx": (other, south)}


def enter(ids):
    barrier = pltpu.get_barrier_semaphore()
    for target in ids.values():
        pl.semaphore_signal(barrier, inc=I1, device_id=target, device_id_type=MESH)
    pl.semaphore_wait(barrier, len(ids))


def wide_pack(lane, m0t0, m0t1, m1t0, m1t1):
    first = jnp.where(lane < 64, m0t0, m0t1)
    second = jnp.where(lane < 64, m1t0, m1t1)
    return jnp.where((lane < 32) | (lane >= 96), first, rot(second, 64))


def edges_kernel(u, v, te, sa, eta, tx, ty, dep, kmt, px, pd, hr, hx2, hd2, hre, hrx, hry, hrh, hrk, big, s2, sh, sk, pk, rowb, pk2, load_sem, load2_sem, send_sem, recv_sem):
    ids = neighbours()
    fields = (u, v, te, sa)
    loads = []
    for m in range(MEM):
        loads.append([pltpu.make_async_copy(fields[f].at[:, m], big.at[m, f], load_sem.at[m, f]) for f in range(4)])
    loads2 = [pltpu.make_async_copy(a, s2.at[i], load2_sem.at[i]) for i, a in enumerate((eta, tx, ty))]
    loads2.append(pltpu.make_async_copy(dep, sh, load2_sem.at[I3]))
    loads2.append(pltpu.make_async_copy(kmt, sk, load2_sem.at[4]))
    for cp in loads2:
        cp.start()
    for cp in loads[I0] + loads[I1]:
        cp.start()
    enter(ids)
    sent = []

    def send(src, dst, who):
        i = len(sent)
        cp = pltpu.make_async_remote_copy(src_ref=src, dst_ref=dst, send_sem=send_sem.at[i], recv_sem=recv_sem.at[i], device_id=ids[who], device_id_type=MESH)
        cp.start()
        sent.append(cp)
        return cp

    for src, dst in ((eta, hre), (tx, hrx), (ty, hry)):
        send(src.at[:, pl.ds(ROWS - HALO, HALO), :], dst.at[I0], "n")
        send(src.at[:, pl.ds(I0, HALO), :], dst.at[I1], "s")
    for src, dst in ((dep, hrh), (kmt, hrk)):
        send(src.at[pl.ds(ROWS - HALO, HALO), :], dst.at[I0], "n")
        send(src.at[pl.ds(I0, HALO), :], dst.at[I1], "s")
    lane = lane_ids()
    for cp in loads2:
        cp.wait()

    for r in range(ROWS // SUB):
        rows = pl.ds(SUB * r, SUB)
        for i in range(I3):
            pk2[i, rows, :] = wide_pack(lane, *[s2[i, m, rows, t] for m in range(MEM) for t in TILES])
        pk2[I3, rows, :] = wide_pack(lane, *[sh[rows, t] for t in TILES], *[sk[rows, t].astype(F32) for t in TILES])
    pair = lax.rem(lane + I1, LANE) // I2

    def pack3(m):
        for cp in loads[m]:
            cp.wait()

        def body(g, carry):
            for j in range(4):
                rows = pl.ds(pl.multiple_of(g * 32 + SUB * j, SUB), SUB)
                acc = jnp.zeros((SUB, LANE), F32)
                for f in range(4):
                    for k in range(LEV):
                        q = f * LEV + k
                        both = jnp.where(lane < 64, big[m, f, k, rows, TILES[I0]], big[m, f, k, rows, TILES[I1]])
                        acc = jnp.where(pair == q, rot(both, I2 * q), acc)
                pk[m, rows, :] = acc
            return carry

        lax.fori_loop(I0, 4, body, I0)
        for f in range(4):
            for t in range(I2):
                for g in range(I2):
                    ks = pl.ds(SUB * g, SUB)
                    rowb[I0, m, f, t, ks, :] = big[m, f, ks, ROWS - I1, TILES[t]]
                    rowb[I1, m, f, t, ks, :] = big[m, f, ks, I0, TILES[t]]

    def send3(m):
        send(pk.at[m], px.at[m], "x")
        send(pk.at[m, pl.ds(ROWS - SUB, SUB), :], pd.at[I0, m], "nx")
        send(pk.at[m, pl.ds(I0, SUB), :], pd.at[I1, m], "sx")
        send(rowb.at[I0, m], hr.at[I0, m], "n")
        send(rowb.at[I1, m], hr.at[I1, m], "s")

    side = send(pk2, hx2, "x")
    pack3(I0)
    send3(I0)
    pack3(I1)
    send3(I1)
    side.wait()
    send(hx2.at[:, pl.ds(ROWS - HALO, HALO), :], hd2.at[I0], "n")
    send(hx2.at[:, pl.ds(I0, HALO), :], hd2.at[I1], "s")
    for cp in sent:
        if cp is not side:
            cp.wait()


def sds(*shape, dtype=F32):
    return jax.ShapeDtypeStruct(shape, dtype)


NSEND_A = 23


def edges_call(u, v, te, sa, eta, tx, ty, dep, kmt):
    return pl.pallas_call(
        edges_kernel,
        name="edges",
        out_shape=(
            sds(MEM, ROWS, LANE), sds(I2, MEM, SUB, LANE), sds(I2, MEM, 4, I2, LEV, LANE),
            sds(4, ROWS, LANE), sds(I2, 4, HALO, LANE),
            sds(I2, MEM, HALO, COLS), sds(I2, MEM, HALO, COLS), sds(I2, MEM, HALO, COLS),
            sds(I2, HALO, COLS), sds(I2, HALO, COLS, dtype=jnp.int32),
        ),
        in_specs=[ANY] * 9,
        out_specs=(ANY,) * 10,
        scratch_shapes=[
            pltpu.VMEM((MEM, 4, LEV, ROWS, COLS), F32),
            pltpu.VMEM((I3, MEM, ROWS, COLS), F32),
            pltpu.VMEM((ROWS, COLS), F32),
            pltpu.VMEM((ROWS, COLS), jnp.int32),
            pltpu.VMEM((MEM, ROWS, LANE), F32),
            pltpu.VMEM((I2, MEM, 4, I2, LEV, LANE), F32),
            pltpu.VMEM((4, ROWS, LANE), F32),
            pltpu.SemaphoreType.DMA((MEM, 4)),
            pltpu.SemaphoreType.DMA((5,)),
            pltpu.SemaphoreType.DMA((NSEND_A,)),
            pltpu.SemaphoreType.DMA((NSEND_A,)),
        ],
        compiler_params=pltpu.CompilerParams(collective_id=I0, has_side_effects=True, vmem_limit_bytes=LIMIT),
    )(u, v, te, sa, eta, tx, ty, dep, kmt)


def columns_kernel(u, v, te, sa, px, pd, hr, dep, kmt, hx2, hrh, hrk, bu, bv, ot, os, sx, sy, nx, ny, us, vs, ts, ss, ps, vel, uwl, sides, stage, pxs, hrs, hs, ki, kf, hks, obu, obv, ost, oss, load_sem, misc_sem, out_sem):
    row = lax.axis_index("row")
    not_south = jnp.where(row == I0, ZERO, ONE).astype(F32)
    not_north = jnp.where(row == NR - I1, ZERO, ONE).astype(F32)
    fields = ((u, us), (v, vs), (te, ts), (sa, ss))

    def load_copies(c):
        rows = pl.ds(pl.multiple_of(CHUNK * c, CHUNK), CHUNK)
        slot = lax.rem(c, SLOTS)
        return [pltpu.make_async_copy(src.at[:, :, rows, :], stage.at[slot, f], load_sem.at[slot, f]) for f, (src, _) in enumerate(fields)]

    def out_copies(c):
        rows = pl.ds(pl.multiple_of(CHUNK * c, CHUNK), CHUNK)
        return [pltpu.make_async_copy(a.at[:, :, rows, :], b.at[:, :, rows, :], out_sem.at[i]) for i, (a, b) in enumerate(((obu, bu), (obv, bv), (ost, ot), (oss, os)))]

    for c in range(NCH - I1, NCH - I1 - SLOTS, -I1):
        for cp in load_copies(jnp.int32(c)):
            cp.start()
    misc = [
        pltpu.make_async_copy(px, pxs.at[:, pl.ds(SUB, ROWS), :], misc_sem.at[I0]),
        pltpu.make_async_copy(pd.at[I0], pxs.at[:, pl.ds(I0, SUB), :], misc_sem.at[I1]),
        pltpu.make_async_copy(pd.at[I1], pxs.at[:, pl.ds(SUB + ROWS, SUB), :], misc_sem.at[I2]),
        pltpu.make_async_copy(hr, hrs, misc_sem.at[I3]),
        pltpu.make_async_copy(hx2.at[I3], hks, misc_sem.at[4]),
    ]
    for t in range(I2):
        cols = pl.ds(LANE * t, LANE)
        misc.append(pltpu.make_async_copy(dep.at[:, cols], hs.at[t, pl.ds(SUB, ROWS), :], misc_sem.at[5 + 4 * t]))
        misc.append(pltpu.make_async_copy(kmt.at[:, cols], ki.at[t, pl.ds(SUB, ROWS), :], misc_sem.at[6 + 4 * t]))
        misc.append(pltpu.make_async_copy(hrh.at[I1, pl.ds(I0, SUB), cols], hs.at[t, pl.ds(SUB + ROWS, SUB), :], misc_sem.at[7 + 4 * t]))
        misc.append(pltpu.make_async_copy(hrk.at[I1, pl.ds(I0, SUB), cols], ki.at[t, pl.ds(SUB + ROWS, SUB), :], misc_sem.at[SUB + 4 * t]))
    for cp in misc:
        cp.start()
    for cp in misc:
        cp.wait()
    lane = lane_ids()
    is_last = lane == LAST
    is_first = lane == I0
    two = range(I2)
    for m in range(MEM):
        pxs[m, I0:SUB, :] = pxs[m, I0:SUB, :] * not_south
        pxs[m, SUB + ROWS:NEXT, :] = pxs[m, SUB + ROWS:NEXT, :] * not_north
        for f, (_, dst) in enumerate(fields):
            for t in two:
                for g in two:
                    ks = pl.ds(SUB * g, SUB)
                    dst[t, ks, m, 7:SUB, :] = (hrs[I0, m, f, t, ks, :] * not_south)[:, None, :]
                    dst[t, ks, m, SUB + ROWS:9 + ROWS, :] = (hrs[I1, m, f, t, ks, :] * not_north)[:, None, :]
    for t in two:
        kf[t, SUB:SUB + ROWS, :] = ki[t, SUB:SUB + ROWS, :].astype(F32)
        kf[t, SUB + ROWS:NEXT, :] = ki[t, SUB + ROWS:NEXT, :].astype(F32) * not_north
    rho_s = PRESS / LEV * HALINE
    rho_t = PRESS / LEV * THERM
    gain, inner, last = solve_factors(DIFF)
    zero = jnp.zeros((SUB, LANE), F32)

    def east(a, b, halo):
        ra, rb = rot(a, LAST), rot(b, LAST)
        return jnp.where(is_last, rb, ra), jnp.where(is_last, halo, rb)

    def push(x, edge, q):
        return [rot(a, LAST) for a in x] + [rot(edge, LAST - I2 * q)], [rot(a, I1) for a in x] + [rot(edge, 129 - I2 * q)]

    def pop_east(east_):
        return jnp.where(is_last, east_[I1], east_[I0]), jnp.where(is_last, east_[I2], east_[I1])

    def pop_west(west_):
        return jnp.where(is_first, west_[I2], west_[I0]), jnp.where(is_first, west_[I0], west_[I1])

    def unpack(r, m, k, edge):
        slot = lax.rem(jnp.maximum(r, I0) // BPC, SLOTS)
        src_rows = pl.ds(pl.multiple_of(SUB * lax.rem(jnp.maximum(r, I0), BPC), SUB), SUB)
        dst_rows = pl.ds(pl.multiple_of(jnp.where(r < I0, NEXT, SUB * r + SUB), SUB), SUB)
        rolled = []
        for f, (_, dst) in enumerate(fields):
            x = [stage[slot, f, k, m, src_rows, TILES[t]] for t in two]
            for t in two:
                dst[t, k, m, dst_rows, :] = x[t]
            rolled.append(push(x, edge, f * LEV + k))
        return rolled

    def settle(r, m, k, rolled):
        dst_rows = pl.ds(pl.multiple_of(jnp.where(r < I0, NEXT, SUB * r + SUB), SUB), SUB)
        ring = lax.rem(r + I2, I2)
        for f in range(4):
            east_, west_ = pop_east(rolled[f][I0]), pop_west(rolled[f][I1])
            for t in two:
                if f == I0:
                    sides[I0, ring, t, k, m, :, :] = east_[t]
                    uwl[t, k, m, dst_rows, :] = west_[t]
                elif f == I1:
                    vel[t, k, m, dst_rows, :] = east_[t]
                    sides[I1, ring, t, k, m, :, :] = west_[t]
                else:
                    sides[I2 * f - I2, ring, t, k, m, :, :] = east_[t]
                    sides[I2 * f - I1, ring, t, k, m, :, :] = west_[t]

    def prime(m, carry):
        south, north, first = pl.ds(I0, SUB), pl.ds(SUB + ROWS, SUB), pl.ds(ROWS, SUB)
        below = [zero, zero]
        for k in range(LEV):
            settle(jnp.int32(ROWS // SUB - I1), m, k, unpack(jnp.int32(ROWS // SUB - I1), m, k, pxs[m, first, :]))
            v_side = push([vs[t, k, m, south, :] for t in two], pxs[m, south, :], LEV + k)[I0]
            u_side = push([us[t, k, m, north, :] for t in two], pxs[m, north, :], k)[I1]
            for t, x in enumerate(pop_east(v_side)):
                vel[t, k, m, south, :] = x
            for t, x in enumerate(pop_west(u_side)):
                uwl[t, k, m, north, :] = x
            for t in two:
                half = (HALF * rho_s) * ss[t, k, m, north, :] - (HALF * rho_t) * ts[t, k, m, north, :]
                ps[t, k, m, north, :] = below[t] + half
                below[t] = (below[t] + half) + half
        return carry

    def block(r):
        y = pl.multiple_of(r * SUB + SUB, SUB)
        rows = pl.ds(y, SUB)
        up = pl.ds(y + I1, SUB)
        down = pl.ds(y - I1, SUB)
        south = pl.ds(y - SUB, SUB)
        out_rows = pl.ds(pl.multiple_of(r * SUB, SUB), SUB)
        kc = [kf[t, rows, :] for t in two]
        hk = hks[out_rows, :]
        ke = east(kc[I0], kc[I1], rot(hk, 63))
        hc = [hs[t, rows, :] for t in two]
        he = east(hc[I0], hc[I1], rot(hk, LAST))
        kx = [jnp.minimum(kc[t], ke[t]) for t in two]
        ky = [jnp.minimum(kc[t], kf[t, up, :]) for t in two]
        scale_x, scale_y = [], []
        for t in two:
            nx[out_rows, TILES[t]] = kx[t]
            ny[out_rows, TILES[t]] = ky[t]
            scale_x.append(jnp.where(kx[t] > ZERO, HALF * (hc[t] + he[t]), ZERO) / (jnp.maximum(kx[t], ONE) * NSUB))
            scale_y.append(jnp.where(ky[t] > ZERO, HALF * (hc[t] + hs[t, up, :]), ZERO) / (jnp.maximum(ky[t], ONE) * NSUB))

        ring = lax.rem(r, I2)

        def member(m, carry):
            edge = pxs[m, south, :]
            below = [zero] * 4
            sum_x = [zero, zero]
            sum_y = [zero, zero]
            run_t = [None, None]
            run_s = [None, None]
            waiting = []
            for ahead in range(LEV + DEPTH):
                if ahead < LEV:
                    waiting.append(unpack(r - I1, m, ahead, edge))
                k = ahead - DEPTH
                if k < I0:
                    continue
                settle(r - I1, m, k, waiting.pop(I0))
                for t in two:
                    uc, un, ud = us[t, k, m, rows, :], us[t, k, m, up, :], us[t, k, m, down, :]
                    vc, vn, vd = vs[t, k, m, rows, :], vs[t, k, m, up, :], vs[t, k, m, down, :]
                    tc, sc = ts[t, k, m, rows, :], ss[t, k, m, rows, :]
                    ue, vw, t_e, t_w, s_e, s_w = [sides[i, ring, t, k, m, :, :] for i in range(6)]
                    uw, ve = uwl[t, k, m, rows, :], vel[t, k, m, rows, :]
                    half = (HALF * rho_s) * sc - (HALF * rho_t) * tc
                    press = below[t] + half
                    below[t] = press + half
                    half = (HALF * rho_s) * s_e - (HALF * rho_t) * t_e
                    press_e = below[I2 + t] + half
                    below[I2 + t] = press_e + half
                    ps[t, k, m, rows, :] = press
                    uh, vh, vdh, uwh = HALF * uc, HALF * vc, HALF * vd, HALF * uw
                    vq = (vc + vd) + (ve + vel[t, k, m, down, :])
                    uq = (uc + un) + (uw + uwl[t, k, m, up, :])
                    gu = (press - press_e) - uh * (ue - uw) - 0.125 * (vq * (un - ud))
                    gu = jnp.where(kx[t] > float(k), gu, ZERO)
                    sum_x[t] = sum_x[t] + gu
                    obu[k, m, out_rows, TILES[t]] = uc + gu
                    gv = (press - ps[t, k, m, up, :]) - 0.125 * (uq * (ve - vw)) - vh * (vn - vd)
                    gv = jnp.where(ky[t] > float(k), gv, ZERO)
                    sum_y[t] = sum_y[t] + gv
                    obv[k, m, out_rows, TILES[t]] = vc + gv
                    wet = kc[t] > float(k)
                    for scr, cen, e, w, run, dst in ((ts, tc, t_e, t_w, run_t, ost), (ss, sc, s_e, s_w, run_s, oss)):
                        fx = uh * (cen + e) - uwh * (w + cen)
                        fy = vh * (cen + scr[t, k, m, up, :]) - vdh * (scr[t, k, m, down, :] + cen)
                        new = jnp.where(wet, cen - (fx + fy), ZERO)
                        run[t] = new if k == I0 else new + gain[k - I1] * run[t]
                        dst[k, m, out_rows, TILES[t]] = run[t]
            for t in two:
                sx[m, out_rows, TILES[t]] = scale_x[t] * sum_x[t]
                sy[m, out_rows, TILES[t]] = scale_y[t] * sum_y[t]
                nt = ns = zero
                for k in range(LEV - I1, -I1, -I1):
                    coef = level_factor(kc[t], k, inner, last)
                    nt = coef * ost[k, m, out_rows, TILES[t]] + gain[k] * nt
                    ns = coef * oss[k, m, out_rows, TILES[t]] + gain[k] * ns
                    ost[k, m, out_rows, TILES[t]] = nt
                    oss[k, m, out_rows, TILES[t]] = ns
            return carry

        lax.fori_loop(I0, MEM, member, I0)

    for cp in load_copies(jnp.int32(NCH - I1)):
        cp.wait()
    lax.fori_loop(I0, MEM, prime, I0)

    def step(i, carry):
        r = ROWS // SUB - I1 - i
        c = r // BPC
        edge = lax.rem(r, BPC) == I0

        @pl.when(edge & (c >= I1))
        def _():
            for cp in load_copies(c - I1):
                cp.wait()

        @pl.when(edge & (c >= SLOTS))
        def _():
            for cp in load_copies(c - SLOTS):
                cp.start()

        @pl.when(edge & (c + I1 < NCH))
        def _():
            for cp in out_copies(c + I1):
                cp.start()

        block(r)
        return carry

    lax.fori_loop(I0, ROWS // SUB, step, I0)
    for cp in out_copies(jnp.int32(I0)):
        cp.start()
    for c in range(NCH):
        for cp in out_copies(jnp.int32(c)):
            cp.wait()


def columns_call(u, v, te, sa, px, pd, hr, dep, kmt, hx2, hrh, hrk):
    big = pltpu.VMEM((I2, LEV, MEM, EXT, LANE), F32)
    full = pltpu.VMEM((LEV, MEM, ROWS, COLS), F32)
    o3 = sds(LEV, MEM, ROWS, COLS)
    o2 = sds(MEM, ROWS, COLS)
    o1 = sds(ROWS, COLS)
    return pl.pallas_call(
        columns_kernel,
        name="columns",
        out_shape=(o3, o3, o3, o3, o2, o2, o1, o1),
        in_specs=[ANY] * 12,
        out_specs=(ANY,) * 4 + (VM,) * 4,
        scratch_shapes=[big] * 7
        + [
            pltpu.VMEM((6, I2, I2, LEV, MEM, SUB, LANE), F32),
            pltpu.VMEM((SLOTS, 4, LEV, MEM, CHUNK, COLS), F32),
            pltpu.VMEM((MEM, NEXT, LANE), F32),
            pltpu.VMEM((I2, MEM, 4, I2, LEV, LANE), F32),
            pltpu.VMEM((I2, NEXT, LANE), F32),
            pltpu.VMEM((I2, NEXT, LANE), jnp.int32),
            pltpu.VMEM((I2, NEXT, LANE), F32),
            pltpu.VMEM((ROWS, LANE), F32),
            full, full, full, full,
            pltpu.SemaphoreType.DMA((SLOTS, 4)),
            pltpu.SemaphoreType.DMA((13,)),
            pltpu.SemaphoreType.DMA((4,)),
        ],
        compiler_params=pltpu.CompilerParams(vmem_limit_bytes=LIMIT),
    )(u, v, te, sa, px, pd, hr, dep, kmt, hx2, hrh, hrk)


def forcing_kernel(sx, sy, hxs, hds, hrx, hry, pk, send_sem, recv_sem):
    ids = neighbours()
    enter(ids)
    lane = lane_ids()
    sent = []

    def send(src, dst, who):
        i = len(sent)
        cp = pltpu.make_async_remote_copy(src_ref=src, dst_ref=dst, send_sem=send_sem.at[i], recv_sem=recv_sem.at[i], device_id=ids[who], device_id_type=MESH)
        cp.start()
        sent.append(cp)

    for r in range(ROWS // SUB):
        rows = pl.ds(SUB * r, SUB)
        for i, a in enumerate((sx, sy)):
            pk[i, rows, :] = wide_pack(lane, *[a[m, rows, t] for m in range(MEM) for t in TILES])
    for src, dst in ((sx, hrx), (sy, hry)):
        send(src.at[:, pl.ds(ROWS - HALO, HALO), :], dst.at[I0], "n")
        send(src.at[:, pl.ds(I0, HALO), :], dst.at[I1], "s")
    send(pk, hxs, "x")
    send(pk.at[:, pl.ds(ROWS - HALO, HALO), :], hds.at[I0], "nx")
    send(pk.at[:, pl.ds(I0, HALO), :], hds.at[I1], "sx")
    for cp in sent:
        cp.wait()


def forcing_call(sx, sy):
    return pl.pallas_call(
        forcing_kernel,
        name="forcing",
        out_shape=(sds(I2, ROWS, LANE), sds(I2, I2, HALO, LANE), sds(I2, MEM, HALO, COLS), sds(I2, MEM, HALO, COLS)),
        in_specs=[VM, VM],
        out_specs=(ANY,) * 4,
        scratch_shapes=[pltpu.VMEM((I2, ROWS, LANE), F32), pltpu.SemaphoreType.DMA((7,)), pltpu.SemaphoreType.DMA((7,))],
        compiler_params=pltpu.CompilerParams(collective_id=I1, has_side_effects=True, vmem_limit_bytes=LIMIT),
    )(sx, sy)


def turn_east(x):
    return [rot(a, LAST) for a in x] + [rot(x[I2], 63), rot(x[4], 63)]


def pick_east(r, lane):
    last = lane == LAST
    far = jnp.where(lane == 63, r[5], r[4])
    return [jnp.where(last, r[I1], r[I0]), jnp.where(last, r[4], r[I1]), jnp.where(last, r[I3], r[I2]), jnp.where(last, r[6], r[I3]), jnp.where(last, r[I0], far)]


def turn_west(x):
    return [rot(a, I1) for a in x] + [rot(x[I3], 65), rot(x[4], 65)]


def pick_west(r, lane):
    first = lane == I0
    far = jnp.where(lane == 64, r[5], r[4])
    return [jnp.where(first, r[4], r[I0]), jnp.where(first, r[I0], r[I1]), jnp.where(first, r[6], r[I2]), jnp.where(first, r[I2], r[I3]), jnp.where(first, r[I1], far)]


def turn_east3(x):
    return [rot(a, LAST) for a in x] + [rot(x[I0], 63)]


def pick_east3(r, lane):
    last = lane == LAST
    far = jnp.where(lane == 63, r[I3], r[I2])
    return [jnp.where(last, r[I1], r[I0]), jnp.where(last, r[I2], r[I1]), jnp.where(last, r[I0], far)]


def turn_west3(x):
    return [rot(a, I1) for a in x] + [rot(x[I1], 65)]


def pick_west3(r, lane):
    first = lane == I0
    far = jnp.where(lane == 64, r[I3], r[I2])
    return [jnp.where(first, r[I2], r[I0]), jnp.where(first, r[I0], r[I1]), jnp.where(first, r[I1], far)]


def staged(items, issue, finish, depth):
    queue = []
    for item in items:
        queue.append((item, issue(item)))
        if len(queue) > depth:
            finish(*queue.pop(I0))
    for item, value in queue:
        finish(item, value)


SHARED = (I0, I1, I0, I1, I2)


def subcycle_kernel(weights, eta, tx, ty, sx, sy, dep, kmt, hx2, hd2, hre, hrx, hry, hrh, hrk, hxs, hds, hrsx, hrsy, eta_out, tx_out, ty_out, cx_out, cy_out, nat, side, hn, kn, e0, e1, t1, t2, f1, f2, hh, kf, gx, gy, gxw, gc, wv, fo, acc1, acc2, ee, ew, tails, sem):
    row = lax.axis_index("row")
    not_south = jnp.where(row == I0, ZERO, ONE).astype(F32)
    not_north = jnp.where(row == NR - I1, ZERO, ONE).astype(F32)
    lane = lane_ids()
    base = SUB + HALO
    top = base + ROWS
    low, mid, high = pl.ds(I0, HALO), pl.ds(HALO, ROWS), pl.ds(HALO + ROWS, HALO)
    copies = []

    def fetch(src, dst):
        copies.append(pltpu.make_async_copy(src, dst, sem))

    for i, (own_, rows_) in enumerate(((eta, hre), (tx, hrx), (ty, hry), (sx, hrsx), (sy, hrsy))):
        fetch(own_, nat.at[i, :, mid, :])
        fetch(rows_.at[I0], nat.at[i, :, low, :])
        fetch(rows_.at[I1], nat.at[i, :, high, :])
    for first, count, main, corner in ((I0, 4, hx2, hd2), (4, I2, hxs, hds)):
        part = pl.ds(first, count)
        fetch(main, side.at[part, mid, :])
        fetch(corner.at[I0], side.at[part, low, :])
        fetch(corner.at[I1], side.at[part, high, :])
    for own_, rows_, dst in ((dep, hrh, hn), (kmt, hrk, kn)):
        fetch(own_, dst.at[mid, :])
        fetch(rows_.at[I0], dst.at[low, :])
        fetch(rows_.at[I1], dst.at[high, :])
    for cp in copies:
        cp.start()
    total = jnp.float32(ZERO)
    moment = jnp.float32(ZERO)
    for n in range(NSUB - I1, -I1, -I1):
        total = total + weights[n]
        moment = moment + total
        tails[n] = total
    for cp in copies:
        cp.wait()
    own = (lane < 32) | (lane >= 96)
    zero = jnp.zeros((SUB, LANE), F32)
    three, five = range(I3), range(5)
    for i in three:
        kf[i, I0:SUB, :] = zero
        kf[i, SUB + NEAR:BEXT, :] = zero
    everything = range(I1, I1 + NEAR // SUB)

    def rows_of(r):
        return pl.ds(SUB * r, SUB), pl.ds(SUB * r + I1, SUB), pl.ds(SUB * r - I1, SUB), pl.ds(SUB * r - SUB, SUB)

    def level_issue(r):
        here = rows_of(r)[I3]
        packed = side[I3, here, :]
        return packed, rot(packed, 64)

    def level_finish(r, value):
        packed, turned = value
        rows, _, _, here = rows_of(r)
        levels = [kn[here, t].astype(F32) for t in TILES] + [jnp.where(own, turned, packed)]
        depths = [hn[here, t] for t in TILES] + [jnp.where(own, packed, turned)]
        keep = not_south if r < base // SUB else not_north
        inside = base // SUB <= r < top // SUB
        for i in three:
            kf[i, rows, :] = levels[i] if inside else levels[i] * keep
            hh[i, rows, :] = depths[i]

    staged(everything, level_issue, level_finish, SUB)

    def mask_issue(r):
        rows = rows_of(r)[I0]
        kc = [kf[i, rows, :] for i in three]
        hc = [hh[i, rows, :] for i in three]
        return kc, hc, turn_east3(kc), turn_east3(hc)

    def mask_finish(r, value):
        kc, hc, kt, ht = value
        rows, up, down, here = rows_of(r)
        ke, he = pick_east3(kt, lane), pick_east3(ht, lane)
        wet = [kc[i] > ZERO for i in three]
        wet_x = [jnp.minimum(kc[i], ke[i]) > ZERO for i in three]
        wet_y = [jnp.minimum(kc[i], kf[i, up, :]) > ZERO for i in three]
        for i in three:
            gx[i, rows, :] = jnp.where(wet_x[i], (HALF * WAVE * WAVE) * (hc[i] + he[i]), ZERO)
            gy[i, rows, :] = jnp.where(wet_y[i], (HALF * WAVE * WAVE) * (hc[i] + hh[i, up, :]), ZERO)
        for f, mask, dst in ((I0, wet, e0), (I1, wet_x, t1), (I2, wet_y, t2), (I3, wet_x, f1), (4, wet_y, f2)):
            slot = f if f < I3 else f + I1
            raw = [nat[f, m, here, t] for m in range(MEM) for t in TILES] + [side[slot, here, :]]
            for i in five:
                dst[i, rows, :] = jnp.where(mask[SHARED[i]], raw[i], ZERO)

    staged(everything, mask_issue, mask_finish, I3)

    def start_issue(r):
        rows = rows_of(r)[I0]
        a = [t1[i, rows, :] for i in five]
        c = [f1[i, rows, :] for i in five]
        return a, c, turn_west(a), turn_west(c), turn_west3([gx[i, rows, :] for i in three])

    late = []

    def start_finish(r, value):
        a, c, at, ct, gt = value
        rows, up, down, here = rows_of(r)
        aw, cw, gw = pick_west(at, lane), pick_west(ct, lane), pick_west3(gt, lane)
        for i in three:
            gxw[i, rows, :] = gw[i]
            gc[i, rows, :] = (gx[i, rows, :] + gw[i]) + (gy[i, rows, :] + gy[i, down, :])
        fresh = []
        for i in five:
            w = -WAVE * ((a[i] - aw[i]) + (t2[i, rows, :] - t2[i, down, :]))
            fo[i, rows, :] = -WAVE * ((c[i] - cw[i]) + (f2[i, rows, :] - f2[i, down, :]))
            now = e0[i, rows, :] + w
            wv[i, rows, :] = w
            e0[i, rows, :] = now
            acc1[i, rows, :] = weights[I0] * now
            acc2[i, rows, :] = tails[I0] * now
            fresh.append(now)
        late.append((r, turn_east(fresh), turn_west(fresh)))
        if len(late) > I3:
            store_sides(*late.pop(I0), I0)

    def store_sides(r, et, wt, buf):
        rows = rows_of(r)[I0]
        ne, nw = pick_east(et, lane), pick_west(wt, lane)
        for i in five:
            ee[buf, i, rows, :] = ne[i]
            ew[buf, i, rows, :] = nw[i]

    staged(everything, start_issue, start_finish, I3)
    for item in late:
        store_sides(*item, I0)

    def advance(src, buf, dst, r, plan):
        rows, up, down, _ = rows_of(r)
        gxc, gxm, gyc, gyd, gcc = [[g[i, rows_, :] for i in three] for g, rows_ in ((gx, rows), (gxw, rows), (gy, rows), (gy, down), (gc, rows))]
        fresh = []
        for i in five:
            j = SHARED[i]
            now = src[i, rows, :]
            w = (wv[i, rows, :] + fo[i, rows, :]) - gcc[j] * now
            w = w + ((gxc[j] * ee[buf, i, rows, :] + gxm[j] * ew[buf, i, rows, :]) + (gyc[j] * src[i, up, :] + gyd[j] * src[i, down, :]))
            new = now + w
            wv[i, rows, :] = w
            dst[i, rows, :] = new
            fresh.append(new)
            if plan is not None:
                prev, a0, b0, a1, b1 = plan
                s1, s2 = acc1[i, rows, :], acc2[i, rows, :]
                if prev:
                    s1 = s1 + a0 * now
                    s2 = s2 + b0 * now
                acc1[i, rows, :] = s1 + a1 * new
                acc2[i, rows, :] = s2 + b1 * new
        return turn_east(fresh), turn_west(fresh)

    def sweep(src, buf, dst, lo, hi, plan, depth=I3):
        def issue(r):
            return advance(src, buf, dst, r, plan if base // SUB <= r <= top // SUB else None)

        def finish(r, value):
            store_sides(r, *value, I1 - buf)

        staged(range(lo, hi), issue, finish, depth)

    for begin, end in ((I0, I2), (I2, 6), (6, 10), (10, 14)):
        lo = (I2 * begin + 12) // SUB
        hi = (196 - I2 * begin) // SUB + I1

        def pair(i, carry):
            m = I2 * i + I2
            sweep(e0, I0, e1, lo, hi, None)
            sweep(e1, I1, e0, lo, hi, (True, weights[m - I1], tails[m - I1], weights[m], tails[m]))
            return carry

        lax.fori_loop(begin, end, pair, I0)
    sweep(e0, I0, e1, base // SUB, top // SUB + I1, (False, None, None, weights[NSUB - I1], tails[NSUB - I1]))

    def end_issue(r):
        rows = rows_of(r)[I0]
        s = [acc2[i, rows, :] for i in five]
        return s, turn_east(s)

    def end_finish(r, value):
        s, st = value
        rows, up, _, _ = rows_of(r)
        out_rows = pl.ds(SUB * r - base, SUB)
        se = pick_east(st, lane)
        for m in range(MEM):
            for t in range(I2):
                i = I2 * m + t
                cols = TILES[t]
                eta_out[m, out_rows, cols] = acc1[i, rows, :]
                gxc, gyc = gx[t, rows, :], gy[t, rows, :]
                ux = total * t1[i, rows, :] + moment * f1[i, rows, :] - (ONE / WAVE) * (gxc * (se[i] - s[i]))
                uy = total * t2[i, rows, :] + moment * f2[i, rows, :] - (ONE / WAVE) * (gyc * (acc2[i, up, :] - s[i]))
                tx_out[m, out_rows, cols] = ux
                ty_out[m, out_rows, cols] = uy
                cx_out[m, out_rows, cols] = ux / jnp.where(gxc > ZERO, gxc * (ONE / (WAVE * WAVE)), ONE)
                cy_out[m, out_rows, cols] = uy / jnp.where(gyc > ZERO, gyc * (ONE / (WAVE * WAVE)), ONE)

    staged(range(base // SUB, top // SUB), end_issue, end_finish, I3)


def subcycle_call(weights, *arrays):
    o2 = sds(MEM, ROWS, COLS)
    five = pltpu.VMEM((5, BEXT, LANE), F32)
    three = pltpu.VMEM((I3, BEXT, LANE), F32)
    return pl.pallas_call(
        subcycle_kernel,
        name="subcycle",
        out_shape=(o2,) * 5,
        in_specs=[SM] + [ANY] * len(arrays),
        out_specs=(VM,) * 5,
        scratch_shapes=[
            pltpu.VMEM((5, MEM, NEAR, COLS), F32),
            pltpu.VMEM((6, NEAR, LANE), F32),
            pltpu.VMEM((NEAR, COLS), F32),
            pltpu.VMEM((NEAR, COLS), jnp.int32),
            *[five] * 6, *[three] * 6, *[five] * 4, pltpu.VMEM((I2, 5, BEXT, LANE), F32), pltpu.VMEM((I2, 5, BEXT, LANE), F32),
            pltpu.SMEM((NSUB,), F32),
            pltpu.SemaphoreType.DMA,
        ],
        compiler_params=pltpu.CompilerParams(vmem_limit_bytes=LIMIT),
    )(weights, *arrays)


DROWS = 16


def correct_kernel(bu, bv, nx, ny, cx, cy, ou, ov):
    gain, inner, last = solve_factors(VISC)

    def body(j, carry):
        rows = pl.ds(pl.multiple_of(j * SUB, SUB), SUB)
        for src, cnt, shift, dst in ((bu, nx, cx, ou), (bv, ny, cy, ov)):
            for cols in TILES:
                n = cnt[rows, cols]
                run = []
                for k in range(LEV):
                    b = [src[k, m, rows, cols] for m in range(MEM)]
                    run.append(b if k == I0 else [b[m] + gain[k - I1] * run[-I1][m] for m in range(MEM)])
                nxt = [jnp.zeros((SUB, LANE), F32)] * MEM
                tot = list(nxt)
                sol = [None] * LEV
                for k in range(LEV - I1, -I1, -I1):
                    coef = level_factor(n, k, inner, last)
                    nxt = [coef * run[k][m] + gain[k] * nxt[m] for m in range(MEM)]
                    tot = [tot[m] + nxt[m] for m in range(MEM)]
                    sol[k] = nxt
                share = ONE / jnp.maximum(n, ONE)
                add = [shift[m, rows, cols] - tot[m] * share for m in range(MEM)]
                for k in range(LEV):
                    wet = n > float(k)
                    for m in range(MEM):
                        dst[k, m, rows, cols] = jnp.where(wet, sol[k][m] + add[m], ZERO)
        return carry

    lax.fori_loop(I0, DROWS // SUB, body, I0)


def correct_call(bu, bv, nx, ny, cx, cy):
    s3 = pl.BlockSpec((LEV, MEM, DROWS, COLS), lambda r: (I0, I0, r, I0))
    s2 = pl.BlockSpec((MEM, DROWS, COLS), lambda r: (I0, r, I0))
    s1 = pl.BlockSpec((DROWS, COLS), lambda r: (r, I0))
    o3 = sds(LEV, MEM, ROWS, COLS)
    return pl.pallas_call(
        correct_kernel,
        name="correct",
        grid=(ROWS // DROWS,),
        out_shape=(o3, o3),
        in_specs=[s3, s3, s1, s1, s2, s2],
        out_specs=(s3, s3),
        compiler_params=pltpu.CompilerParams(vmem_limit_bytes=LIMIT),
    )(bu, bv, nx, ny, cx, cy)


def local_step(u, v, te, sa, eta, tx, ty, dep, kmt, weights):
    px, pd, hr, hx2, hd2, hre, hrx, hry, hrh, hrk = edges_call(u, v, te, sa, eta, tx, ty, dep, kmt)
    bu, bv, ot, os, sx, sy, nx, ny = columns_call(u, v, te, sa, px, pd, hr, dep, kmt, hx2, hrh, hrk)
    hxs, hds, hrsx, hrsy = forcing_call(sx, sy)
    eta_new, tx_new, ty_new, cx, cy = subcycle_call(weights, eta, tx, ty, sx, sy, dep, kmt, hx2, hd2, hre, hrx, hry, hrh, hrk, hxs, hds, hrsx, hrsy)
    ou, ov = correct_call(bu, bv, nx, ny, cx, cy)
    return eta_new, tx_new, ty_new, ou, ov, ot, os


def solution(mesh):
    s3 = P(None, None, "row", "col")
    s2 = P(None, "row", "col")
    s1 = P("row", "col")
    return jax.shard_map(local_step, mesh=mesh, in_specs=(s3, s3, s3, s3, s2, s2, s2, s1, s1, P()), out_specs=(s2, s2, s2, s3, s3, s3, s3), check_vma=False)
```

```python
import functools
import jax
import jax.numpy as jnp
from jax import lax
from jax.experimental import pallas as pl
from jax.experimental.pallas import tpu as pltpu
from jax.sharding import PartitionSpec as P

SUB = 8
LANE = 128
LAST = 127
ZERO = 0.0
ONE = 1.0
HALF = 0.5
I0, I1, I2, I3 = range(4)
WAVE = 0.4
THERM = 0.2
HALINE = 0.15
PRESS = HALF
VISC = ONE
DIFF = HALF
LEV = 16
MEM = I2
NSUB = 30
ROWS = LANE
COLS = 256
NR = SUB
NC = I2
HALO = 32
NEXT = 144
EXT = 152
BEXT = 208
NEAR = 192
F32 = jnp.float32
CHUNK = 16
NCH = ROWS // CHUNK
SLOTS = I3
BPC = CHUNK // SUB
DEPTH = I2
MESH = pl.DeviceIdType.MESH
LIMIT = 67043328
TILES = (slice(I0, LANE), slice(LANE, 256))
ANY = pl.BlockSpec(memory_space=pl.ANY)
VM = pl.BlockSpec(memory_space=pltpu.VMEM)
SM = pl.BlockSpec(memory_space=pltpu.SMEM)


def solve_factors(strength):
    gain, inner, last = [], [], []
    prev = None
    for k in range(LEV):
        if k == I0:
            diag, edge = ONE + strength, ONE
        else:
            diag, edge = ONE + 2.0 * strength - strength * prev, ONE + strength - strength * prev
        inner.append(ONE / diag)
        last.append(ONE / edge)
        prev = strength / diag
        gain.append(prev)
    return gain, inner, last


def level_factor(count, k, inner, last):
    edge = jnp.where(count > float(k), last[k], ZERO)
    return edge if k == LEV - I1 else jnp.where(count > float(k + I1), inner[k], edge)


def lane_ids():
    return lax.broadcasted_iota(jnp.int32, (SUB, LANE), I1)


def rot(x, shift):
    shift %= LANE
    return x if shift == I0 else pltpu.roll(x, shift, I1)


def neighbours():
    col = lax.axis_index("col")
    row = lax.axis_index("row")
    other = I1 - col
    north = lax.rem(row + I1, NR)
    south = lax.rem(row + NR - I1, NR)
    return {"x": (other, row), "n": (col, north), "s": (col, south), "nx": (other, north), "sx": (other, south)}


def enter(ids):
    barrier = pltpu.get_barrier_semaphore()
    for target in ids.values():
        pl.semaphore_signal(barrier, inc=I1, device_id=target, device_id_type=MESH)
    pl.semaphore_wait(barrier, len(ids))


def wide_pack(lane, m0t0, m0t1, m1t0, m1t1):
    first = jnp.where(lane < 64, m0t0, m0t1)
    second = jnp.where(lane < 64, m1t0, m1t1)
    return jnp.where((lane < 32) | (lane >= 96), first, rot(second, 64))


def edges_kernel(u, v, te, sa, eta, tx, ty, dep, kmt, px, pd, hr, hx2, hd2, hre, hrx, hry, hrh, hrk, big, s2, sh, sk, pk, rowb, pk2, load_sem, load2_sem, send_sem, recv_sem):
    ids = neighbours()
    fields = (u, v, te, sa)
    loads = []
    for m in range(MEM):
        loads.append([pltpu.make_async_copy(fields[f].at[:, m], big.at[m, f], load_sem.at[m, f]) for f in range(4)])
    loads2 = [pltpu.make_async_copy(a, s2.at[i], load2_sem.at[i]) for i, a in enumerate((eta, tx, ty))]
    loads2.append(pltpu.make_async_copy(dep, sh, load2_sem.at[I3]))
    loads2.append(pltpu.make_async_copy(kmt, sk, load2_sem.at[4]))
    for cp in loads2:
        cp.start()
    for cp in loads[I0] + loads[I1]:
        cp.start()
    enter(ids)
    sent = []

    def send(src, dst, who):
        i = len(sent)
        cp = pltpu.make_async_remote_copy(src_ref=src, dst_ref=dst, send_sem=send_sem.at[i], recv_sem=recv_sem.at[i], device_id=ids[who], device_id_type=MESH)
        cp.start()
        sent.append(cp)
        return cp

    lane = lane_ids()
    for cp in loads2:
        cp.wait()
    for src, dst in ((s2.at[I0], hre), (s2.at[I1], hrx), (s2.at[I2], hry)):
        send(src.at[:, pl.ds(ROWS - HALO, HALO), :], dst.at[I0], "n")
        send(src.at[:, pl.ds(I0, HALO), :], dst.at[I1], "s")
    for src, dst in ((sh, hrh), (sk, hrk)):
        send(src.at[pl.ds(ROWS - HALO, HALO), :], dst.at[I0], "n")
        send(src.at[pl.ds(I0, HALO), :], dst.at[I1], "s")

    for r in range(ROWS // SUB):
        rows = pl.ds(SUB * r, SUB)
        for i in range(I3):
            pk2[i, rows, :] = wide_pack(lane, *[s2[i, m, rows, t] for m in range(MEM) for t in TILES])
        pk2[I3, rows, :] = wide_pack(lane, *[sh[rows, t] for t in TILES], *[sk[rows, t].astype(F32) for t in TILES])
    pair = lax.rem(lane + I1, LANE) // I2

    def pack3(m):
        for cp in loads[m]:
            cp.wait()

        def body(g, carry):
            for j in range(4):
                rows = pl.ds(pl.multiple_of(g * 32 + SUB * j, SUB), SUB)
                acc = jnp.zeros((SUB, LANE), F32)
                for f in range(4):
                    for k in range(LEV):
                        q = f * LEV + k
                        both = jnp.where(lane < 64, big[m, f, k, rows, TILES[I0]], big[m, f, k, rows, TILES[I1]])
                        acc = jnp.where(pair == q, rot(both, I2 * q), acc)
                pk[m, rows, :] = acc
            return carry

        lax.fori_loop(I0, 4, body, I0)
        for f in range(4):
            for t in range(I2):
                for g in range(I2):
                    ks = pl.ds(SUB * g, SUB)
                    rowb[I0, m, f, t, ks, :] = big[m, f, ks, ROWS - I1, TILES[t]]
                    rowb[I1, m, f, t, ks, :] = big[m, f, ks, I0, TILES[t]]

    def send3(m):
        send(pk.at[m], px.at[m], "x")
        send(pk.at[m, pl.ds(ROWS - SUB, SUB), :], pd.at[I0, m], "nx")
        send(pk.at[m, pl.ds(I0, SUB), :], pd.at[I1, m], "sx")
        send(rowb.at[I0, m], hr.at[I0, m], "n")
        send(rowb.at[I1, m], hr.at[I1, m], "s")

    side = send(pk2, hx2, "x")
    pack3(I0)
    send3(I0)
    pack3(I1)
    send3(I1)
    side.wait()
    send(hx2.at[:, pl.ds(ROWS - HALO, HALO), :], hd2.at[I0], "n")
    send(hx2.at[:, pl.ds(I0, HALO), :], hd2.at[I1], "s")
    for cp in sent:
        if cp is not side:
            cp.wait()


def sds(*shape, dtype=F32):
    return jax.ShapeDtypeStruct(shape, dtype)


NSEND_A = 23


def edges_call(u, v, te, sa, eta, tx, ty, dep, kmt):
    return pl.pallas_call(
        edges_kernel,
        name="edges",
        out_shape=(
            sds(MEM, ROWS, LANE), sds(I2, MEM, SUB, LANE), sds(I2, MEM, 4, I2, LEV, LANE),
            sds(4, ROWS, LANE), sds(I2, 4, HALO, LANE),
            sds(I2, MEM, HALO, COLS), sds(I2, MEM, HALO, COLS), sds(I2, MEM, HALO, COLS),
            sds(I2, HALO, COLS), sds(I2, HALO, COLS, dtype=jnp.int32),
        ),
        in_specs=[ANY] * 9,
        out_specs=(ANY,) * 10,
        scratch_shapes=[
            pltpu.VMEM((MEM, 4, LEV, ROWS, COLS), F32),
            pltpu.VMEM((I3, MEM, ROWS, COLS), F32),
            pltpu.VMEM((ROWS, COLS), F32),
            pltpu.VMEM((ROWS, COLS), jnp.int32),
            pltpu.VMEM((MEM, ROWS, LANE), F32),
            pltpu.VMEM((I2, MEM, 4, I2, LEV, LANE), F32),
            pltpu.VMEM((4, ROWS, LANE), F32),
            pltpu.SemaphoreType.DMA((MEM, 4)),
            pltpu.SemaphoreType.DMA((5,)),
            pltpu.SemaphoreType.DMA((NSEND_A,)),
            pltpu.SemaphoreType.DMA((NSEND_A,)),
        ],
        compiler_params=pltpu.CompilerParams(collective_id=I0, has_side_effects=True, vmem_limit_bytes=LIMIT),
    )(u, v, te, sa, eta, tx, ty, dep, kmt)


def columns_kernel(u, v, te, sa, px, pd, hr, dep, kmt, hx2, hrh, hrk, bu, bv, ot, os, sx, sy, nx, ny, us, vs, ts, ss, ps, vel, uwl, sides, stage, pxs, hrs, hs, ki, kf, hks, obu, obv, ost, oss, load_sem, misc_sem, out_sem):
    row = lax.axis_index("row")
    not_south = jnp.where(row == I0, ZERO, ONE).astype(F32)
    not_north = jnp.where(row == NR - I1, ZERO, ONE).astype(F32)
    fields = ((u, us), (v, vs), (te, ts), (sa, ss))

    def load_copies(c):
        rows = pl.ds(pl.multiple_of(CHUNK * c, CHUNK), CHUNK)
        slot = lax.rem(c, SLOTS)
        return [pltpu.make_async_copy(src.at[:, :, rows, :], stage.at[slot, f], load_sem.at[slot, f]) for f, (src, _) in enumerate(fields)]

    def out_copies(c):
        rows = pl.ds(pl.multiple_of(CHUNK * c, CHUNK), CHUNK)
        return [pltpu.make_async_copy(a.at[:, :, rows, :], b.at[:, :, rows, :], out_sem.at[i]) for i, (a, b) in enumerate(((obu, bu), (obv, bv), (ost, ot), (oss, os)))]

    misc = [
        pltpu.make_async_copy(px, pxs.at[:, pl.ds(SUB, ROWS), :], misc_sem.at[I0]),
        pltpu.make_async_copy(pd.at[I0], pxs.at[:, pl.ds(I0, SUB), :], misc_sem.at[I1]),
        pltpu.make_async_copy(pd.at[I1], pxs.at[:, pl.ds(SUB + ROWS, SUB), :], misc_sem.at[I2]),
        pltpu.make_async_copy(hr, hrs, misc_sem.at[I3]),
        pltpu.make_async_copy(hx2.at[I3], hks, misc_sem.at[4]),
    ]
    for t in range(I2):
        cols = pl.ds(LANE * t, LANE)
        misc.append(pltpu.make_async_copy(dep.at[:, cols], hs.at[t, pl.ds(SUB, ROWS), :], misc_sem.at[5 + 4 * t]))
        misc.append(pltpu.make_async_copy(kmt.at[:, cols], ki.at[t, pl.ds(SUB, ROWS), :], misc_sem.at[6 + 4 * t]))
        misc.append(pltpu.make_async_copy(hrh.at[I1, pl.ds(I0, SUB), cols], hs.at[t, pl.ds(SUB + ROWS, SUB), :], misc_sem.at[7 + 4 * t]))
        misc.append(pltpu.make_async_copy(hrk.at[I1, pl.ds(I0, SUB), cols], ki.at[t, pl.ds(SUB + ROWS, SUB), :], misc_sem.at[SUB + 4 * t]))
    for cp in misc:
        cp.start()
    for c in range(NCH - I1, NCH - I1 - SLOTS, -I1):
        for cp in load_copies(jnp.int32(c)):
            cp.start()
    for cp in misc:
        cp.wait()
    lane = lane_ids()
    is_last = lane == LAST
    is_first = lane == I0
    two = range(I2)
    for m in range(MEM):
        pxs[m, I0:SUB, :] = pxs[m, I0:SUB, :] * not_south
        pxs[m, SUB + ROWS:NEXT, :] = pxs[m, SUB + ROWS:NEXT, :] * not_north
        for f, (_, dst) in enumerate(fields):
            for t in two:
                for g in two:
                    ks = pl.ds(SUB * g, SUB)
                    dst[t, ks, m, 7:SUB, :] = (hrs[I0, m, f, t, ks, :] * not_south)[:, None, :]
                    dst[t, ks, m, SUB + ROWS:9 + ROWS, :] = (hrs[I1, m, f, t, ks, :] * not_north)[:, None, :]
    for t in two:
        kf[t, SUB:SUB + ROWS, :] = ki[t, SUB:SUB + ROWS, :].astype(F32)
        kf[t, SUB + ROWS:NEXT, :] = ki[t, SUB + ROWS:NEXT, :].astype(F32) * not_north
    rho_s = PRESS / LEV * HALINE
    rho_t = PRESS / LEV * THERM
    gain, inner, last = solve_factors(DIFF)
    zero = jnp.zeros((SUB, LANE), F32)

    def east(a, b, halo):
        ra, rb = rot(a, LAST), rot(b, LAST)
        return jnp.where(is_last, rb, ra), jnp.where(is_last, halo, rb)

    def push(x, edge, q):
        return [rot(a, LAST) for a in x] + [rot(edge, LAST - I2 * q)], [rot(a, I1) for a in x] + [rot(edge, 129 - I2 * q)]

    def pop_east(east_):
        return jnp.where(is_last, east_[I1], east_[I0]), jnp.where(is_last, east_[I2], east_[I1])

    def pop_west(west_):
        return jnp.where(is_first, west_[I2], west_[I0]), jnp.where(is_first, west_[I0], west_[I1])

    def unpack(r, m, k, edge):
        slot = lax.rem(jnp.maximum(r, I0) // BPC, SLOTS)
        src_rows = pl.ds(pl.multiple_of(SUB * lax.rem(jnp.maximum(r, I0), BPC), SUB), SUB)
        dst_rows = pl.ds(pl.multiple_of(jnp.where(r < I0, NEXT, SUB * r + SUB), SUB), SUB)
        rolled = []
        for f, (_, dst) in enumerate(fields):
            x = [stage[slot, f, k, m, src_rows, TILES[t]] for t in two]
            for t in two:
                dst[t, k, m, dst_rows, :] = x[t]
            rolled.append(push(x, edge, f * LEV + k))
        return rolled

    def settle(r, m, k, rolled):
        dst_rows = pl.ds(pl.multiple_of(jnp.where(r < I0, NEXT, SUB * r + SUB), SUB), SUB)
        ring = lax.rem(r + I2, I2)
        for f in range(4):
            east_, west_ = pop_east(rolled[f][I0]), pop_west(rolled[f][I1])
            for t in two:
                if f == I0:
                    sides[I0, ring, t, k, m, :, :] = east_[t]
                    uwl[t, k, m, dst_rows, :] = west_[t]
                elif f == I1:
                    vel[t, k, m, dst_rows, :] = east_[t]
                    sides[I1, ring, t, k, m, :, :] = west_[t]
                else:
                    sides[I2 * f - I2, ring, t, k, m, :, :] = east_[t]
                    sides[I2 * f - I1, ring, t, k, m, :, :] = west_[t]

    def prime(m, carry):
        south, north, first = pl.ds(I0, SUB), pl.ds(SUB + ROWS, SUB), pl.ds(ROWS, SUB)
        below = [zero, zero]
        for k in range(LEV):
            settle(jnp.int32(ROWS // SUB - I1), m, k, unpack(jnp.int32(ROWS // SUB - I1), m, k, pxs[m, first, :]))
            v_side = push([vs[t, k, m, south, :] for t in two], pxs[m, south, :], LEV + k)[I0]
            u_side = push([us[t, k, m, north, :] for t in two], pxs[m, north, :], k)[I1]
            for t, x in enumerate(pop_east(v_side)):
                vel[t, k, m, south, :] = x
            for t, x in enumerate(pop_west(u_side)):
                uwl[t, k, m, north, :] = x
            for t in two:
                half = (HALF * rho_s) * ss[t, k, m, north, :] - (HALF * rho_t) * ts[t, k, m, north, :]
                ps[t, k, m, north, :] = below[t] + half
                below[t] = (below[t] + half) + half
        return carry

    def block(r):
        y = pl.multiple_of(r * SUB + SUB, SUB)
        rows = pl.ds(y, SUB)
        up = pl.ds(y + I1, SUB)
        down = pl.ds(y - I1, SUB)
        south = pl.ds(y - SUB, SUB)
        out_rows = pl.ds(pl.multiple_of(r * SUB, SUB), SUB)
        kc = [kf[t, rows, :] for t in two]
        hk = hks[out_rows, :]
        ke = east(kc[I0], kc[I1], rot(hk, 63))
        hc = [hs[t, rows, :] for t in two]
        he = east(hc[I0], hc[I1], rot(hk, LAST))
        kx = [jnp.minimum(kc[t], ke[t]) for t in two]
        ky = [jnp.minimum(kc[t], kf[t, up, :]) for t in two]
        scale_x, scale_y = [], []
        for t in two:
            nx[out_rows, TILES[t]] = kx[t]
            ny[out_rows, TILES[t]] = ky[t]
            scale_x.append(jnp.where(kx[t] > ZERO, HALF * (hc[t] + he[t]), ZERO) / (jnp.maximum(kx[t], ONE) * NSUB))
            scale_y.append(jnp.where(ky[t] > ZERO, HALF * (hc[t] + hs[t, up, :]), ZERO) / (jnp.maximum(ky[t], ONE) * NSUB))

        ring = lax.rem(r, I2)

        def member(m, carry):
            edge = pxs[m, south, :]
            below = [zero] * 4
            sum_x = [zero, zero]
            sum_y = [zero, zero]
            run_t = [None, None]
            run_s = [None, None]
            waiting = []
            for ahead in range(LEV + DEPTH):
                if ahead < LEV:
                    waiting.append(unpack(r - I1, m, ahead, edge))
                k = ahead - DEPTH
                if k < I0:
                    continue
                settle(r - I1, m, k, waiting.pop(I0))
                for t in two:
                    uc, un, ud = us[t, k, m, rows, :], us[t, k, m, up, :], us[t, k, m, down, :]
                    vc, vn, vd = vs[t, k, m, rows, :], vs[t, k, m, up, :], vs[t, k, m, down, :]
                    tc, sc = ts[t, k, m, rows, :], ss[t, k, m, rows, :]
                    ue, vw, t_e, t_w, s_e, s_w = [sides[i, ring, t, k, m, :, :] for i in range(6)]
                    uw, ve = uwl[t, k, m, rows, :], vel[t, k, m, rows, :]
                    half = (HALF * rho_s) * sc - (HALF * rho_t) * tc
                    press = below[t] + half
                    below[t] = press + half
                    half = (HALF * rho_s) * s_e - (HALF * rho_t) * t_e
                    press_e = below[I2 + t] + half
                    below[I2 + t] = press_e + half
                    ps[t, k, m, rows, :] = press
                    uh, vh, vdh, uwh = HALF * uc, HALF * vc, HALF * vd, HALF * uw
                    vq = (vc + vd) + (ve + vel[t, k, m, down, :])
                    uq = (uc + un) + (uw + uwl[t, k, m, up, :])
                    gu = (press - press_e) - uh * (ue - uw) - 0.125 * (vq * (un - ud))
                    gu = jnp.where(kx[t] > float(k), gu, ZERO)
                    sum_x[t] = sum_x[t] + gu
                    obu[k, m, out_rows, TILES[t]] = uc + gu
                    gv = (press - ps[t, k, m, up, :]) - 0.125 * (uq * (ve - vw)) - vh * (vn - vd)
                    gv = jnp.where(ky[t] > float(k), gv, ZERO)
                    sum_y[t] = sum_y[t] + gv
                    obv[k, m, out_rows, TILES[t]] = vc + gv
                    wet = kc[t] > float(k)
                    for scr, cen, e, w, run, dst in ((ts, tc, t_e, t_w, run_t, ost), (ss, sc, s_e, s_w, run_s, oss)):
                        fx = uh * (cen + e) - uwh * (w + cen)
                        fy = vh * (cen + scr[t, k, m, up, :]) - vdh * (scr[t, k, m, down, :] + cen)
                        new = jnp.where(wet, cen - (fx + fy), ZERO)
                        run[t] = new if k == I0 else new + gain[k - I1] * run[t]
                        dst[k, m, out_rows, TILES[t]] = run[t]
            for t in two:
                sx[m, out_rows, TILES[t]] = scale_x[t] * sum_x[t]
                sy[m, out_rows, TILES[t]] = scale_y[t] * sum_y[t]
                nt = ns = zero
                for k in range(LEV - I1, -I1, -I1):
                    coef = level_factor(kc[t], k, inner, last)
                    nt = coef * ost[k, m, out_rows, TILES[t]] + gain[k] * nt
                    ns = coef * oss[k, m, out_rows, TILES[t]] + gain[k] * ns
                    ost[k, m, out_rows, TILES[t]] = nt
                    oss[k, m, out_rows, TILES[t]] = ns
            return carry

        lax.fori_loop(I0, MEM, member, I0)

    for cp in load_copies(jnp.int32(NCH - I1)):
        cp.wait()
    lax.fori_loop(I0, MEM, prime, I0)

    def step(i, carry):
        r = ROWS // SUB - I1 - i
        c = r // BPC
        edge = lax.rem(r, BPC) == I0

        @pl.when(edge & (c >= I1))
        def _():
            for cp in load_copies(c - I1):
                cp.wait()

        @pl.when(edge & (c >= SLOTS))
        def _():
            for cp in load_copies(c - SLOTS):
                cp.start()

        @pl.when(edge & (c + I1 < NCH))
        def _():
            for cp in out_copies(c + I1):
                cp.start()

        block(r)
        return carry

    lax.fori_loop(I0, ROWS // SUB, step, I0)
    for cp in out_copies(jnp.int32(I0)):
        cp.start()
    for c in range(NCH):
        for cp in out_copies(jnp.int32(c)):
            cp.wait()


def columns_call(u, v, te, sa, px, pd, hr, dep, kmt, hx2, hrh, hrk):
    big = pltpu.VMEM((I2, LEV, MEM, EXT, LANE), F32)
    full = pltpu.VMEM((LEV, MEM, ROWS, COLS), F32)
    o3 = sds(LEV, MEM, ROWS, COLS)
    o2 = sds(MEM, ROWS, COLS)
    o1 = sds(ROWS, COLS)
    return pl.pallas_call(
        columns_kernel,
        name="columns",
        out_shape=(o3, o3, o3, o3, o2, o2, o1, o1),
        in_specs=[ANY] * 12,
        out_specs=(ANY,) * 4 + (VM,) * 4,
        scratch_shapes=[big] * 7
        + [
            pltpu.VMEM((6, I2, I2, LEV, MEM, SUB, LANE), F32),
            pltpu.VMEM((SLOTS, 4, LEV, MEM, CHUNK, COLS), F32),
            pltpu.VMEM((MEM, NEXT, LANE), F32),
            pltpu.VMEM((I2, MEM, 4, I2, LEV, LANE), F32),
            pltpu.VMEM((I2, NEXT, LANE), F32),
            pltpu.VMEM((I2, NEXT, LANE), jnp.int32),
            pltpu.VMEM((I2, NEXT, LANE), F32),
            pltpu.VMEM((ROWS, LANE), F32),
            full, full, full, full,
            pltpu.SemaphoreType.DMA((SLOTS, 4)),
            pltpu.SemaphoreType.DMA((13,)),
            pltpu.SemaphoreType.DMA((4,)),
        ],
        compiler_params=pltpu.CompilerParams(vmem_limit_bytes=LIMIT),
    )(u, v, te, sa, px, pd, hr, dep, kmt, hx2, hrh, hrk)


def forcing_kernel(sx, sy, hxs, hds, hrx, hry, pk, send_sem, recv_sem):
    ids = neighbours()
    enter(ids)
    lane = lane_ids()
    sent = []

    def send(src, dst, who):
        i = len(sent)
        cp = pltpu.make_async_remote_copy(src_ref=src, dst_ref=dst, send_sem=send_sem.at[i], recv_sem=recv_sem.at[i], device_id=ids[who], device_id_type=MESH)
        cp.start()
        sent.append(cp)

    for r in range(ROWS // SUB):
        rows = pl.ds(SUB * r, SUB)
        for i, a in enumerate((sx, sy)):
            pk[i, rows, :] = wide_pack(lane, *[a[m, rows, t] for m in range(MEM) for t in TILES])
    for src, dst in ((sx, hrx), (sy, hry)):
        send(src.at[:, pl.ds(ROWS - HALO, HALO), :], dst.at[I0], "n")
        send(src.at[:, pl.ds(I0, HALO), :], dst.at[I1], "s")
    send(pk, hxs, "x")
    send(pk.at[:, pl.ds(ROWS - HALO, HALO), :], hds.at[I0], "nx")
    send(pk.at[:, pl.ds(I0, HALO), :], hds.at[I1], "sx")
    for cp in sent:
        cp.wait()


def forcing_call(sx, sy):
    return pl.pallas_call(
        forcing_kernel,
        name="forcing",
        out_shape=(sds(I2, ROWS, LANE), sds(I2, I2, HALO, LANE), sds(I2, MEM, HALO, COLS), sds(I2, MEM, HALO, COLS)),
        in_specs=[VM, VM],
        out_specs=(ANY,) * 4,
        scratch_shapes=[pltpu.VMEM((I2, ROWS, LANE), F32), pltpu.SemaphoreType.DMA((7,)), pltpu.SemaphoreType.DMA((7,))],
        compiler_params=pltpu.CompilerParams(collective_id=I1, has_side_effects=True, vmem_limit_bytes=LIMIT),
    )(sx, sy)


def turn_east(x):
    return [rot(a, LAST) for a in x] + [rot(x[I2], 63), rot(x[4], 63)]


def pick_east(r, lane):
    last = lane == LAST
    far = jnp.where(lane == 63, r[5], r[4])
    return [jnp.where(last, r[I1], r[I0]), jnp.where(last, r[4], r[I1]), jnp.where(last, r[I3], r[I2]), jnp.where(last, r[6], r[I3]), jnp.where(last, r[I0], far)]


def turn_west(x):
    return [rot(a, I1) for a in x] + [rot(x[I3], 65), rot(x[4], 65)]


def pick_west(r, lane):
    first = lane == I0
    far = jnp.where(lane == 64, r[5], r[4])
    return [jnp.where(first, r[4], r[I0]), jnp.where(first, r[I0], r[I1]), jnp.where(first, r[6], r[I2]), jnp.where(first, r[I2], r[I3]), jnp.where(first, r[I1], far)]


def turn_east3(x):
    return [rot(a, LAST) for a in x] + [rot(x[I0], 63)]


def pick_east3(r, lane):
    last = lane == LAST
    far = jnp.where(lane == 63, r[I3], r[I2])
    return [jnp.where(last, r[I1], r[I0]), jnp.where(last, r[I2], r[I1]), jnp.where(last, r[I0], far)]


def turn_west3(x):
    return [rot(a, I1) for a in x] + [rot(x[I1], 65)]


def pick_west3(r, lane):
    first = lane == I0
    far = jnp.where(lane == 64, r[I3], r[I2])
    return [jnp.where(first, r[I2], r[I0]), jnp.where(first, r[I0], r[I1]), jnp.where(first, r[I1], far)]


def staged(items, issue, finish, depth):
    queue = []
    for item in items:
        queue.append((item, issue(item)))
        if len(queue) > depth:
            finish(*queue.pop(I0))
    for item, value in queue:
        finish(item, value)


SHARED = (I0, I1, I0, I1, I2)


def subcycle_kernel(weights, eta, tx, ty, sx, sy, dep, kmt, hx2, hd2, hre, hrx, hry, hrh, hrk, hxs, hds, hrsx, hrsy, bu, bv, nx, ny, eta_out, tx_out, ty_out, ou, ov, cx_out, cy_out, sol_u, sol_v, cnt_x, cnt_y, far_sem, nat, side, hn, kn, e0, e1, t1, t2, f1, f2, hh, kf, gx, gy, gxw, gc, wv, fo, acc1, acc2, ee, ew, tails, sem):
    row = lax.axis_index("row")
    not_south = jnp.where(row == I0, ZERO, ONE).astype(F32)
    not_north = jnp.where(row == NR - I1, ZERO, ONE).astype(F32)
    lane = lane_ids()
    base = SUB + HALO
    top = base + ROWS
    low, mid, high = pl.ds(I0, HALO), pl.ds(HALO, ROWS), pl.ds(HALO + ROWS, HALO)
    copies = []

    def fetch(src, dst):
        copies.append(pltpu.make_async_copy(src, dst, sem))

    for i, (own_, rows_) in enumerate(((eta, hre), (tx, hrx), (ty, hry), (sx, hrsx), (sy, hrsy))):
        fetch(own_, nat.at[i, :, mid, :])
        fetch(rows_.at[I0], nat.at[i, :, low, :])
        fetch(rows_.at[I1], nat.at[i, :, high, :])
    for first, count, main, corner in ((I0, 4, hx2, hd2), (4, I2, hxs, hds)):
        part = pl.ds(first, count)
        fetch(main, side.at[part, mid, :])
        fetch(corner.at[I0], side.at[part, low, :])
        fetch(corner.at[I1], side.at[part, high, :])
    for own_, rows_, dst in ((dep, hrh, hn), (kmt, hrk, kn)):
        fetch(own_, dst.at[mid, :])
        fetch(rows_.at[I0], dst.at[low, :])
        fetch(rows_.at[I1], dst.at[high, :])
    for cp in copies:
        cp.start()
    incoming = [pltpu.make_async_copy(src, dst, far_sem.at[I0]) for src, dst in ((bu, sol_u), (bv, sol_v), (nx, cnt_x), (ny, cnt_y))]
    for cp in incoming:
        cp.start()
    total = jnp.float32(ZERO)
    moment = jnp.float32(ZERO)
    for n in range(NSUB - I1, -I1, -I1):
        total = total + weights[n]
        moment = moment + total
        tails[n] = total
    for cp in copies:
        cp.wait()
    own = (lane < 32) | (lane >= 96)
    zero = jnp.zeros((SUB, LANE), F32)
    three, five = range(I3), range(5)
    for i in three:
        kf[i, I0:SUB, :] = zero
        kf[i, SUB + NEAR:BEXT, :] = zero
    everything = range(I1, I1 + NEAR // SUB)

    def rows_of(r):
        return pl.ds(SUB * r, SUB), pl.ds(SUB * r + I1, SUB), pl.ds(SUB * r - I1, SUB), pl.ds(SUB * r - SUB, SUB)

    def level_issue(r):
        here = rows_of(r)[I3]
        packed = side[I3, here, :]
        return packed, rot(packed, 64)

    def level_finish(r, value):
        packed, turned = value
        rows, _, _, here = rows_of(r)
        levels = [kn[here, t].astype(F32) for t in TILES] + [jnp.where(own, turned, packed)]
        depths = [hn[here, t] for t in TILES] + [jnp.where(own, packed, turned)]
        keep = not_south if r < base // SUB else not_north
        inside = base // SUB <= r < top // SUB
        for i in three:
            kf[i, rows, :] = levels[i] if inside else levels[i] * keep
            hh[i, rows, :] = depths[i]

    staged(everything, level_issue, level_finish, SUB)

    def mask_issue(r):
        rows = rows_of(r)[I0]
        kc = [kf[i, rows, :] for i in three]
        hc = [hh[i, rows, :] for i in three]
        return kc, hc, turn_east3(kc), turn_east3(hc)

    def mask_finish(r, value):
        kc, hc, kt, ht = value
        rows, up, down, here = rows_of(r)
        ke, he = pick_east3(kt, lane), pick_east3(ht, lane)
        wet = [kc[i] > ZERO for i in three]
        wet_x = [jnp.minimum(kc[i], ke[i]) > ZERO for i in three]
        wet_y = [jnp.minimum(kc[i], kf[i, up, :]) > ZERO for i in three]
        for i in three:
            gx[i, rows, :] = jnp.where(wet_x[i], (HALF * WAVE * WAVE) * (hc[i] + he[i]), ZERO)
            gy[i, rows, :] = jnp.where(wet_y[i], (HALF * WAVE * WAVE) * (hc[i] + hh[i, up, :]), ZERO)
        for f, mask, dst in ((I0, wet, e0), (I1, wet_x, t1), (I2, wet_y, t2), (I3, wet_x, f1), (4, wet_y, f2)):
            slot = f if f < I3 else f + I1
            raw = [nat[f, m, here, t] for m in range(MEM) for t in TILES] + [side[slot, here, :]]
            for i in five:
                dst[i, rows, :] = jnp.where(mask[SHARED[i]], raw[i], ZERO)

    staged(everything, mask_issue, mask_finish, I3)

    def start_issue(r):
        rows = rows_of(r)[I0]
        a = [t1[i, rows, :] for i in five]
        c = [f1[i, rows, :] for i in five]
        return a, c, turn_west(a), turn_west(c), turn_west3([gx[i, rows, :] for i in three])

    late = []

    def start_finish(r, value):
        a, c, at, ct, gt = value
        rows, up, down, here = rows_of(r)
        aw, cw, gw = pick_west(at, lane), pick_west(ct, lane), pick_west3(gt, lane)
        for i in three:
            gxw[i, rows, :] = gw[i]
            gc[i, rows, :] = (gx[i, rows, :] + gw[i]) + (gy[i, rows, :] + gy[i, down, :])
        fresh = []
        for i in five:
            w = -WAVE * ((a[i] - aw[i]) + (t2[i, rows, :] - t2[i, down, :]))
            fo[i, rows, :] = -WAVE * ((c[i] - cw[i]) + (f2[i, rows, :] - f2[i, down, :]))
            now = e0[i, rows, :] + w
            wv[i, rows, :] = w
            e0[i, rows, :] = now
            acc1[i, rows, :] = weights[I0] * now
            acc2[i, rows, :] = tails[I0] * now
            fresh.append(now)
        late.append((r, turn_east(fresh), turn_west(fresh)))
        if len(late) > I3:
            store_sides(*late.pop(I0), I0)

    def store_sides(r, et, wt, buf):
        rows = rows_of(r)[I0]
        ne, nw = pick_east(et, lane), pick_west(wt, lane)
        for i in five:
            ee[buf, i, rows, :] = ne[i]
            ew[buf, i, rows, :] = nw[i]

    staged(everything, start_issue, start_finish, I3)
    for item in late:
        store_sides(*item, I0)

    def advance(src, buf, dst, r, plan):
        rows, up, down, _ = rows_of(r)
        gxc, gxm, gyc, gyd, gcc = [[g[i, rows_, :] for i in three] for g, rows_ in ((gx, rows), (gxw, rows), (gy, rows), (gy, down), (gc, rows))]
        fresh = []
        for i in five:
            j = SHARED[i]
            now = src[i, rows, :]
            w = (wv[i, rows, :] + fo[i, rows, :]) - gcc[j] * now
            w = w + ((gxc[j] * ee[buf, i, rows, :] + gxm[j] * ew[buf, i, rows, :]) + (gyc[j] * src[i, up, :] + gyd[j] * src[i, down, :]))
            new = now + w
            wv[i, rows, :] = w
            dst[i, rows, :] = new
            fresh.append(new)
            if plan is not None:
                prev, a0, b0, a1, b1 = plan
                s1, s2 = acc1[i, rows, :], acc2[i, rows, :]
                if prev:
                    s1 = s1 + a0 * now
                    s2 = s2 + b0 * now
                acc1[i, rows, :] = s1 + a1 * new
                acc2[i, rows, :] = s2 + b1 * new
        return turn_east(fresh), turn_west(fresh)

    def sweep(src, buf, dst, lo, hi, plan, depth=I3):
        def issue(r):
            return advance(src, buf, dst, r, plan if base // SUB <= r <= top // SUB else None)

        def finish(r, value):
            store_sides(r, *value, I1 - buf)

        staged(range(lo, hi), issue, finish, depth)

    for begin, end in ((I0, I2), (I2, 6), (6, 10), (10, 14)):
        lo = (I2 * begin + 12) // SUB
        hi = (196 - I2 * begin) // SUB + I1

        def pair(i, carry):
            m = I2 * i + I2
            sweep(e0, I0, e1, lo, hi, None)
            sweep(e1, I1, e0, lo, hi, (True, weights[m - I1], tails[m - I1], weights[m], tails[m]))
            return carry

        lax.fori_loop(begin, end, pair, I0)
    sweep(e0, I0, e1, base // SUB, top // SUB + I1, (False, None, None, weights[NSUB - I1], tails[NSUB - I1]))

    def end_issue(r):
        rows = rows_of(r)[I0]
        s = [acc2[i, rows, :] for i in five]
        return s, turn_east(s)

    def end_finish(r, value):
        s, st = value
        rows, up, _, _ = rows_of(r)
        out_rows = pl.ds(SUB * r - base, SUB)
        se = pick_east(st, lane)
        for m in range(MEM):
            for t in range(I2):
                i = I2 * m + t
                cols = TILES[t]
                eta_out[m, out_rows, cols] = acc1[i, rows, :]
                gxc, gyc = gx[t, rows, :], gy[t, rows, :]
                ux = total * t1[i, rows, :] + moment * f1[i, rows, :] - (ONE / WAVE) * (gxc * (se[i] - s[i]))
                uy = total * t2[i, rows, :] + moment * f2[i, rows, :] - (ONE / WAVE) * (gyc * (acc2[i, up, :] - s[i]))
                tx_out[m, out_rows, cols] = ux
                ty_out[m, out_rows, cols] = uy
                cx_out[m, out_rows, cols] = ux / jnp.where(gxc > ZERO, gxc * (ONE / (WAVE * WAVE)), ONE)
                cy_out[m, out_rows, cols] = uy / jnp.where(gyc > ZERO, gyc * (ONE / (WAVE * WAVE)), ONE)

    staged(range(base // SUB, top // SUB), end_issue, end_finish, I3)
    for cp in incoming:
        cp.wait()
    gain, inner, last = solve_factors(VISC)

    def body(j, carry):
        rows = pl.ds(pl.multiple_of(j * SUB, SUB), SUB)
        for src, cnt, shift in ((sol_u, cnt_x, cx_out), (sol_v, cnt_y, cy_out)):
            for cols in TILES:
                n = cnt[rows, cols]
                run = []
                for k in range(LEV):
                    b = [src[k, m, rows, cols] for m in range(MEM)]
                    run.append(b if k == I0 else [b[m] + gain[k - I1] * run[-I1][m] for m in range(MEM)])
                nxt = [jnp.zeros((SUB, LANE), F32)] * MEM
                tot = list(nxt)
                sol = [None] * LEV
                for k in range(LEV - I1, -I1, -I1):
                    coef = level_factor(n, k, inner, last)
                    nxt = [coef * run[k][m] + gain[k] * nxt[m] for m in range(MEM)]
                    tot = [tot[m] + nxt[m] for m in range(MEM)]
                    sol[k] = nxt
                share = ONE / jnp.maximum(n, ONE)
                add = [shift[m, rows, cols] - tot[m] * share for m in range(MEM)]
                for k in range(LEV):
                    wet = n > float(k)
                    for m in range(MEM):
                        src[k, m, rows, cols] = jnp.where(wet, sol[k][m] + add[m], ZERO)
        return carry

    def outgoing(c):
        rows = pl.ds(HALO * c, HALO)
        return [pltpu.make_async_copy(a.at[:, :, rows, :], b.at[:, :, rows, :], far_sem.at[I1]) for a, b in ((sol_u, ou), (sol_v, ov))]

    for c in range(ROWS // HALO):
        lax.fori_loop(c * (HALO // SUB), (c + I1) * (HALO // SUB), body, I0)
        for cp in outgoing(c):
            cp.start()
    for c in range(ROWS // HALO):
        for cp in outgoing(c):
            cp.wait()


def subcycle_call(weights, *arrays):
    o2 = sds(MEM, ROWS, COLS)
    o3 = sds(LEV, MEM, ROWS, COLS)
    five = pltpu.VMEM((5, BEXT, LANE), F32)
    three = pltpu.VMEM((I3, BEXT, LANE), F32)
    return pl.pallas_call(
        subcycle_kernel,
        name="subcycle",
        out_shape=(o2, o2, o2, o3, o3),
        in_specs=[SM] + [ANY] * len(arrays),
        out_specs=(VM, VM, VM, ANY, ANY),
        scratch_shapes=[
            pltpu.VMEM((MEM, ROWS, COLS), F32),
            pltpu.VMEM((MEM, ROWS, COLS), F32),
            pltpu.VMEM((LEV, MEM, ROWS, COLS), F32),
            pltpu.VMEM((LEV, MEM, ROWS, COLS), F32),
            pltpu.VMEM((ROWS, COLS), F32),
            pltpu.VMEM((ROWS, COLS), F32),
            pltpu.SemaphoreType.DMA((I2,)),
            pltpu.VMEM((5, MEM, NEAR, COLS), F32),
            pltpu.VMEM((6, NEAR, LANE), F32),
            pltpu.VMEM((NEAR, COLS), F32),
            pltpu.VMEM((NEAR, COLS), jnp.int32),
            *[five] * 6, *[three] * 6, *[five] * 4, pltpu.VMEM((I2, 5, BEXT, LANE), F32), pltpu.VMEM((I2, 5, BEXT, LANE), F32),
            pltpu.SMEM((NSUB,), F32),
            pltpu.SemaphoreType.DMA,
        ],
        compiler_params=pltpu.CompilerParams(vmem_limit_bytes=LIMIT),
    )(weights, *arrays)


def local_step(u, v, te, sa, eta, tx, ty, dep, kmt, weights):
    px, pd, hr, hx2, hd2, hre, hrx, hry, hrh, hrk = edges_call(u, v, te, sa, eta, tx, ty, dep, kmt)
    bu, bv, ot, os, sx, sy, nx, ny = columns_call(u, v, te, sa, px, pd, hr, dep, kmt, hx2, hrh, hrk)
    hxs, hds, hrsx, hrsy = forcing_call(sx, sy)
    eta_new, tx_new, ty_new, ou, ov = subcycle_call(weights, eta, tx, ty, sx, sy, dep, kmt, hx2, hd2, hre, hrx, hry, hrh, hrk, hxs, hds, hrsx, hrsy, bu, bv, nx, ny)
    return eta_new, tx_new, ty_new, ou, ov, ot, os


def solution(mesh):
    s3 = P(None, None, "row", "col")
    s2 = P(None, "row", "col")
    s1 = P("row", "col")
    return jax.shard_map(local_step, mesh=mesh, in_specs=(s3, s3, s3, s3, s2, s2, s2, s1, s1, P()), out_specs=(s2, s2, s2, s3, s3, s3, s3), check_vma=False)
```

```python
import functools
import jax
import jax.numpy as jnp
from jax import lax
from jax.experimental import pallas as pl
from jax.experimental.pallas import tpu as pltpu
from jax.sharding import PartitionSpec as P

SUB = 8
LANE = 128
LAST = 127
ZERO = 0.0
ONE = 1.0
HALF = 0.5
I0, I1, I2, I3 = range(4)
WAVE = 0.4
THERM = 0.2
HALINE = 0.15
PRESS = HALF
VISC = ONE
DIFF = HALF
LEV = 16
MEM = I2
NSUB = 30
ROWS = LANE
COLS = 256
NR = SUB
NC = I2
HALO = 32
NEXT = 144
EXT = 152
BEXT = 208
NEAR = 192
F32 = jnp.float32
CHUNK = 32
NCH = ROWS // CHUNK
SLOTS = I2
BPC = CHUNK // SUB
DEPTH = I2
MESH = pl.DeviceIdType.MESH
LIMIT = 67043328
TILES = (slice(I0, LANE), slice(LANE, 256))
ANY = pl.BlockSpec(memory_space=pl.ANY)
VM = pl.BlockSpec(memory_space=pltpu.VMEM)
SM = pl.BlockSpec(memory_space=pltpu.SMEM)


def solve_factors(strength):
    gain, inner, last = [], [], []
    prev = None
    for k in range(LEV):
        if k == I0:
            diag, edge = ONE + strength, ONE
        else:
            diag, edge = ONE + 2.0 * strength - strength * prev, ONE + strength - strength * prev
        inner.append(ONE / diag)
        last.append(ONE / edge)
        prev = strength / diag
        gain.append(prev)
    return gain, inner, last


def level_factor(count, k, inner, last):
    edge = jnp.where(count > float(k), last[k], ZERO)
    return edge if k == LEV - I1 else jnp.where(count > float(k + I1), inner[k], edge)


def lane_ids():
    return lax.broadcasted_iota(jnp.int32, (SUB, LANE), I1)


def rot(x, shift):
    shift %= LANE
    return x if shift == I0 else pltpu.roll(x, shift, I1)


def neighbours():
    col = lax.axis_index("col")
    row = lax.axis_index("row")
    other = I1 - col
    north = lax.rem(row + I1, NR)
    south = lax.rem(row + NR - I1, NR)
    return {"x": (other, row), "n": (col, north), "s": (col, south), "nx": (other, north), "sx": (other, south)}


def enter(ids):
    barrier = pltpu.get_barrier_semaphore()
    for target in ids.values():
        pl.semaphore_signal(barrier, inc=I1, device_id=target, device_id_type=MESH)
    pl.semaphore_wait(barrier, len(ids))


def wide_pack(lane, m0t0, m0t1, m1t0, m1t1):
    first = jnp.where(lane < 64, m0t0, m0t1)
    second = jnp.where(lane < 64, m1t0, m1t1)
    return jnp.where((lane < 32) | (lane >= 96), first, rot(second, 64))


def edges_kernel(u, v, te, sa, eta, tx, ty, dep, kmt, px, pd, hr, hx2, hd2, hre, hrx, hry, hrh, hrk, big, s2, sh, sk, pk, rowb, pk2, load_sem, load2_sem, send_sem, recv_sem):
    ids = neighbours()
    fields = (u, v, te, sa)
    loads = []
    for m in range(MEM):
        loads.append([pltpu.make_async_copy(fields[f].at[:, m], big.at[m, f], load_sem.at[m, f]) for f in range(4)])
    loads2 = [pltpu.make_async_copy(a, s2.at[i], load2_sem.at[i]) for i, a in enumerate((eta, tx, ty))]
    loads2.append(pltpu.make_async_copy(dep, sh, load2_sem.at[I3]))
    loads2.append(pltpu.make_async_copy(kmt, sk, load2_sem.at[4]))
    for cp in loads2:
        cp.start()
    for cp in loads[I0] + loads[I1]:
        cp.start()
    enter(ids)
    sent = []

    def send(src, dst, who):
        i = len(sent)
        cp = pltpu.make_async_remote_copy(src_ref=src, dst_ref=dst, send_sem=send_sem.at[i], recv_sem=recv_sem.at[i], device_id=ids[who], device_id_type=MESH)
        cp.start()
        sent.append(cp)
        return cp

    for src, dst in ((eta, hre), (tx, hrx), (ty, hry)):
        send(src.at[:, pl.ds(ROWS - HALO, HALO), :], dst.at[I0], "n")
        send(src.at[:, pl.ds(I0, HALO), :], dst.at[I1], "s")
    for src, dst in ((dep, hrh), (kmt, hrk)):
        send(src.at[pl.ds(ROWS - HALO, HALO), :], dst.at[I0], "n")
        send(src.at[pl.ds(I0, HALO), :], dst.at[I1], "s")
    lane = lane_ids()
    for cp in loads2:
        cp.wait()
    for r in range(ROWS // SUB):
        rows = pl.ds(SUB * r, SUB)
        for i in range(I3):
            pk2[i, rows, :] = wide_pack(lane, *[s2[i, m, rows, t] for m in range(MEM) for t in TILES])
        pk2[I3, rows, :] = wide_pack(lane, *[sh[rows, t] for t in TILES], *[sk[rows, t].astype(F32) for t in TILES])
    pair = lax.rem(lane + I1, LANE) // I2

    def pack3(m):
        for cp in loads[m]:
            cp.wait()

        def body(g, carry):
            for j in range(4):
                rows = pl.ds(pl.multiple_of(g * 32 + SUB * j, SUB), SUB)
                acc = jnp.zeros((SUB, LANE), F32)
                for f in range(4):
                    for k in range(LEV):
                        q = f * LEV + k
                        both = jnp.where(lane < 64, big[m, f, k, rows, TILES[I0]], big[m, f, k, rows, TILES[I1]])
                        acc = jnp.where(pair == q, rot(both, I2 * q), acc)
                pk[m, rows, :] = acc
            return carry

        lax.fori_loop(I0, 4, body, I0)
        for f in range(4):
            for t in range(I2):
                for g in range(I2):
                    ks = pl.ds(SUB * g, SUB)
                    rowb[I0, m, f, t, ks, :] = big[m, f, ks, ROWS - I1, TILES[t]]
                    rowb[I1, m, f, t, ks, :] = big[m, f, ks, I0, TILES[t]]

    def send3(m):
        send(pk.at[m], px.at[m], "x")
        send(pk.at[m, pl.ds(ROWS - SUB, SUB), :], pd.at[I0, m], "nx")
        send(pk.at[m, pl.ds(I0, SUB), :], pd.at[I1, m], "sx")
        send(rowb.at[I0, m], hr.at[I0, m], "n")
        send(rowb.at[I1, m], hr.at[I1, m], "s")

    side = send(pk2, hx2, "x")
    pack3(I0)
    send3(I0)
    pack3(I1)
    send3(I1)
    side.wait()
    send(hx2.at[:, pl.ds(ROWS - HALO, HALO), :], hd2.at[I0], "n")
    send(hx2.at[:, pl.ds(I0, HALO), :], hd2.at[I1], "s")
    for cp in sent:
        if cp is not side:
            cp.wait()


def sds(*shape, dtype=F32):
    return jax.ShapeDtypeStruct(shape, dtype)


NSEND_A = 23


def edges_call(u, v, te, sa, eta, tx, ty, dep, kmt):
    return pl.pallas_call(
        edges_kernel,
        name="edges",
        out_shape=(
            sds(MEM, ROWS, LANE), sds(I2, MEM, SUB, LANE), sds(I2, MEM, 4, I2, LEV, LANE),
            sds(4, ROWS, LANE), sds(I2, 4, HALO, LANE),
            sds(I2, MEM, HALO, COLS), sds(I2, MEM, HALO, COLS), sds(I2, MEM, HALO, COLS),
            sds(I2, HALO, COLS), sds(I2, HALO, COLS, dtype=jnp.int32),
        ),
        in_specs=[ANY] * 9,
        out_specs=(ANY,) * 10,
        scratch_shapes=[
            pltpu.VMEM((MEM, 4, LEV, ROWS, COLS), F32),
            pltpu.VMEM((I3, MEM, ROWS, COLS), F32),
            pltpu.VMEM((ROWS, COLS), F32),
            pltpu.VMEM((ROWS, COLS), jnp.int32),
            pltpu.VMEM((MEM, ROWS, LANE), F32),
            pltpu.VMEM((I2, MEM, 4, I2, LEV, LANE), F32),
            pltpu.VMEM((4, ROWS, LANE), F32),
            pltpu.SemaphoreType.DMA((MEM, 4)),
            pltpu.SemaphoreType.DMA((5,)),
            pltpu.SemaphoreType.DMA((NSEND_A,)),
            pltpu.SemaphoreType.DMA((NSEND_A,)),
        ],
        compiler_params=pltpu.CompilerParams(collective_id=I0, has_side_effects=True, vmem_limit_bytes=LIMIT),
    )(u, v, te, sa, eta, tx, ty, dep, kmt)


def columns_kernel(u, v, te, sa, px, pd, hr, dep, kmt, hx2, hrh, hrk, bu, bv, ot, os, sx, sy, nx, ny, us, vs, ts, ss, ps, vel, uwl, sides, stage, pxs, hrs, hs, ki, kf, hks, obu, obv, ost, oss, load_sem, misc_sem, out_sem):
    row = lax.axis_index("row")
    not_south = jnp.where(row == I0, ZERO, ONE).astype(F32)
    not_north = jnp.where(row == NR - I1, ZERO, ONE).astype(F32)
    fields = ((u, us), (v, vs), (te, ts), (sa, ss))

    def load_copies(c):
        rows = pl.ds(pl.multiple_of(CHUNK * c, CHUNK), CHUNK)
        slot = lax.rem(c, SLOTS)
        return [pltpu.make_async_copy(src.at[:, :, rows, :], stage.at[slot, f], load_sem.at[slot, f]) for f, (src, _) in enumerate(fields)]

    def out_copies(c):
        rows = pl.ds(pl.multiple_of(CHUNK * c, CHUNK), CHUNK)
        return [pltpu.make_async_copy(a.at[:, :, rows, :], b.at[:, :, rows, :], out_sem.at[i]) for i, (a, b) in enumerate(((obu, bu), (obv, bv), (ost, ot), (oss, os)))]

    misc = [
        pltpu.make_async_copy(px, pxs.at[:, pl.ds(SUB, ROWS), :], misc_sem.at[I0]),
        pltpu.make_async_copy(pd.at[I0], pxs.at[:, pl.ds(I0, SUB), :], misc_sem.at[I1]),
        pltpu.make_async_copy(pd.at[I1], pxs.at[:, pl.ds(SUB + ROWS, SUB), :], misc_sem.at[I2]),
        pltpu.make_async_copy(hr, hrs, misc_sem.at[I3]),
        pltpu.make_async_copy(hx2.at[I3], hks, misc_sem.at[4]),
    ]
    for t in range(I2):
        cols = pl.ds(LANE * t, LANE)
        misc.append(pltpu.make_async_copy(dep.at[:, cols], hs.at[t, pl.ds(SUB, ROWS), :], misc_sem.at[5 + 4 * t]))
        misc.append(pltpu.make_async_copy(kmt.at[:, cols], ki.at[t, pl.ds(SUB, ROWS), :], misc_sem.at[6 + 4 * t]))
        misc.append(pltpu.make_async_copy(hrh.at[I1, pl.ds(I0, SUB), cols], hs.at[t, pl.ds(SUB + ROWS, SUB), :], misc_sem.at[7 + 4 * t]))
        misc.append(pltpu.make_async_copy(hrk.at[I1, pl.ds(I0, SUB), cols], ki.at[t, pl.ds(SUB + ROWS, SUB), :], misc_sem.at[SUB + 4 * t]))
    for cp in misc:
        cp.start()
    for c in range(NCH - I1, NCH - I1 - SLOTS, -I1):
        for cp in load_copies(jnp.int32(c)):
            cp.start()
    for cp in misc:
        cp.wait()
    lane = lane_ids()
    is_last = lane == LAST
    is_first = lane == I0
    two = range(I2)
    for m in range(MEM):
        pxs[m, I0:SUB, :] = pxs[m, I0:SUB, :] * not_south
        pxs[m, SUB + ROWS:NEXT, :] = pxs[m, SUB + ROWS:NEXT, :] * not_north
        for f, (_, dst) in enumerate(fields):
            for t in two:
                for g in two:
                    ks = pl.ds(SUB * g, SUB)
                    dst[t, ks, m, 7:SUB, :] = (hrs[I0, m, f, t, ks, :] * not_south)[:, None, :]
                    dst[t, ks, m, SUB + ROWS:9 + ROWS, :] = (hrs[I1, m, f, t, ks, :] * not_north)[:, None, :]
    for t in two:
        kf[t, SUB:SUB + ROWS, :] = ki[t, SUB:SUB + ROWS, :].astype(F32)
        kf[t, SUB + ROWS:NEXT, :] = ki[t, SUB + ROWS:NEXT, :].astype(F32) * not_north
    rho_s = PRESS / LEV * HALINE
    rho_t = PRESS / LEV * THERM
    gain, inner, last = solve_factors(DIFF)
    zero = jnp.zeros((SUB, LANE), F32)

    def east(a, b, halo):
        ra, rb = rot(a, LAST), rot(b, LAST)
        return jnp.where(is_last, rb, ra), jnp.where(is_last, halo, rb)

    def push(x, edge, q):
        return [rot(a, LAST) for a in x] + [rot(edge, LAST - I2 * q)], [rot(a, I1) for a in x] + [rot(edge, 129 - I2 * q)]

    def pop_east(east_):
        return jnp.where(is_last, east_[I1], east_[I0]), jnp.where(is_last, east_[I2], east_[I1])

    def pop_west(west_):
        return jnp.where(is_first, west_[I2], west_[I0]), jnp.where(is_first, west_[I0], west_[I1])

    def unpack(r, m, k, edge):
        slot = lax.rem(jnp.maximum(r, I0) // BPC, SLOTS)
        src_rows = pl.ds(pl.multiple_of(SUB * lax.rem(jnp.maximum(r, I0), BPC), SUB), SUB)
        dst_rows = pl.ds(pl.multiple_of(jnp.where(r < I0, NEXT, SUB * r + SUB), SUB), SUB)
        rolled = []
        for f, (_, dst) in enumerate(fields):
            x = [stage[slot, f, k, m, src_rows, TILES[t]] for t in two]
            for t in two:
                dst[t, k, m, dst_rows, :] = x[t]
            rolled.append(push(x, edge, f * LEV + k))
        return rolled

    def settle(r, m, k, rolled):
        dst_rows = pl.ds(pl.multiple_of(jnp.where(r < I0, NEXT, SUB * r + SUB), SUB), SUB)
        ring = lax.rem(r + I2, I2)
        for f in range(4):
            east_, west_ = pop_east(rolled[f][I0]), pop_west(rolled[f][I1])
            for t in two:
                if f == I0:
                    sides[I0, ring, t, k, m, :, :] = east_[t]
                    uwl[t, k, m, dst_rows, :] = west_[t]
                elif f == I1:
                    vel[t, k, m, dst_rows, :] = east_[t]
                    sides[I1, ring, t, k, m, :, :] = west_[t]
                else:
                    sides[I2 * f - I2, ring, t, k, m, :, :] = east_[t]
                    sides[I2 * f - I1, ring, t, k, m, :, :] = west_[t]

    def prime(m, carry):
        south, north, first = pl.ds(I0, SUB), pl.ds(SUB + ROWS, SUB), pl.ds(ROWS, SUB)
        below = [zero, zero]
        for k in range(LEV):
            settle(jnp.int32(ROWS // SUB - I1), m, k, unpack(jnp.int32(ROWS // SUB - I1), m, k, pxs[m, first, :]))
            v_side = push([vs[t, k, m, south, :] for t in two], pxs[m, south, :], LEV + k)[I0]
            u_side = push([us[t, k, m, north, :] for t in two], pxs[m, north, :], k)[I1]
            for t, x in enumerate(pop_east(v_side)):
                vel[t, k, m, south, :] = x
            for t, x in enumerate(pop_west(u_side)):
                uwl[t, k, m, north, :] = x
            for t in two:
                half = (HALF * rho_s) * ss[t, k, m, north, :] - (HALF * rho_t) * ts[t, k, m, north, :]
                ps[t, k, m, north, :] = below[t] + half
                below[t] = (below[t] + half) + half
        return carry

    def block(r):
        y = pl.multiple_of(r * SUB + SUB, SUB)
        rows = pl.ds(y, SUB)
        up = pl.ds(y + I1, SUB)
        down = pl.ds(y - I1, SUB)
        south = pl.ds(y - SUB, SUB)
        out_rows = pl.ds(pl.multiple_of(r * SUB, SUB), SUB)
        kc = [kf[t, rows, :] for t in two]
        hk = hks[out_rows, :]
        ke = east(kc[I0], kc[I1], rot(hk, 63))
        hc = [hs[t, rows, :] for t in two]
        he = east(hc[I0], hc[I1], rot(hk, LAST))
        kx = [jnp.minimum(kc[t], ke[t]) for t in two]
        ky = [jnp.minimum(kc[t], kf[t, up, :]) for t in two]
        scale_x, scale_y = [], []
        for t in two:
            nx[out_rows, TILES[t]] = kx[t]
            ny[out_rows, TILES[t]] = ky[t]
            scale_x.append(jnp.where(kx[t] > ZERO, HALF * (hc[t] + he[t]), ZERO) / (jnp.maximum(kx[t], ONE) * NSUB))
            scale_y.append(jnp.where(ky[t] > ZERO, HALF * (hc[t] + hs[t, up, :]), ZERO) / (jnp.maximum(ky[t], ONE) * NSUB))

        ring = lax.rem(r, I2)

        def member(m, carry):
            edge = pxs[m, south, :]
            below = [zero] * 4
            sum_x = [zero, zero]
            sum_y = [zero, zero]
            run_t = [None, None]
            run_s = [None, None]
            waiting = []
            for ahead in range(LEV + DEPTH):
                if ahead < LEV:
                    waiting.append(unpack(r - I1, m, ahead, edge))
                k = ahead - DEPTH
                if k < I0:
                    continue
                settle(r - I1, m, k, waiting.pop(I0))
                for t in two:
                    uc, un, ud = us[t, k, m, rows, :], us[t, k, m, up, :], us[t, k, m, down, :]
                    vc, vn, vd = vs[t, k, m, rows, :], vs[t, k, m, up, :], vs[t, k, m, down, :]
                    tc, sc = ts[t, k, m, rows, :], ss[t, k, m, rows, :]
                    ue, vw, t_e, t_w, s_e, s_w = [sides[i, ring, t, k, m, :, :] for i in range(6)]
                    uw, ve = uwl[t, k, m, rows, :], vel[t, k, m, rows, :]
                    half = (HALF * rho_s) * sc - (HALF * rho_t) * tc
                    press = below[t] + half
                    below[t] = press + half
                    half = (HALF * rho_s) * s_e - (HALF * rho_t) * t_e
                    press_e = below[I2 + t] + half
                    below[I2 + t] = press_e + half
                    ps[t, k, m, rows, :] = press
                    uh, vh, vdh, uwh = HALF * uc, HALF * vc, HALF * vd, HALF * uw
                    vq = (vc + vd) + (ve + vel[t, k, m, down, :])
                    uq = (uc + un) + (uw + uwl[t, k, m, up, :])
                    gu = (press - press_e) - uh * (ue - uw) - 0.125 * (vq * (un - ud))
                    gu = jnp.where(kx[t] > float(k), gu, ZERO)
                    sum_x[t] = sum_x[t] + gu
                    obu[k, m, out_rows, TILES[t]] = uc + gu
                    gv = (press - ps[t, k, m, up, :]) - 0.125 * (uq * (ve - vw)) - vh * (vn - vd)
                    gv = jnp.where(ky[t] > float(k), gv, ZERO)
                    sum_y[t] = sum_y[t] + gv
                    obv[k, m, out_rows, TILES[t]] = vc + gv
                    wet = kc[t] > float(k)
                    for scr, cen, e, w, run, dst in ((ts, tc, t_e, t_w, run_t, ost), (ss, sc, s_e, s_w, run_s, oss)):
                        fx = uh * (cen + e) - uwh * (w + cen)
                        fy = vh * (cen + scr[t, k, m, up, :]) - vdh * (scr[t, k, m, down, :] + cen)
                        new = jnp.where(wet, cen - (fx + fy), ZERO)
                        run[t] = new if k == I0 else new + gain[k - I1] * run[t]
                        dst[k, m, out_rows, TILES[t]] = run[t]
            for t in two:
                sx[m, out_rows, TILES[t]] = scale_x[t] * sum_x[t]
                sy[m, out_rows, TILES[t]] = scale_y[t] * sum_y[t]
                nt = ns = zero
                for k in range(LEV - I1, -I1, -I1):
                    coef = level_factor(kc[t], k, inner, last)
                    nt = coef * ost[k, m, out_rows, TILES[t]] + gain[k] * nt
                    ns = coef * oss[k, m, out_rows, TILES[t]] + gain[k] * ns
                    ost[k, m, out_rows, TILES[t]] = nt
                    oss[k, m, out_rows, TILES[t]] = ns
            return carry

        lax.fori_loop(I0, MEM, member, I0)

    for cp in load_copies(jnp.int32(NCH - I1)):
        cp.wait()
    lax.fori_loop(I0, MEM, prime, I0)

    def step(i, carry):
        r = ROWS // SUB - I1 - i
        c = r // BPC
        edge = lax.rem(r, BPC) == I0

        @pl.when(edge & (c >= I1))
        def _():
            for cp in load_copies(c - I1):
                cp.wait()

        @pl.when(edge & (c >= SLOTS))
        def _():
            for cp in load_copies(c - SLOTS):
                cp.start()

        @pl.when(edge & (c + I1 < NCH))
        def _():
            for cp in out_copies(c + I1):
                cp.start()

        block(r)
        return carry

    lax.fori_loop(I0, ROWS // SUB, step, I0)
    for cp in out_copies(jnp.int32(I0)):
        cp.start()
    for c in range(NCH):
        for cp in out_copies(jnp.int32(c)):
            cp.wait()


def columns_call(u, v, te, sa, px, pd, hr, dep, kmt, hx2, hrh, hrk):
    big = pltpu.VMEM((I2, LEV, MEM, EXT, LANE), F32)
    full = pltpu.VMEM((LEV, MEM, ROWS, COLS), F32)
    o3 = sds(LEV, MEM, ROWS, COLS)
    o2 = sds(MEM, ROWS, COLS)
    o1 = sds(ROWS, COLS)
    return pl.pallas_call(
        columns_kernel,
        name="columns",
        out_shape=(o3, o3, o3, o3, o2, o2, o1, o1),
        in_specs=[ANY] * 12,
        out_specs=(ANY,) * 4 + (VM,) * 4,
        scratch_shapes=[big] * 7
        + [
            pltpu.VMEM((6, I2, I2, LEV, MEM, SUB, LANE), F32),
            pltpu.VMEM((SLOTS, 4, LEV, MEM, CHUNK, COLS), F32),
            pltpu.VMEM((MEM, NEXT, LANE), F32),
            pltpu.VMEM((I2, MEM, 4, I2, LEV, LANE), F32),
            pltpu.VMEM((I2, NEXT, LANE), F32),
            pltpu.VMEM((I2, NEXT, LANE), jnp.int32),
            pltpu.VMEM((I2, NEXT, LANE), F32),
            pltpu.VMEM((ROWS, LANE), F32),
            full, full, full, full,
            pltpu.SemaphoreType.DMA((SLOTS, 4)),
            pltpu.SemaphoreType.DMA((13,)),
            pltpu.SemaphoreType.DMA((4,)),
        ],
        compiler_params=pltpu.CompilerParams(vmem_limit_bytes=LIMIT),
    )(u, v, te, sa, px, pd, hr, dep, kmt, hx2, hrh, hrk)


def forcing_kernel(sx, sy, hxs, hds, hrx, hry, pk, send_sem, recv_sem):
    ids = neighbours()
    enter(ids)
    lane = lane_ids()
    sent = []

    def send(src, dst, who):
        i = len(sent)
        cp = pltpu.make_async_remote_copy(src_ref=src, dst_ref=dst, send_sem=send_sem.at[i], recv_sem=recv_sem.at[i], device_id=ids[who], device_id_type=MESH)
        cp.start()
        sent.append(cp)

    for r in range(ROWS // SUB):
        rows = pl.ds(SUB * r, SUB)
        for i, a in enumerate((sx, sy)):
            pk[i, rows, :] = wide_pack(lane, *[a[m, rows, t] for m in range(MEM) for t in TILES])
    for src, dst in ((sx, hrx), (sy, hry)):
        send(src.at[:, pl.ds(ROWS - HALO, HALO), :], dst.at[I0], "n")
        send(src.at[:, pl.ds(I0, HALO), :], dst.at[I1], "s")
    send(pk, hxs, "x")
    send(pk.at[:, pl.ds(ROWS - HALO, HALO), :], hds.at[I0], "nx")
    send(pk.at[:, pl.ds(I0, HALO), :], hds.at[I1], "sx")
    for cp in sent:
        cp.wait()


def forcing_call(sx, sy):
    return pl.pallas_call(
        forcing_kernel,
        name="forcing",
        out_shape=(sds(I2, ROWS, LANE), sds(I2, I2, HALO, LANE), sds(I2, MEM, HALO, COLS), sds(I2, MEM, HALO, COLS)),
        in_specs=[VM, VM],
        out_specs=(ANY,) * 4,
        scratch_shapes=[pltpu.VMEM((I2, ROWS, LANE), F32), pltpu.SemaphoreType.DMA((7,)), pltpu.SemaphoreType.DMA((7,))],
        compiler_params=pltpu.CompilerParams(collective_id=I1, has_side_effects=True, vmem_limit_bytes=LIMIT),
    )(sx, sy)


def turn_east(x):
    return [rot(a, LAST) for a in x] + [rot(x[I2], 63), rot(x[4], 63)]


def pick_east(r, lane):
    last = lane == LAST
    far = jnp.where(lane == 63, r[5], r[4])
    return [jnp.where(last, r[I1], r[I0]), jnp.where(last, r[4], r[I1]), jnp.where(last, r[I3], r[I2]), jnp.where(last, r[6], r[I3]), jnp.where(last, r[I0], far)]


def turn_west(x):
    return [rot(a, I1) for a in x] + [rot(x[I3], 65), rot(x[4], 65)]


def pick_west(r, lane):
    first = lane == I0
    far = jnp.where(lane == 64, r[5], r[4])
    return [jnp.where(first, r[4], r[I0]), jnp.where(first, r[I0], r[I1]), jnp.where(first, r[6], r[I2]), jnp.where(first, r[I2], r[I3]), jnp.where(first, r[I1], far)]


def turn_east3(x):
    return [rot(a, LAST) for a in x] + [rot(x[I0], 63)]


def pick_east3(r, lane):
    last = lane == LAST
    far = jnp.where(lane == 63, r[I3], r[I2])
    return [jnp.where(last, r[I1], r[I0]), jnp.where(last, r[I2], r[I1]), jnp.where(last, r[I0], far)]


def turn_west3(x):
    return [rot(a, I1) for a in x] + [rot(x[I1], 65)]


def pick_west3(r, lane):
    first = lane == I0
    far = jnp.where(lane == 64, r[I3], r[I2])
    return [jnp.where(first, r[I2], r[I0]), jnp.where(first, r[I0], r[I1]), jnp.where(first, r[I1], far)]


def staged(items, issue, finish, depth):
    queue = []
    for item in items:
        queue.append((item, issue(item)))
        if len(queue) > depth:
            finish(*queue.pop(I0))
    for item, value in queue:
        finish(item, value)


SHARED = (I0, I1, I0, I1, I2)


def subcycle_kernel(weights, eta, tx, ty, sx, sy, dep, kmt, hx2, hd2, hre, hrx, hry, hrh, hrk, hxs, hds, hrsx, hrsy, bu, bv, nx, ny, eta_out, tx_out, ty_out, ou, ov, cx_out, cy_out, sol_u, sol_v, cnt_x, cnt_y, far_sem, nat, side, hn, kn, e0, e1, t1, t2, f1, f2, hh, kf, gx, gy, gxw, gc, wv, fo, acc1, acc2, ee, ew, tails, sem):
    row = lax.axis_index("row")
    not_south = jnp.where(row == I0, ZERO, ONE).astype(F32)
    not_north = jnp.where(row == NR - I1, ZERO, ONE).astype(F32)
    lane = lane_ids()
    base = SUB + HALO
    top = base + ROWS
    low, mid, high = pl.ds(I0, HALO), pl.ds(HALO, ROWS), pl.ds(HALO + ROWS, HALO)
    copies = []

    def fetch(src, dst):
        copies.append(pltpu.make_async_copy(src, dst, sem))

    for i, (own_, rows_) in enumerate(((eta, hre), (tx, hrx), (ty, hry), (sx, hrsx), (sy, hrsy))):
        fetch(own_, nat.at[i, :, mid, :])
        fetch(rows_.at[I0], nat.at[i, :, low, :])
        fetch(rows_.at[I1], nat.at[i, :, high, :])
    for first, count, main, corner in ((I0, 4, hx2, hd2), (4, I2, hxs, hds)):
        part = pl.ds(first, count)
        fetch(main, side.at[part, mid, :])
        fetch(corner.at[I0], side.at[part, low, :])
        fetch(corner.at[I1], side.at[part, high, :])
    for own_, rows_, dst in ((dep, hrh, hn), (kmt, hrk, kn)):
        fetch(own_, dst.at[mid, :])
        fetch(rows_.at[I0], dst.at[low, :])
        fetch(rows_.at[I1], dst.at[high, :])
    for cp in copies:
        cp.start()
    incoming = [pltpu.make_async_copy(src, dst, far_sem.at[I0]) for src, dst in ((bu, sol_u), (bv, sol_v), (nx, cnt_x), (ny, cnt_y))]
    for cp in incoming:
        cp.start()
    total = jnp.float32(ZERO)
    moment = jnp.float32(ZERO)
    for n in range(NSUB - I1, -I1, -I1):
        total = total + weights[n]
        moment = moment + total
        tails[n] = total
    for cp in copies:
        cp.wait()
    own = (lane < 32) | (lane >= 96)
    zero = jnp.zeros((SUB, LANE), F32)
    three, five = range(I3), range(5)
    for i in three:
        kf[i, I0:SUB, :] = zero
        kf[i, SUB + NEAR:BEXT, :] = zero
    everything = range(I1, I1 + NEAR // SUB)

    def rows_of(r):
        return pl.ds(SUB * r, SUB), pl.ds(SUB * r + I1, SUB), pl.ds(SUB * r - I1, SUB), pl.ds(SUB * r - SUB, SUB)

    def level_issue(r):
        here = rows_of(r)[I3]
        packed = side[I3, here, :]
        return packed, rot(packed, 64)

    def level_finish(r, value):
        packed, turned = value
        rows, _, _, here = rows_of(r)
        levels = [kn[here, t].astype(F32) for t in TILES] + [jnp.where(own, turned, packed)]
        depths = [hn[here, t] for t in TILES] + [jnp.where(own, packed, turned)]
        keep = not_south if r < base // SUB else not_north
        inside = base // SUB <= r < top // SUB
        for i in three:
            kf[i, rows, :] = levels[i] if inside else levels[i] * keep
            hh[i, rows, :] = depths[i]

    staged(everything, level_issue, level_finish, SUB)

    def mask_issue(r):
        rows = rows_of(r)[I0]
        kc = [kf[i, rows, :] for i in three]
        hc = [hh[i, rows, :] for i in three]
        return kc, hc, turn_east3(kc), turn_east3(hc)

    def mask_finish(r, value):
        kc, hc, kt, ht = value
        rows, up, down, here = rows_of(r)
        ke, he = pick_east3(kt, lane), pick_east3(ht, lane)
        wet = [kc[i] > ZERO for i in three]
        wet_x = [jnp.minimum(kc[i], ke[i]) > ZERO for i in three]
        wet_y = [jnp.minimum(kc[i], kf[i, up, :]) > ZERO for i in three]
        for i in three:
            gx[i, rows, :] = jnp.where(wet_x[i], (HALF * WAVE * WAVE) * (hc[i] + he[i]), ZERO)
            gy[i, rows, :] = jnp.where(wet_y[i], (HALF * WAVE * WAVE) * (hc[i] + hh[i, up, :]), ZERO)
        for f, mask, dst in ((I0, wet, e0), (I1, wet_x, t1), (I2, wet_y, t2), (I3, wet_x, f1), (4, wet_y, f2)):
            slot = f if f < I3 else f + I1
            raw = [nat[f, m, here, t] for m in range(MEM) for t in TILES] + [side[slot, here, :]]
            for i in five:
                dst[i, rows, :] = jnp.where(mask[SHARED[i]], raw[i], ZERO)

    staged(everything, mask_issue, mask_finish, I3)

    def start_issue(r):
        rows = rows_of(r)[I0]
        a = [t1[i, rows, :] for i in five]
        c = [f1[i, rows, :] for i in five]
        return a, c, turn_west(a), turn_west(c), turn_west3([gx[i, rows, :] for i in three])

    late = []

    def start_finish(r, value):
        a, c, at, ct, gt = value
        rows, up, down, here = rows_of(r)
        aw, cw, gw = pick_west(at, lane), pick_west(ct, lane), pick_west3(gt, lane)
        for i in three:
            gxw[i, rows, :] = gw[i]
            gc[i, rows, :] = (gx[i, rows, :] + gw[i]) + (gy[i, rows, :] + gy[i, down, :])
        fresh = []
        for i in five:
            w = -WAVE * ((a[i] - aw[i]) + (t2[i, rows, :] - t2[i, down, :]))
            fo[i, rows, :] = -WAVE * ((c[i] - cw[i]) + (f2[i, rows, :] - f2[i, down, :]))
            now = e0[i, rows, :] + w
            wv[i, rows, :] = w
            e0[i, rows, :] = now
            acc1[i, rows, :] = weights[I0] * now
            acc2[i, rows, :] = tails[I0] * now
            fresh.append(now)
        late.append((r, turn_east(fresh), turn_west(fresh)))
        if len(late) > I3:
            store_sides(*late.pop(I0), I0)

    def store_sides(r, et, wt, buf):
        rows = rows_of(r)[I0]
        ne, nw = pick_east(et, lane), pick_west(wt, lane)
        for i in five:
            ee[buf, i, rows, :] = ne[i]
            ew[buf, i, rows, :] = nw[i]

    staged(everything, start_issue, start_finish, I3)
    for item in late:
        store_sides(*item, I0)

    def advance(src, buf, dst, r, plan):
        rows, up, down, _ = rows_of(r)
        gxc, gxm, gyc, gyd, gcc = [[g[i, rows_, :] for i in three] for g, rows_ in ((gx, rows), (gxw, rows), (gy, rows), (gy, down), (gc, rows))]
        fresh = []
        for i in five:
            j = SHARED[i]
            now = src[i, rows, :]
            w = (wv[i, rows, :] + fo[i, rows, :]) - gcc[j] * now
            w = w + ((gxc[j] * ee[buf, i, rows, :] + gxm[j] * ew[buf, i, rows, :]) + (gyc[j] * src[i, up, :] + gyd[j] * src[i, down, :]))
            new = now + w
            wv[i, rows, :] = w
            dst[i, rows, :] = new
            fresh.append(new)
            if plan is not None:
                prev, a0, b0, a1, b1 = plan
                s1, s2 = acc1[i, rows, :], acc2[i, rows, :]
                if prev:
                    s1 = s1 + a0 * now
                    s2 = s2 + b0 * now
                acc1[i, rows, :] = s1 + a1 * new
                acc2[i, rows, :] = s2 + b1 * new
        return turn_east(fresh), turn_west(fresh)

    def sweep(src, buf, dst, lo, hi, plan, depth=I3):
        def issue(r):
            return advance(src, buf, dst, r, plan if base // SUB <= r <= top // SUB else None)

        def finish(r, value):
            store_sides(r, *value, I1 - buf)

        staged(range(lo, hi), issue, finish, depth)

    for begin, end in ((I0, I2), (I2, 6), (6, 10), (10, 14)):
        lo = (I2 * begin + 12) // SUB
        hi = (196 - I2 * begin) // SUB + I1

        def pair(i, carry):
            m = I2 * i + I2
            sweep(e0, I0, e1, lo, hi, None)
            sweep(e1, I1, e0, lo, hi, (True, weights[m - I1], tails[m - I1], weights[m], tails[m]))
            return carry

        lax.fori_loop(begin, end, pair, I0)
    sweep(e0, I0, e1, base // SUB, top // SUB + I1, (False, None, None, weights[NSUB - I1], tails[NSUB - I1]))

    def end_issue(r):
        rows = rows_of(r)[I0]
        s = [acc2[i, rows, :] for i in five]
        return s, turn_east(s)

    def end_finish(r, value):
        s, st = value
        rows, up, _, _ = rows_of(r)
        out_rows = pl.ds(SUB * r - base, SUB)
        se = pick_east(st, lane)
        for m in range(MEM):
            for t in range(I2):
                i = I2 * m + t
                cols = TILES[t]
                eta_out[m, out_rows, cols] = acc1[i, rows, :]
                gxc, gyc = gx[t, rows, :], gy[t, rows, :]
                ux = total * t1[i, rows, :] + moment * f1[i, rows, :] - (ONE / WAVE) * (gxc * (se[i] - s[i]))
                uy = total * t2[i, rows, :] + moment * f2[i, rows, :] - (ONE / WAVE) * (gyc * (acc2[i, up, :] - s[i]))
                tx_out[m, out_rows, cols] = ux
                ty_out[m, out_rows, cols] = uy
                cx_out[m, out_rows, cols] = ux / jnp.where(gxc > ZERO, gxc * (ONE / (WAVE * WAVE)), ONE)
                cy_out[m, out_rows, cols] = uy / jnp.where(gyc > ZERO, gyc * (ONE / (WAVE * WAVE)), ONE)

    staged(range(base // SUB, top // SUB), end_issue, end_finish, I3)
    for cp in incoming:
        cp.wait()
    gain, inner, last = solve_factors(VISC)

    def body(j, carry):
        rows = pl.ds(pl.multiple_of(j * SUB, SUB), SUB)
        for src, cnt, shift in ((sol_u, cnt_x, cx_out), (sol_v, cnt_y, cy_out)):
            for cols in TILES:
                n = cnt[rows, cols]
                run = []
                for k in range(LEV):
                    b = [src[k, m, rows, cols] for m in range(MEM)]
                    run.append(b if k == I0 else [b[m] + gain[k - I1] * run[-I1][m] for m in range(MEM)])
                nxt = [jnp.zeros((SUB, LANE), F32)] * MEM
                tot = list(nxt)
                sol = [None] * LEV
                for k in range(LEV - I1, -I1, -I1):
                    coef = level_factor(n, k, inner, last)
                    nxt = [coef * run[k][m] + gain[k] * nxt[m] for m in range(MEM)]
                    tot = [tot[m] + nxt[m] for m in range(MEM)]
                    sol[k] = nxt
                share = ONE / jnp.maximum(n, ONE)
                add = [shift[m, rows, cols] - tot[m] * share for m in range(MEM)]
                for k in range(LEV):
                    wet = n > float(k)
                    for m in range(MEM):
                        src[k, m, rows, cols] = jnp.where(wet, sol[k][m] + add[m], ZERO)
        return carry

    def outgoing(c):
        rows = pl.ds(HALO * c, HALO)
        return [pltpu.make_async_copy(a.at[:, :, rows, :], b.at[:, :, rows, :], far_sem.at[I1]) for a, b in ((sol_u, ou), (sol_v, ov))]

    for c in range(ROWS // HALO):
        lax.fori_loop(c * (HALO // SUB), (c + I1) * (HALO // SUB), body, I0)
        for cp in outgoing(c):
            cp.start()
    for c in range(ROWS // HALO):
        for cp in outgoing(c):
            cp.wait()


def subcycle_call(weights, *arrays):
    o2 = sds(MEM, ROWS, COLS)
    o3 = sds(LEV, MEM, ROWS, COLS)
    five = pltpu.VMEM((5, BEXT, LANE), F32)
    three = pltpu.VMEM((I3, BEXT, LANE), F32)
    return pl.pallas_call(
        subcycle_kernel,
        name="subcycle",
        out_shape=(o2, o2, o2, o3, o3),
        in_specs=[SM] + [ANY] * len(arrays),
        out_specs=(VM, VM, VM, ANY, ANY),
        scratch_shapes=[
            pltpu.VMEM((MEM, ROWS, COLS), F32),
            pltpu.VMEM((MEM, ROWS, COLS), F32),
            pltpu.VMEM((LEV, MEM, ROWS, COLS), F32),
            pltpu.VMEM((LEV, MEM, ROWS, COLS), F32),
            pltpu.VMEM((ROWS, COLS), F32),
            pltpu.VMEM((ROWS, COLS), F32),
            pltpu.SemaphoreType.DMA((I2,)),
            pltpu.VMEM((5, MEM, NEAR, COLS), F32),
            pltpu.VMEM((6, NEAR, LANE), F32),
            pltpu.VMEM((NEAR, COLS), F32),
            pltpu.VMEM((NEAR, COLS), jnp.int32),
            *[five] * 6, *[three] * 6, *[five] * 4, pltpu.VMEM((I2, 5, BEXT, LANE), F32), pltpu.VMEM((I2, 5, BEXT, LANE), F32),
            pltpu.SMEM((NSUB,), F32),
            pltpu.SemaphoreType.DMA,
        ],
        compiler_params=pltpu.CompilerParams(vmem_limit_bytes=LIMIT),
    )(weights, *arrays)


def local_step(u, v, te, sa, eta, tx, ty, dep, kmt, weights):
    px, pd, hr, hx2, hd2, hre, hrx, hry, hrh, hrk = edges_call(u, v, te, sa, eta, tx, ty, dep, kmt)
    bu, bv, ot, os, sx, sy, nx, ny = columns_call(u, v, te, sa, px, pd, hr, dep, kmt, hx2, hrh, hrk)
    hxs, hds, hrsx, hrsy = forcing_call(sx, sy)
    eta_new, tx_new, ty_new, ou, ov = subcycle_call(weights, eta, tx, ty, sx, sy, dep, kmt, hx2, hd2, hre, hrx, hry, hrh, hrk, hxs, hds, hrsx, hrsy, bu, bv, nx, ny)
    return eta_new, tx_new, ty_new, ou, ov, ot, os


def solution(mesh):
    s3 = P(None, None, "row", "col")
    s2 = P(None, "row", "col")
    s1 = P("row", "col")
    return jax.shard_map(local_step, mesh=mesh, in_specs=(s3, s3, s3, s3, s2, s2, s2, s1, s1, P()), out_specs=(s2, s2, s2, s3, s3, s3, s3), check_vma=False)
```

```python
import functools
import jax
import jax.numpy as jnp
from jax import lax
from jax.experimental import pallas as pl
from jax.experimental.pallas import tpu as pltpu
from jax.sharding import PartitionSpec as P

SUB = 8
LANE = 128
LAST = 127
ZERO = 0.0
ONE = 1.0
HALF = 0.5
I0, I1, I2, I3 = range(4)
WAVE = 0.4
THERM = 0.2
HALINE = 0.15
PRESS = HALF
VISC = ONE
DIFF = HALF
LEV = 16
MEM = I2
NSUB = 30
ROWS = LANE
COLS = 256
NR = SUB
NC = I2
HALO = 32
NEXT = 144
EXT = 152
BEXT = 208
NEAR = 192
F32 = jnp.float32
CHUNK = 16
NCH = ROWS // CHUNK
SLOTS = I3
BPC = CHUNK // SUB
DEPTH = I2
MESH = pl.DeviceIdType.MESH
LIMIT = 67043328
TILES = (slice(I0, LANE), slice(LANE, 256))
ANY = pl.BlockSpec(memory_space=pl.ANY)
VM = pl.BlockSpec(memory_space=pltpu.VMEM)
SM = pl.BlockSpec(memory_space=pltpu.SMEM)


def solve_factors(strength):
    gain, inner, last = [], [], []
    prev = None
    for k in range(LEV):
        if k == I0:
            diag, edge = ONE + strength, ONE
        else:
            diag, edge = ONE + 2.0 * strength - strength * prev, ONE + strength - strength * prev
        inner.append(ONE / diag)
        last.append(ONE / edge)
        prev = strength / diag
        gain.append(prev)
    return gain, inner, last


def level_factor(count, k, inner, last):
    edge = jnp.where(count > float(k), last[k], ZERO)
    return edge if k == LEV - I1 else jnp.where(count > float(k + I1), inner[k], edge)


def lane_ids():
    return lax.broadcasted_iota(jnp.int32, (SUB, LANE), I1)


def rot(x, shift):
    shift %= LANE
    return x if shift == I0 else pltpu.roll(x, shift, I1)


def neighbours():
    col = lax.axis_index("col")
    row = lax.axis_index("row")
    other = I1 - col
    north = lax.rem(row + I1, NR)
    south = lax.rem(row + NR - I1, NR)
    return {"x": (other, row), "n": (col, north), "s": (col, south), "nx": (other, north), "sx": (other, south)}


def enter(ids):
    barrier = pltpu.get_barrier_semaphore()
    for target in ids.values():
        pl.semaphore_signal(barrier, inc=I1, device_id=target, device_id_type=MESH)
    pl.semaphore_wait(barrier, len(ids))


def wide_pack(lane, m0t0, m0t1, m1t0, m1t1):
    first = jnp.where(lane < 64, m0t0, m0t1)
    second = jnp.where(lane < 64, m1t0, m1t1)
    return jnp.where((lane < 32) | (lane >= 96), first, rot(second, 64))


def edges_kernel(u, v, te, sa, eta, tx, ty, dep, kmt, px, pd, hr, hx2, hd2, hre, hrx, hry, hrh, hrk, big, s2, sh, sk, pk, rowb, pk2, load_sem, load2_sem, send_sem, recv_sem):
    ids = neighbours()
    fields = (u, v, te, sa)
    loads = []
    for m in range(MEM):
        loads.append([pltpu.make_async_copy(fields[f].at[:, m], big.at[m, f], load_sem.at[m, f]) for f in range(4)])
    loads2 = [pltpu.make_async_copy(a, s2.at[i], load2_sem.at[i]) for i, a in enumerate((eta, tx, ty))]
    loads2.append(pltpu.make_async_copy(dep, sh, load2_sem.at[I3]))
    loads2.append(pltpu.make_async_copy(kmt, sk, load2_sem.at[4]))
    for cp in loads2:
        cp.start()
    for cp in loads[I0] + loads[I1]:
        cp.start()
    enter(ids)
    sent = []

    def send(src, dst, who):
        i = len(sent)
        cp = pltpu.make_async_remote_copy(src_ref=src, dst_ref=dst, send_sem=send_sem.at[i], recv_sem=recv_sem.at[i], device_id=ids[who], device_id_type=MESH)
        cp.start()
        sent.append(cp)
        return cp

    for src, dst in ((eta, hre), (tx, hrx), (ty, hry)):
        send(src.at[:, pl.ds(ROWS - HALO, HALO), :], dst.at[I0], "n")
        send(src.at[:, pl.ds(I0, HALO), :], dst.at[I1], "s")
    for src, dst in ((dep, hrh), (kmt, hrk)):
        send(src.at[pl.ds(ROWS - HALO, HALO), :], dst.at[I0], "n")
        send(src.at[pl.ds(I0, HALO), :], dst.at[I1], "s")
    lane = lane_ids()
    for cp in loads2:
        cp.wait()
    for r in range(ROWS // SUB):
        rows = pl.ds(SUB * r, SUB)
        for i in range(I3):
            pk2[i, rows, :] = wide_pack(lane, *[s2[i, m, rows, t] for m in range(MEM) for t in TILES])
        pk2[I3, rows, :] = wide_pack(lane, *[sh[rows, t] for t in TILES], *[sk[rows, t].astype(F32) for t in TILES])
    pair = lax.rem(lane + I1, LANE) // I2

    def pack3(m):
        for cp in loads[m]:
            cp.wait()

        def body(g, carry):
            for j in range(4):
                rows = pl.ds(pl.multiple_of(g * 32 + SUB * j, SUB), SUB)
                acc = jnp.zeros((SUB, LANE), F32)
                for f in range(4):
                    for k in range(LEV):
                        q = f * LEV + k
                        both = jnp.where(lane < 64, big[m, f, k, rows, TILES[I0]], big[m, f, k, rows, TILES[I1]])
                        acc = jnp.where(pair == q, rot(both, I2 * q), acc)
                pk[m, rows, :] = acc
            return carry

        lax.fori_loop(I0, 4, body, I0)
        for f in range(4):
            for t in range(I2):
                for g in range(I2):
                    ks = pl.ds(SUB * g, SUB)
                    rowb[I0, m, f, t, ks, :] = big[m, f, ks, ROWS - I1, TILES[t]]
                    rowb[I1, m, f, t, ks, :] = big[m, f, ks, I0, TILES[t]]

    def send3(m):
        send(pk.at[m], px.at[m], "x")
        send(pk.at[m, pl.ds(ROWS - SUB, SUB), :], pd.at[I0, m], "nx")
        send(pk.at[m, pl.ds(I0, SUB), :], pd.at[I1, m], "sx")
        send(rowb.at[I0, m], hr.at[I0, m], "n")
        send(rowb.at[I1, m], hr.at[I1, m], "s")

    side = send(pk2, hx2, "x")
    pack3(I0)
    send3(I0)
    pack3(I1)
    send3(I1)
    side.wait()
    send(hx2.at[:, pl.ds(ROWS - HALO, HALO), :], hd2.at[I0], "n")
    send(hx2.at[:, pl.ds(I0, HALO), :], hd2.at[I1], "s")
    for cp in sent:
        if cp is not side:
            cp.wait()


def sds(*shape, dtype=F32):
    return jax.ShapeDtypeStruct(shape, dtype)


NSEND_A = 23


def edges_call(u, v, te, sa, eta, tx, ty, dep, kmt):
    return pl.pallas_call(
        edges_kernel,
        name="edges",
        out_shape=(
            sds(MEM, ROWS, LANE), sds(I2, MEM, SUB, LANE), sds(I2, MEM, 4, I2, LEV, LANE),
            sds(4, ROWS, LANE), sds(I2, 4, HALO, LANE),
            sds(I2, MEM, HALO, COLS), sds(I2, MEM, HALO, COLS), sds(I2, MEM, HALO, COLS),
            sds(I2, HALO, COLS), sds(I2, HALO, COLS, dtype=jnp.int32),
        ),
        in_specs=[ANY] * 9,
        out_specs=(ANY,) * 10,
        scratch_shapes=[
            pltpu.VMEM((MEM, 4, LEV, ROWS, COLS), F32),
            pltpu.VMEM((I3, MEM, ROWS, COLS), F32),
            pltpu.VMEM((ROWS, COLS), F32),
            pltpu.VMEM((ROWS, COLS), jnp.int32),
            pltpu.VMEM((MEM, ROWS, LANE), F32),
            pltpu.VMEM((I2, MEM, 4, I2, LEV, LANE), F32),
            pltpu.VMEM((4, ROWS, LANE), F32),
            pltpu.SemaphoreType.DMA((MEM, 4)),
            pltpu.SemaphoreType.DMA((5,)),
            pltpu.SemaphoreType.DMA((NSEND_A,)),
            pltpu.SemaphoreType.DMA((NSEND_A,)),
        ],
        compiler_params=pltpu.CompilerParams(collective_id=I0, has_side_effects=True, vmem_limit_bytes=LIMIT),
    )(u, v, te, sa, eta, tx, ty, dep, kmt)


def columns_kernel(u, v, te, sa, px, pd, hr, dep, kmt, hx2, hrh, hrk, bu, bv, ot, os, sx, sy, nx, ny, us, vs, ts, ss, ps, vel, uwl, sides, stage, pxs, hrs, hs, ki, kf, hks, obu, obv, ost, oss, load_sem, misc_sem, out_sem):
    row = lax.axis_index("row")
    not_south = jnp.where(row == I0, ZERO, ONE).astype(F32)
    not_north = jnp.where(row == NR - I1, ZERO, ONE).astype(F32)
    fields = ((u, us), (v, vs), (te, ts), (sa, ss))

    def load_copies(c):
        rows = pl.ds(pl.multiple_of(CHUNK * c, CHUNK), CHUNK)
        slot = lax.rem(c, SLOTS)
        return [pltpu.make_async_copy(src.at[:, :, rows, :], stage.at[slot, f], load_sem.at[slot, f]) for f, (src, _) in enumerate(fields)]

    def out_copies(c):
        rows = pl.ds(pl.multiple_of(CHUNK * c, CHUNK), CHUNK)
        return [pltpu.make_async_copy(a.at[:, :, rows, :], b.at[:, :, rows, :], out_sem.at[i]) for i, (a, b) in enumerate(((obu, bu), (obv, bv), (ost, ot), (oss, os)))]

    misc = [
        pltpu.make_async_copy(px, pxs.at[:, pl.ds(SUB, ROWS), :], misc_sem.at[I0]),
        pltpu.make_async_copy(pd.at[I0], pxs.at[:, pl.ds(I0, SUB), :], misc_sem.at[I1]),
        pltpu.make_async_copy(pd.at[I1], pxs.at[:, pl.ds(SUB + ROWS, SUB), :], misc_sem.at[I2]),
        pltpu.make_async_copy(hr, hrs, misc_sem.at[I3]),
        pltpu.make_async_copy(hx2.at[I3], hks, misc_sem.at[4]),
    ]
    for t in range(I2):
        cols = pl.ds(LANE * t, LANE)
        misc.append(pltpu.make_async_copy(dep.at[:, cols], hs.at[t, pl.ds(SUB, ROWS), :], misc_sem.at[5 + 4 * t]))
        misc.append(pltpu.make_async_copy(kmt.at[:, cols], ki.at[t, pl.ds(SUB, ROWS), :], misc_sem.at[6 + 4 * t]))
        misc.append(pltpu.make_async_copy(hrh.at[I1, pl.ds(I0, SUB), cols], hs.at[t, pl.ds(SUB + ROWS, SUB), :], misc_sem.at[7 + 4 * t]))
        misc.append(pltpu.make_async_copy(hrk.at[I1, pl.ds(I0, SUB), cols], ki.at[t, pl.ds(SUB + ROWS, SUB), :], misc_sem.at[SUB + 4 * t]))
    for cp in misc:
        cp.start()
    for c in range(NCH - I1, NCH - I1 - SLOTS, -I1):
        for cp in load_copies(jnp.int32(c)):
            cp.start()
    for cp in misc:
        cp.wait()
    lane = lane_ids()
    is_last = lane == LAST
    is_first = lane == I0
    two = range(I2)
    for m in range(MEM):
        pxs[m, I0:SUB, :] = pxs[m, I0:SUB, :] * not_south
        pxs[m, SUB + ROWS:NEXT, :] = pxs[m, SUB + ROWS:NEXT, :] * not_north
        for f, (_, dst) in enumerate(fields):
            for t in two:
                for g in two:
                    ks = pl.ds(SUB * g, SUB)
                    dst[t, ks, m, 7:SUB, :] = (hrs[I0, m, f, t, ks, :] * not_south)[:, None, :]
                    dst[t, ks, m, SUB + ROWS:9 + ROWS, :] = (hrs[I1, m, f, t, ks, :] * not_north)[:, None, :]
    for t in two:
        kf[t, SUB:SUB + ROWS, :] = ki[t, SUB:SUB + ROWS, :].astype(F32)
        kf[t, SUB + ROWS:NEXT, :] = ki[t, SUB + ROWS:NEXT, :].astype(F32) * not_north
    rho_s = PRESS / LEV * HALINE
    rho_t = PRESS / LEV * THERM
    gain, inner, last = solve_factors(DIFF)
    zero = jnp.zeros((SUB, LANE), F32)

    def east(a, b, halo):
        ra, rb = rot(a, LAST), rot(b, LAST)
        return jnp.where(is_last, rb, ra), jnp.where(is_last, halo, rb)

    def push(x, edge, q):
        return [rot(a, LAST) for a in x] + [rot(edge, LAST - I2 * q)], [rot(a, I1) for a in x] + [rot(edge, 129 - I2 * q)]

    def pop_east(east_):
        return jnp.where(is_last, east_[I1], east_[I0]), jnp.where(is_last, east_[I2], east_[I1])

    def pop_west(west_):
        return jnp.where(is_first, west_[I2], west_[I0]), jnp.where(is_first, west_[I0], west_[I1])

    def unpack(r, m, k, edge):
        slot = lax.rem(jnp.maximum(r, I0) // BPC, SLOTS)
        src_rows = pl.ds(pl.multiple_of(SUB * lax.rem(jnp.maximum(r, I0), BPC), SUB), SUB)
        dst_rows = pl.ds(pl.multiple_of(jnp.where(r < I0, NEXT, SUB * r + SUB), SUB), SUB)
        rolled = []
        for f, (_, dst) in enumerate(fields):
            x = [stage[slot, f, k, m, src_rows, TILES[t]] for t in two]
            for t in two:
                dst[t, k, m, dst_rows, :] = x[t]
            rolled.append(push(x, edge, f * LEV + k))
        return rolled

    def settle(r, m, k, rolled):
        dst_rows = pl.ds(pl.multiple_of(jnp.where(r < I0, NEXT, SUB * r + SUB), SUB), SUB)
        ring = lax.rem(r + I2, I2)
        for f in range(4):
            east_, west_ = pop_east(rolled[f][I0]), pop_west(rolled[f][I1])
            for t in two:
                if f == I0:
                    sides[I0, ring, t, k, m, :, :] = east_[t]
                    uwl[t, k, m, dst_rows, :] = west_[t]
                elif f == I1:
                    vel[t, k, m, dst_rows, :] = east_[t]
                    sides[I1, ring, t, k, m, :, :] = west_[t]
                else:
                    sides[I2 * f - I2, ring, t, k, m, :, :] = east_[t]
                    sides[I2 * f - I1, ring, t, k, m, :, :] = west_[t]

    def prime(m, carry):
        south, north, first = pl.ds(I0, SUB), pl.ds(SUB + ROWS, SUB), pl.ds(ROWS, SUB)
        below = [zero, zero]
        for k in range(LEV):
            settle(jnp.int32(ROWS // SUB - I1), m, k, unpack(jnp.int32(ROWS // SUB - I1), m, k, pxs[m, first, :]))
            v_side = push([vs[t, k, m, south, :] for t in two], pxs[m, south, :], LEV + k)[I0]
            u_side = push([us[t, k, m, north, :] for t in two], pxs[m, north, :], k)[I1]
            for t, x in enumerate(pop_east(v_side)):
                vel[t, k, m, south, :] = x
            for t, x in enumerate(pop_west(u_side)):
                uwl[t, k, m, north, :] = x
            for t in two:
                half = (HALF * rho_s) * ss[t, k, m, north, :] - (HALF * rho_t) * ts[t, k, m, north, :]
                ps[t, k, m, north, :] = below[t] + half
                below[t] = (below[t] + half) + half
        return carry

    def block(r):
        y = pl.multiple_of(r * SUB + SUB, SUB)
        rows = pl.ds(y, SUB)
        up = pl.ds(y + I1, SUB)
        down = pl.ds(y - I1, SUB)
        south = pl.ds(y - SUB, SUB)
        out_rows = pl.ds(pl.multiple_of(r * SUB, SUB), SUB)
        kc = [kf[t, rows, :] for t in two]
        hk = hks[out_rows, :]
        ke = east(kc[I0], kc[I1], rot(hk, 63))
        hc = [hs[t, rows, :] for t in two]
        he = east(hc[I0], hc[I1], rot(hk, LAST))
        kx = [jnp.minimum(kc[t], ke[t]) for t in two]
        ky = [jnp.minimum(kc[t], kf[t, up, :]) for t in two]
        scale_x, scale_y = [], []
        for t in two:
            nx[out_rows, TILES[t]] = kx[t]
            ny[out_rows, TILES[t]] = ky[t]
            scale_x.append(jnp.where(kx[t] > ZERO, HALF * (hc[t] + he[t]), ZERO) / (jnp.maximum(kx[t], ONE) * NSUB))
            scale_y.append(jnp.where(ky[t] > ZERO, HALF * (hc[t] + hs[t, up, :]), ZERO) / (jnp.maximum(ky[t], ONE) * NSUB))

        ring = lax.rem(r, I2)

        def member(m, carry):
            edge = pxs[m, south, :]
            below = [zero] * 4
            sum_x = [zero, zero]
            sum_y = [zero, zero]
            run_t = [None, None]
            run_s = [None, None]
            waiting = []
            for ahead in range(LEV + DEPTH):
                if ahead < LEV:
                    waiting.append(unpack(r - I1, m, ahead, edge))
                k = ahead - DEPTH
                if k < I0:
                    continue
                settle(r - I1, m, k, waiting.pop(I0))
                for t in two:
                    uc, un, ud = us[t, k, m, rows, :], us[t, k, m, up, :], us[t, k, m, down, :]
                    vc, vn, vd = vs[t, k, m, rows, :], vs[t, k, m, up, :], vs[t, k, m, down, :]
                    tc, sc = ts[t, k, m, rows, :], ss[t, k, m, rows, :]
                    ue, vw, t_e, t_w, s_e, s_w = [sides[i, ring, t, k, m, :, :] for i in range(6)]
                    uw, ve = uwl[t, k, m, rows, :], vel[t, k, m, rows, :]
                    half = (HALF * rho_s) * sc - (HALF * rho_t) * tc
                    press = below[t] + half
                    below[t] = press + half
                    half = (HALF * rho_s) * s_e - (HALF * rho_t) * t_e
                    press_e = below[I2 + t] + half
                    below[I2 + t] = press_e + half
                    ps[t, k, m, rows, :] = press
                    uh, vh, vdh, uwh = HALF * uc, HALF * vc, HALF * vd, HALF * uw
                    vq = (vc + vd) + (ve + vel[t, k, m, down, :])
                    uq = (uc + un) + (uw + uwl[t, k, m, up, :])
                    gu = (press - press_e) - uh * (ue - uw) - 0.125 * (vq * (un - ud))
                    gu = jnp.where(kx[t] > float(k), gu, ZERO)
                    sum_x[t] = sum_x[t] + gu
                    obu[k, m, out_rows, TILES[t]] = uc + gu
                    gv = (press - ps[t, k, m, up, :]) - 0.125 * (uq * (ve - vw)) - vh * (vn - vd)
                    gv = jnp.where(ky[t] > float(k), gv, ZERO)
                    sum_y[t] = sum_y[t] + gv
                    obv[k, m, out_rows, TILES[t]] = vc + gv
                    wet = kc[t] > float(k)
                    for scr, cen, e, w, run, dst in ((ts, tc, t_e, t_w, run_t, ost), (ss, sc, s_e, s_w, run_s, oss)):
                        fx = uh * (cen + e) - uwh * (w + cen)
                        fy = vh * (cen + scr[t, k, m, up, :]) - vdh * (scr[t, k, m, down, :] + cen)
                        new = jnp.where(wet, cen - (fx + fy), ZERO)
                        run[t] = new if k == I0 else new + gain[k - I1] * run[t]
                        dst[k, m, out_rows, TILES[t]] = run[t]
            for t in two:
                sx[m, out_rows, TILES[t]] = scale_x[t] * sum_x[t]
                sy[m, out_rows, TILES[t]] = scale_y[t] * sum_y[t]
                nt = ns = zero
                for k in range(LEV - I1, -I1, -I1):
                    coef = level_factor(kc[t], k, inner, last)
                    nt = coef * ost[k, m, out_rows, TILES[t]] + gain[k] * nt
                    ns = coef * oss[k, m, out_rows, TILES[t]] + gain[k] * ns
                    ost[k, m, out_rows, TILES[t]] = nt
                    oss[k, m, out_rows, TILES[t]] = ns
            return carry

        lax.fori_loop(I0, MEM, member, I0)

    for cp in load_copies(jnp.int32(NCH - I1)):
        cp.wait()
    lax.fori_loop(I0, MEM, prime, I0)

    def step(i, carry):
        r = ROWS // SUB - I1 - i
        c = r // BPC
        edge = lax.rem(r, BPC) == I0

        @pl.when(edge & (c >= I1))
        def _():
            for cp in load_copies(c - I1):
                cp.wait()

        @pl.when(edge & (c >= SLOTS))
        def _():
            for cp in load_copies(c - SLOTS):
                cp.start()

        @pl.when(edge & (c + I1 < NCH))
        def _():
            for cp in out_copies(c + I1):
                cp.start()

        block(r)
        return carry

    lax.fori_loop(I0, ROWS // SUB, step, I0)
    for cp in out_copies(jnp.int32(I0)):
        cp.start()
    for c in range(NCH):
        for cp in out_copies(jnp.int32(c)):
            cp.wait()


def columns_call(u, v, te, sa, px, pd, hr, dep, kmt, hx2, hrh, hrk):
    big = pltpu.VMEM((I2, LEV, MEM, EXT, LANE), F32)
    full = pltpu.VMEM((LEV, MEM, ROWS, COLS), F32)
    o3 = sds(LEV, MEM, ROWS, COLS)
    o2 = sds(MEM, ROWS, COLS)
    o1 = sds(ROWS, COLS)
    return pl.pallas_call(
        columns_kernel,
        name="columns",
        out_shape=(o3, o3, o3, o3, o2, o2, o1, o1),
        in_specs=[ANY] * 12,
        out_specs=(ANY,) * 4 + (VM,) * 4,
        scratch_shapes=[big] * 7
        + [
            pltpu.VMEM((6, I2, I2, LEV, MEM, SUB, LANE), F32),
            pltpu.VMEM((SLOTS, 4, LEV, MEM, CHUNK, COLS), F32),
            pltpu.VMEM((MEM, NEXT, LANE), F32),
            pltpu.VMEM((I2, MEM, 4, I2, LEV, LANE), F32),
            pltpu.VMEM((I2, NEXT, LANE), F32),
            pltpu.VMEM((I2, NEXT, LANE), jnp.int32),
            pltpu.VMEM((I2, NEXT, LANE), F32),
            pltpu.VMEM((ROWS, LANE), F32),
            full, full, full, full,
            pltpu.SemaphoreType.DMA((SLOTS, 4)),
            pltpu.SemaphoreType.DMA((13,)),
            pltpu.SemaphoreType.DMA((4,)),
        ],
        compiler_params=pltpu.CompilerParams(vmem_limit_bytes=LIMIT),
    )(u, v, te, sa, px, pd, hr, dep, kmt, hx2, hrh, hrk)


def forcing_kernel(sx, sy, hxs, hds, hrx, hry, pk, send_sem, recv_sem):
    ids = neighbours()
    enter(ids)
    lane = lane_ids()
    sent = []

    def send(src, dst, who):
        i = len(sent)
        cp = pltpu.make_async_remote_copy(src_ref=src, dst_ref=dst, send_sem=send_sem.at[i], recv_sem=recv_sem.at[i], device_id=ids[who], device_id_type=MESH)
        cp.start()
        sent.append(cp)

    for r in range(ROWS // SUB):
        rows = pl.ds(SUB * r, SUB)
        for i, a in enumerate((sx, sy)):
            pk[i, rows, :] = wide_pack(lane, *[a[m, rows, t] for m in range(MEM) for t in TILES])
    for src, dst in ((sx, hrx), (sy, hry)):
        send(src.at[:, pl.ds(ROWS - HALO, HALO), :], dst.at[I0], "n")
        send(src.at[:, pl.ds(I0, HALO), :], dst.at[I1], "s")
    send(pk, hxs, "x")
    send(pk.at[:, pl.ds(ROWS - HALO, HALO), :], hds.at[I0], "nx")
    send(pk.at[:, pl.ds(I0, HALO), :], hds.at[I1], "sx")
    for cp in sent:
        cp.wait()


def forcing_call(sx, sy):
    return pl.pallas_call(
        forcing_kernel,
        name="forcing",
        out_shape=(sds(I2, ROWS, LANE), sds(I2, I2, HALO, LANE), sds(I2, MEM, HALO, COLS), sds(I2, MEM, HALO, COLS)),
        in_specs=[VM, VM],
        out_specs=(ANY,) * 4,
        scratch_shapes=[pltpu.VMEM((I2, ROWS, LANE), F32), pltpu.SemaphoreType.DMA((7,)), pltpu.SemaphoreType.DMA((7,))],
        compiler_params=pltpu.CompilerParams(collective_id=I1, has_side_effects=True, vmem_limit_bytes=LIMIT),
    )(sx, sy)


def turn_east(x):
    return [rot(a, LAST) for a in x] + [rot(x[I2], 63), rot(x[4], 63)]


def pick_east(r, lane):
    last = lane == LAST
    far = jnp.where(lane == 63, r[5], r[4])
    return [jnp.where(last, r[I1], r[I0]), jnp.where(last, r[4], r[I1]), jnp.where(last, r[I3], r[I2]), jnp.where(last, r[6], r[I3]), jnp.where(last, r[I0], far)]


def turn_west(x):
    return [rot(a, I1) for a in x] + [rot(x[I3], 65), rot(x[4], 65)]


def pick_west(r, lane):
    first = lane == I0
    far = jnp.where(lane == 64, r[5], r[4])
    return [jnp.where(first, r[4], r[I0]), jnp.where(first, r[I0], r[I1]), jnp.where(first, r[6], r[I2]), jnp.where(first, r[I2], r[I3]), jnp.where(first, r[I1], far)]


def turn_east3(x):
    return [rot(a, LAST) for a in x] + [rot(x[I0], 63)]


def pick_east3(r, lane):
    last = lane == LAST
    far = jnp.where(lane == 63, r[I3], r[I2])
    return [jnp.where(last, r[I1], r[I0]), jnp.where(last, r[I2], r[I1]), jnp.where(last, r[I0], far)]


def turn_west3(x):
    return [rot(a, I1) for a in x] + [rot(x[I1], 65)]


def pick_west3(r, lane):
    first = lane == I0
    far = jnp.where(lane == 64, r[I3], r[I2])
    return [jnp.where(first, r[I2], r[I0]), jnp.where(first, r[I0], r[I1]), jnp.where(first, r[I1], far)]


def staged(items, issue, finish, depth):
    queue = []
    for item in items:
        queue.append((item, issue(item)))
        if len(queue) > depth:
            finish(*queue.pop(I0))
    for item, value in queue:
        finish(item, value)


SHARED = (I0, I1, I0, I1, I2)


def subcycle_kernel(weights, eta, tx, ty, sx, sy, dep, kmt, hx2, hd2, hre, hrx, hry, hrh, hrk, hxs, hds, hrsx, hrsy, bu, bv, nx, ny, eta_out, tx_out, ty_out, ou, ov, cx_out, cy_out, sol_u, sol_v, cnt_x, cnt_y, far_sem, nat, side, hn, kn, e0, e1, t1, t2, f1, f2, hh, kf, gx, gy, gxw, gc, wv, fo, acc1, acc2, ee, ew, tails, sem):
    row = lax.axis_index("row")
    not_south = jnp.where(row == I0, ZERO, ONE).astype(F32)
    not_north = jnp.where(row == NR - I1, ZERO, ONE).astype(F32)
    lane = lane_ids()
    base = SUB + HALO
    top = base + ROWS
    low, mid, high = pl.ds(I0, HALO), pl.ds(HALO, ROWS), pl.ds(HALO + ROWS, HALO)
    copies = []

    def fetch(src, dst):
        copies.append(pltpu.make_async_copy(src, dst, sem))

    for i, (own_, rows_) in enumerate(((eta, hre), (tx, hrx), (ty, hry), (sx, hrsx), (sy, hrsy))):
        fetch(own_, nat.at[i, :, mid, :])
        fetch(rows_.at[I0], nat.at[i, :, low, :])
        fetch(rows_.at[I1], nat.at[i, :, high, :])
    for first, count, main, corner in ((I0, 4, hx2, hd2), (4, I2, hxs, hds)):
        part = pl.ds(first, count)
        fetch(main, side.at[part, mid, :])
        fetch(corner.at[I0], side.at[part, low, :])
        fetch(corner.at[I1], side.at[part, high, :])
    for own_, rows_, dst in ((dep, hrh, hn), (kmt, hrk, kn)):
        fetch(own_, dst.at[mid, :])
        fetch(rows_.at[I0], dst.at[low, :])
        fetch(rows_.at[I1], dst.at[high, :])
    for cp in copies:
        cp.start()
    incoming = [pltpu.make_async_copy(src, dst, far_sem.at[I0]) for src, dst in ((bu, sol_u), (bv, sol_v), (nx, cnt_x), (ny, cnt_y))]
    for cp in incoming:
        cp.start()
    total = jnp.float32(ZERO)
    moment = jnp.float32(ZERO)
    for n in range(NSUB - I1, -I1, -I1):
        total = total + weights[n]
        moment = moment + total
        tails[n] = total
    for cp in copies:
        cp.wait()
    own = (lane < 32) | (lane >= 96)
    zero = jnp.zeros((SUB, LANE), F32)
    three, five = range(I3), range(5)
    for i in three:
        kf[i, I0:SUB, :] = zero
        kf[i, SUB + NEAR:BEXT, :] = zero
    everything = range(I1, I1 + NEAR // SUB)

    def rows_of(r):
        return pl.ds(SUB * r, SUB), pl.ds(SUB * r + I1, SUB), pl.ds(SUB * r - I1, SUB), pl.ds(SUB * r - SUB, SUB)

    def level_issue(r):
        here = rows_of(r)[I3]
        packed = side[I3, here, :]
        return packed, rot(packed, 64)

    def level_finish(r, value):
        packed, turned = value
        rows, _, _, here = rows_of(r)
        levels = [kn[here, t].astype(F32) for t in TILES] + [jnp.where(own, turned, packed)]
        depths = [hn[here, t] for t in TILES] + [jnp.where(own, packed, turned)]
        keep = not_south if r < base // SUB else not_north
        inside = base // SUB <= r < top // SUB
        for i in three:
            kf[i, rows, :] = levels[i] if inside else levels[i] * keep
            hh[i, rows, :] = depths[i]

    staged(everything, level_issue, level_finish, SUB)

    def mask_issue(r):
        rows = rows_of(r)[I0]
        kc = [kf[i, rows, :] for i in three]
        hc = [hh[i, rows, :] for i in three]
        return kc, hc, turn_east3(kc), turn_east3(hc)

    def mask_finish(r, value):
        kc, hc, kt, ht = value
        rows, up, down, here = rows_of(r)
        ke, he = pick_east3(kt, lane), pick_east3(ht, lane)
        wet = [kc[i] > ZERO for i in three]
        wet_x = [jnp.minimum(kc[i], ke[i]) > ZERO for i in three]
        wet_y = [jnp.minimum(kc[i], kf[i, up, :]) > ZERO for i in three]
        for i in three:
            gx[i, rows, :] = jnp.where(wet_x[i], (HALF * WAVE * WAVE) * (hc[i] + he[i]), ZERO)
            gy[i, rows, :] = jnp.where(wet_y[i], (HALF * WAVE * WAVE) * (hc[i] + hh[i, up, :]), ZERO)
        for f, mask, dst in ((I0, wet, e0), (I1, wet_x, t1), (I2, wet_y, t2), (I3, wet_x, f1), (4, wet_y, f2)):
            slot = f if f < I3 else f + I1
            raw = [nat[f, m, here, t] for m in range(MEM) for t in TILES] + [side[slot, here, :]]
            for i in five:
                dst[i, rows, :] = jnp.where(mask[SHARED[i]], raw[i], ZERO)

    staged(everything, mask_issue, mask_finish, I3)

    def start_issue(r):
        rows = rows_of(r)[I0]
        a = [t1[i, rows, :] for i in five]
        c = [f1[i, rows, :] for i in five]
        return a, c, turn_west(a), turn_west(c), turn_west3([gx[i, rows, :] for i in three])

    late = []

    def start_finish(r, value):
        a, c, at, ct, gt = value
        rows, up, down, here = rows_of(r)
        aw, cw, gw = pick_west(at, lane), pick_west(ct, lane), pick_west3(gt, lane)
        for i in three:
            gxw[i, rows, :] = gw[i]
            gc[i, rows, :] = (gx[i, rows, :] + gw[i]) + (gy[i, rows, :] + gy[i, down, :])
        fresh = []
        for i in five:
            w = -WAVE * ((a[i] - aw[i]) + (t2[i, rows, :] - t2[i, down, :]))
            fo[i, rows, :] = -WAVE * ((c[i] - cw[i]) + (f2[i, rows, :] - f2[i, down, :]))
            now = e0[i, rows, :] + w
            wv[i, rows, :] = w
            e0[i, rows, :] = now
            acc1[i, rows, :] = weights[I0] * now
            acc2[i, rows, :] = tails[I0] * now
            fresh.append(now)
        late.append((r, turn_east(fresh), turn_west(fresh)))
        if len(late) > I3:
            store_sides(*late.pop(I0), I0)

    def store_sides(r, et, wt, buf):
        rows = rows_of(r)[I0]
        ne, nw = pick_east(et, lane), pick_west(wt, lane)
        for i in five:
            ee[buf, i, rows, :] = ne[i]
            ew[buf, i, rows, :] = nw[i]

    staged(everything, start_issue, start_finish, I3)
    for item in late:
        store_sides(*item, I0)

    def advance(src, buf, dst, r, plan):
        rows, up, down, _ = rows_of(r)
        gxc, gxm, gyc, gyd, gcc = [[g[i, rows_, :] for i in three] for g, rows_ in ((gx, rows), (gxw, rows), (gy, rows), (gy, down), (gc, rows))]
        fresh = []
        for i in five:
            j = SHARED[i]
            now = src[i, rows, :]
            w = (wv[i, rows, :] + fo[i, rows, :]) - gcc[j] * now
            w = w + ((gxc[j] * ee[buf, i, rows, :] + gxm[j] * ew[buf, i, rows, :]) + (gyc[j] * src[i, up, :] + gyd[j] * src[i, down, :]))
            new = now + w
            wv[i, rows, :] = w
            dst[i, rows, :] = new
            fresh.append(new)
            if plan is not None:
                prev, a0, b0, a1, b1 = plan
                s1, s2 = acc1[i, rows, :], acc2[i, rows, :]
                if prev:
                    s1 = s1 + a0 * now
                    s2 = s2 + b0 * now
                acc1[i, rows, :] = s1 + a1 * new
                acc2[i, rows, :] = s2 + b1 * new
        return turn_east(fresh), turn_west(fresh)

    def sweep(src, buf, dst, lo, hi, plan, depth=I3):
        def issue(r):
            return advance(src, buf, dst, r, plan if base // SUB <= r <= top // SUB else None)

        def finish(r, value):
            store_sides(r, *value, I1 - buf)

        staged(range(lo, hi), issue, finish, depth)

    for begin, end in ((I0, I2), (I2, 6), (6, 10), (10, 14)):
        lo = (I2 * begin + 12) // SUB
        hi = (196 - I2 * begin) // SUB + I1

        def pair(i, carry):
            m = I2 * i + I2
            sweep(e0, I0, e1, lo, hi, None)
            sweep(e1, I1, e0, lo, hi, (True, weights[m - I1], tails[m - I1], weights[m], tails[m]))
            return carry

        lax.fori_loop(begin, end, pair, I0)
    sweep(e0, I0, e1, base // SUB, top // SUB + I1, (False, None, None, weights[NSUB - I1], tails[NSUB - I1]))

    def end_issue(r):
        rows = rows_of(r)[I0]
        s = [acc2[i, rows, :] for i in five]
        return s, turn_east(s)

    def end_finish(r, value):
        s, st = value
        rows, up, _, _ = rows_of(r)
        out_rows = pl.ds(SUB * r - base, SUB)
        se = pick_east(st, lane)
        for m in range(MEM):
            for t in range(I2):
                i = I2 * m + t
                cols = TILES[t]
                eta_out[m, out_rows, cols] = acc1[i, rows, :]
                gxc, gyc = gx[t, rows, :], gy[t, rows, :]
                ux = total * t1[i, rows, :] + moment * f1[i, rows, :] - (ONE / WAVE) * (gxc * (se[i] - s[i]))
                uy = total * t2[i, rows, :] + moment * f2[i, rows, :] - (ONE / WAVE) * (gyc * (acc2[i, up, :] - s[i]))
                tx_out[m, out_rows, cols] = ux
                ty_out[m, out_rows, cols] = uy
                cx_out[m, out_rows, cols] = ux / jnp.where(gxc > ZERO, gxc * (ONE / (WAVE * WAVE)), ONE)
                cy_out[m, out_rows, cols] = uy / jnp.where(gyc > ZERO, gyc * (ONE / (WAVE * WAVE)), ONE)

    staged(range(base // SUB, top // SUB), end_issue, end_finish, I3)
    for cp in incoming:
        cp.wait()
    gain, inner, last = solve_factors(VISC)

    def body(j, carry):
        rows = pl.ds(pl.multiple_of(j * SUB, SUB), SUB)
        for src, cnt, shift in ((sol_u, cnt_x, cx_out), (sol_v, cnt_y, cy_out)):
            for cols in TILES:
                n = cnt[rows, cols]
                run = []
                for k in range(LEV):
                    b = [src[k, m, rows, cols] for m in range(MEM)]
                    run.append(b if k == I0 else [b[m] + gain[k - I1] * run[-I1][m] for m in range(MEM)])
                nxt = [jnp.zeros((SUB, LANE), F32)] * MEM
                tot = list(nxt)
                sol = [None] * LEV
                for k in range(LEV - I1, -I1, -I1):
                    coef = level_factor(n, k, inner, last)
                    nxt = [coef * run[k][m] + gain[k] * nxt[m] for m in range(MEM)]
                    tot = [tot[m] + nxt[m] for m in range(MEM)]
                    sol[k] = nxt
                share = ONE / jnp.maximum(n, ONE)
                add = [shift[m, rows, cols] - tot[m] * share for m in range(MEM)]
                for k in range(LEV):
                    wet = n > float(k)
                    for m in range(MEM):
                        src[k, m, rows, cols] = jnp.where(wet, sol[k][m] + add[m], ZERO)
        return carry

    def outgoing(c):
        rows = pl.ds(HALO * c, HALO)
        return [pltpu.make_async_copy(a.at[:, :, rows, :], b.at[:, :, rows, :], far_sem.at[I1]) for a, b in ((sol_u, ou), (sol_v, ov))]

    for c in range(ROWS // HALO):
        lax.fori_loop(c * (HALO // SUB), (c + I1) * (HALO // SUB), body, I0)
        for cp in outgoing(c):
            cp.start()
    for c in range(ROWS // HALO):
        for cp in outgoing(c):
            cp.wait()


def subcycle_call(weights, *arrays):
    o2 = sds(MEM, ROWS, COLS)
    o3 = sds(LEV, MEM, ROWS, COLS)
    five = pltpu.VMEM((5, BEXT, LANE), F32)
    three = pltpu.VMEM((I3, BEXT, LANE), F32)
    return pl.pallas_call(
        subcycle_kernel,
        name="subcycle",
        out_shape=(o2, o2, o2, o3, o3),
        in_specs=[SM] + [ANY] * len(arrays),
        out_specs=(VM, VM, VM, ANY, ANY),
        scratch_shapes=[
            pltpu.VMEM((MEM, ROWS, COLS), F32),
            pltpu.VMEM((MEM, ROWS, COLS), F32),
            pltpu.VMEM((LEV, MEM, ROWS, COLS), F32),
            pltpu.VMEM((LEV, MEM, ROWS, COLS), F32),
            pltpu.VMEM((ROWS, COLS), F32),
            pltpu.VMEM((ROWS, COLS), F32),
            pltpu.SemaphoreType.DMA((I2,)),
            pltpu.VMEM((5, MEM, NEAR, COLS), F32),
            pltpu.VMEM((6, NEAR, LANE), F32),
            pltpu.VMEM((NEAR, COLS), F32),
            pltpu.VMEM((NEAR, COLS), jnp.int32),
            *[five] * 6, *[three] * 6, *[five] * 4, pltpu.VMEM((I2, 5, BEXT, LANE), F32), pltpu.VMEM((I2, 5, BEXT, LANE), F32),
            pltpu.SMEM((NSUB,), F32),
            pltpu.SemaphoreType.DMA,
        ],
        compiler_params=pltpu.CompilerParams(vmem_limit_bytes=LIMIT),
    )(weights, *arrays)


def local_step(u, v, te, sa, eta, tx, ty, dep, kmt, weights):
    px, pd, hr, hx2, hd2, hre, hrx, hry, hrh, hrk = edges_call(u, v, te, sa, eta, tx, ty, dep, kmt)
    bu, bv, ot, os, sx, sy, nx, ny = columns_call(u, v, te, sa, px, pd, hr, dep, kmt, hx2, hrh, hrk)
    hxs, hds, hrsx, hrsy = forcing_call(sx, sy)
    eta_new, tx_new, ty_new, ou, ov = subcycle_call(weights, eta, tx, ty, sx, sy, dep, kmt, hx2, hd2, hre, hrx, hry, hrh, hrk, hxs, hds, hrsx, hrsy, bu, bv, nx, ny)
    return eta_new, tx_new, ty_new, ou, ov, ot, os


def solution(mesh):
    s3 = P(None, None, "row", "col")
    s2 = P(None, "row", "col")
    s1 = P("row", "col")
    return jax.shard_map(local_step, mesh=mesh, in_specs=(s3, s3, s3, s3, s2, s2, s2, s1, s1, P()), out_specs=(s2, s2, s2, s3, s3, s3, s3), check_vma=False)
```
